256 devices in a mesh: grp: 4 (over x), rep: 8 (over y, z_hi), tp: 8 (over z_lo, core).
Axes of the slice: x: 4, y: 4, z: 8 (z_hi: 2, z_lo: 4; z = z_hi * 4 + z_lo), core: 2. Of those that a mesh axis runs over, the one named last changes fastest.
Arguments:
- noise_in: bfloat16 [1024, 3072], P('rep', 'tp'), may hold values from -6 to 6
- noise_renoise: bfloat16 [1024, 3072], P('rep', 'tp'), may hold values from -6 to 6
- text_cond: bfloat16 [8, 3072], P('rep'), may hold values from -3 to 3
- t_index: int32 [8], P('rep'), may hold values from 0 to 999
- gains: float32 [3, 3072], replicated, may hold values from 0.5 to 1.5
- up_weights: bfloat16 [3, 3072, 12288], P(None, 'rep', 'tp'), may hold values from -0.109375 to 0.109375
- down_weights: bfloat16 [3, 12288, 3072], P(None, 'tp', 'rep'), may hold values from -0.0546875 to 0.0546875
Outputs:
- generated: bfloat16 [1024, 3072], P('rep', 'tp')
- up_grads: float32 [4, 3072, 12288], P('grp', 'rep', 'tp')
- down_grads: float32 [4, 12288, 3072], P('grp', 'tp', 'rep')
The draws below stay inside these ranges and needn't reach their ends.
All inputs are finite; a program needn't handle non-finite values. Where the reference program divides by a largest or mean magnitude, that divisor is 1e-20 or more.
Results may differ from the reference program's by a relative error of at most 0.01.
Values may be sent and summed in bfloat16 or wider, within the bound.
A program may use at most 128 MiB of HBM per device.

```python
import jax
import jax.numpy as jnp
from jax import lax

D = 3072
HID = 12288
IMG_TOK = 128
TOK_DEV = 128
TOKENS = 1024
IMAGES = 8


def touch_ends(drawn, own_key, low, high):
    extent = drawn.shape
    spot = [jax.random.randint(jax.random.fold_in(own_key, axis), (), 0, extent[axis]) for axis in range(len(extent))]
    drawn = drawn.at[tuple(spot)].set(low)
    longest = extent.index(max(extent))
    spot[longest] = (spot[longest] + 1) % extent[longest]
    return drawn.at[tuple(spot)].set(high)


def block_scale(stream_key, dims, split, least, largest):
    def one(axis_at, blocks):
        draws = jax.random.uniform(jax.random.fold_in(jax.random.fold_in(stream_key, 6), axis_at), (blocks,), jnp.float32, least / len(split), largest / len(split))
        return jnp.repeat(jnp.exp(draws), dims[axis_at] // blocks).reshape((-1,) + (1,) * (len(dims) - axis_at - 1))

    factor_of = one(*split[0])
    for cut in split[1:]:
        factor_of = factor_of * one(*cut)
    return factor_of


def bell_draw(own_key, dims, scale, most, cuts=(), kind=jnp.bfloat16):
    result = scale * jax.random.normal(own_key, dims, jnp.float32)
    if cuts:
        result = result * block_scale(own_key, dims, cuts, -0.22, 0.18)
    return jnp.clip(result, -most, most).astype(kind)


def setup_inputs(seed: int = 0) -> dict:
    seeds = jax.random.split(jax.random.key(seed), 8)
    return {
        "noise_in": bell_draw(seeds[0], (TOKENS, D), 1.0, 6.0, ((0, 8), (1, 8))),
        "noise_renoise": bell_draw(seeds[1], (TOKENS, D), 1.0, 6.0, ((0, 8), (1, 8))),
        "text_cond": bell_draw(seeds[2], (IMAGES, D), 0.5, 3.0, ((0, 8),)),
        "t_index": touch_ends(jax.random.randint(seeds[3], (IMAGES,), 0, 1000), jax.random.fold_in(seeds[3], 1), 0, 999).astype(jnp.int32),
        "gains": jnp.clip(1.0 + 0.1 * jax.random.normal(seeds[4], (3, D), jnp.float32), 0.5, 1.5),
        "up_weights": bell_draw(seeds[5], (3, D, HID), D ** -0.5, 0.109375, ((1, 8), (2, 8))),
        "down_weights": bell_draw(seeds[6], (3, HID, D), HID ** -0.5, 0.0546875, ((1, 8), (2, 8))),
    }


def gelu_tanh(value):
    return jax.nn.gelu(value, approximate=True)

def front_pass(inputs, gain_row, cond_rows, up_matrix):
    values = inputs.astype(jnp.float32)
    factor = lax.rsqrt(lax.optimization_barrier(jnp.mean(values * values, axis=-1, keepdims=True)) + 1e-06)
    normed = (values * factor * gain_row[None, :] * (1.0 + cond_rows)).astype(jnp.bfloat16)
    hidden_pre = jnp.dot(normed, up_matrix, preferred_element_type=jnp.float32)
    hidden = gelu_tanh(hidden_pre).astype(jnp.bfloat16)
    return (normed, hidden_pre, hidden)

def block_pass(inputs, gain_row, cond_rows, up_matrix, down_matrix):
    normed, hidden_pre, hidden = front_pass(inputs, gain_row, cond_rows, up_matrix)
    output = (inputs.astype(jnp.float32) + jnp.dot(hidden, down_matrix, preferred_element_type=jnp.float32)).astype(jnp.bfloat16)
    return (output, normed, hidden_pre, hidden)

def backward(normed, hidden_pre, hidden, upstream, down_matrix):
    down_grad = jnp.dot(hidden.T, upstream, preferred_element_type=jnp.float32)
    hidden_grad = jnp.dot(upstream, down_matrix.T, preferred_element_type=jnp.float32)
    pre_grad = jax.vjp(gelu_tanh, hidden_pre)[1](hidden_grad)[0].astype(jnp.bfloat16)
    up_grad = jnp.dot(normed.T, pre_grad, preferred_element_type=jnp.float32)
    return (up_grad, down_grad)

def reference(noise_in, noise_renoise, text_cond, t_index, gains, up_weights, down_weights):
    cond_rows = jnp.repeat(text_cond.astype(jnp.float32), IMG_TOK, axis=0)
    generated, normed_s, pre_s, hidden_s = block_pass(noise_in, gains[0], cond_rows, up_weights[0], down_weights[0])
    sigma = 0.1 + 0.8 * t_index.astype(jnp.float32) / 999.0
    sigma_rows = jnp.repeat(sigma, IMG_TOK)[:, None]
    noised = ((1.0 - sigma_rows) * generated.astype(jnp.float32) + sigma_rows * noise_renoise.astype(jnp.float32)).astype(jnp.bfloat16)
    real_out = block_pass(noised, gains[1], cond_rows, up_weights[1], down_weights[1])[0]
    fake_out, normed_f, pre_f, hidden_f = block_pass(noised, gains[2], cond_rows, up_weights[2], down_weights[2])
    gen_f = generated.astype(jnp.float32)
    real_f = real_out.astype(jnp.float32)
    fake_f = fake_out.astype(jnp.float32)
    images = t_index.shape[0]
    image_norm = lax.optimization_barrier(jnp.mean(jnp.abs(gen_f - real_f).reshape(images, -1), axis=1)) + 1e-05
    push_scale = 1.0 / jnp.sqrt(jnp.float32(TOKENS))
    student_push = ((fake_f - real_f) / jnp.repeat(image_norm, IMG_TOK)[:, None] * push_scale).astype(jnp.bfloat16)
    fake_push = ((fake_f - gen_f) * push_scale).astype(jnp.bfloat16)
    position = jnp.arange(TOKENS, dtype=jnp.int32) % TOK_DEV
    first_half = (position < TOK_DEV // 2)[:, None]
    zeros_push = jnp.zeros_like(student_push)
    push_first = jnp.where(first_half, student_push, zeros_push)
    push_second = jnp.where(first_half, zeros_push, student_push)
    up_a, down_a = backward(normed_s, pre_s, hidden_s, push_first, down_weights[0])
    up_b, down_b = backward(normed_s, pre_s, hidden_s, push_second, down_weights[0])
    up_f, down_f = backward(normed_f, pre_f, hidden_f, fake_push, down_weights[2])
    up_grads = jnp.stack([up_a, up_b, jnp.zeros_like(up_f), up_f])
    down_grads = jnp.stack([down_a, down_b, jnp.zeros_like(down_f), down_f])
    return (generated, up_grads, down_grads)
```

```python
import functools
import math

import jax
import jax.numpy as jnp
from jax import lax
from jax.experimental import pallas as pl
from jax.experimental.pallas import tpu as pltpu
from jax.sharding import PartitionSpec as P

MESH = pl.DeviceIdType.MESH
BF = jnp.bfloat16
F32 = jnp.float32
FEAT = 384
HID = 1536
EXT = 128
ROW = FEAT + EXT
WIDE = EXT + HID
CHUNKS = 2
HC = HID // CHUNKS
BLOCKS = 8
HALF = 64
QUARTER = 32
IMG_TOK = 128
D_ALL = 3072
TOKENS = 1024
GELU_C = math.sqrt(2.0 / math.pi)


def split_scalar(value):
    high = value.astype(BF).astype(F32)
    low = value - high
    lane = lax.broadcasted_iota(jnp.int32, (value.shape[0], EXT), 1)
    return jnp.where(lane < EXT // 2, high, low)


def join_scalar(columns):
    return columns[:, 0:1] + columns[:, EXT // 2 : EXT // 2 + 1]


def gelu_both(a):
    a2 = a * a
    th = jnp.tanh(GELU_C * a * (1.0 + 0.044715 * a2))
    half = 0.5 * (1.0 + th)
    grad = half + 0.5 * a * (1.0 - th * th) * (GELU_C * (1.0 + 3.0 * 0.044715 * a2))
    return a * half, grad


def wide_cols(c):
    return (0, EXT + HC) if c == 0 else (EXT + c * HC, HC)


def kernel(
    msgx, msgr, gain, up_hbm, down_hbm,
    gen_out, upg_out, dng_out,
    xt, rt, gen, gout, fk, dmine, dother,
    upw, dnw, xgs, hs, xgf, hf, dyb, dab, gd,
    sb1, rb1, po1, zs1, zr1, ts1, tr1,
    sb2, rb2, po2, zs2, zr2, ts2, tr2,
    sb3, rb3, po3, zs3, zr3,
    wsem, tsend, trecv, gsend, grecv,
    ag_s, ag_r, ry_s, ry_r, rz_s, rz_r, hy_s, hz_s, h_r, tp_s, tp_r,
):
    g, r, t = lax.axis_index("grp"), lax.axis_index("rep"), lax.axis_index("tp")
    y, zh = lax.div(r, 2), lax.rem(r, 2)
    half, quart = lax.rem(g, 2), lax.div(g, 2)
    g_pair = lax.rem(g + 2, 4)
    g_near = g + 1 - 2 * half
    late = (g >= 2).astype(jnp.int32)
    qrow = pl.multiple_of(quart * QUARTER, QUARTER)
    sends = []

    def dev(gg=None, rr=None, tt=None):
        return (g if gg is None else gg, r if rr is None else rr, t if tt is None else tt)

    def remote(src, dst, ssem, rsem, to, start=True, when=None):
        cp = pltpu.make_async_remote_copy(
            src_ref=src, dst_ref=dst, send_sem=ssem, recv_sem=rsem, device_id=to, device_id_type=MESH
        )
        if when is None:
            cp.start()
        else:
            pl.when(when)(cp.start)
        sends.append((cp, when))
        return cp

    def wait_recv(dst, rsem, when=None):
        cp = pltpu.make_async_remote_copy(
            src_ref=dst, dst_ref=dst, send_sem=rsem, recv_sem=rsem, device_id=dev(), device_id_type=MESH
        )
        if when is None:
            cp.wait_recv()
        else:
            pl.when(when)(cp.wait_recv)

    model = 1 + late
    loads = [
        pltpu.make_async_copy(up_hbm.at[0], upw.at[0], wsem.at[0]),
        pltpu.make_async_copy(down_hbm.at[0], dnw.at[0], wsem.at[1]),
        pltpu.make_async_copy(up_hbm.at[model], upw.at[1], wsem.at[2]),
        pltpu.make_async_copy(down_hbm.at[model], dnw.at[1], wsem.at[3]),
    ]
    for cp in loads:
        cp.start()

    barrier = pltpu.get_barrier_semaphore()
    for k in range(1, 8):
        pl.semaphore_signal(barrier, inc=1, device_id=dev(tt=lax.rem(t + k, 8)), device_id_type=MESH)
    for j in range(1, 4):
        pl.semaphore_signal(
            barrier, inc=1, device_id=dev(rr=2 * lax.rem(y + j, 4) + zh), device_id_type=MESH
        )
    pl.semaphore_signal(barrier, inc=1, device_id=dev(rr=2 * y + 1 - zh), device_id_type=MESH)
    pl.semaphore_signal(barrier, inc=1, device_id=dev(gg=g_pair), device_id_type=MESH)
    pl.semaphore_signal(barrier, inc=1, device_id=dev(gg=g_near), device_id_type=MESH)

    @pl.when(r != t)
    def _():
        pl.semaphore_signal(barrier, inc=1, device_id=dev(rr=t, tt=r), device_id_type=MESH)
        pl.semaphore_wait(barrier, 14)

    @pl.when(r == t)
    def _():
        pl.semaphore_wait(barrier, 13)

    off_diag = r != t
    flip = dev(rr=t, tt=r)
    remote(msgx, xt, tsend.at[0], trecv.at[0], flip, when=off_diag)
    remote(msgr, rt, tsend.at[1], trecv.at[1], flip, when=off_diag)

    @pl.when(jnp.logical_not(off_diag))
    def _():
        xt[...] = msgx[...]
        rt[...] = msgr[...]

    wait_recv(xt, trecv.at[0], off_diag)
    cond1 = 1.0 + xt[QUARTER : QUARTER + 1, :].astype(F32)

    def gather_tp(phase, block_of):
        for k in range(1, 8):
            remote(block_of(t), block_of(t), ag_s.at[phase, k], ag_r.at[phase, t], dev(tt=lax.rem(t + k, 8)))

    def wait_block(phase, block_of, b):
        wait_recv(block_of(b), ag_r.at[phase, b], b != t)

    def reduce_rep(phase, n, rows_of, block_of, product, sb, rb, po, zs, zr, finish):
        waited = set()
        zmine = pl.multiple_of(zh * n, n)
        zpeer = pl.multiple_of((1 - zh) * n, n)
        for c in range(CHUNKS):
            start, width = wide_cols(c)
            for j in (2, 1, 3, 0):
                yy = lax.rem(y + j, 4)
                if j not in waited:
                    waited.add(j)
                    wait_block(phase, block_of, 2 * yy)
                    wait_block(phase, block_of, 2 * yy + 1)
                rows = rows_of(yy)
                part = product(rows[:, :FEAT], c)
                if j:
                    if c == 0:
                        sb[j - 1, :, :EXT] = rows[:, FEAT:]
                        sb[j - 1, :, EXT : EXT + HC] = part.astype(BF)
                    else:
                        sb[j - 1, :, start : start + width] = part.astype(BF)
                    cols = (j - 1, slice(None), pl.ds(start, width))
                    remote(
                        sb.at[cols], rb.at[cols], ry_s.at[phase, c, j], ry_r.at[phase, c, j],
                        dev(rr=2 * yy + zh),
                    )
                else:
                    if c == 0:
                        po[:, :EXT] = rows[:, FEAT:].astype(F32)
                        po[:, EXT : EXT + HC] = part
                    else:
                        po[:, start : start + width] = part
        peer = dev(rr=2 * y + 1 - zh)
        for c in range(CHUNKS):
            start, width = wide_cols(c)
            for j in (1, 3, 2):
                wait_recv(rb.at[j - 1, :, pl.ds(start, width)], ry_r.at[phase, c, j])

            def summed(row, lo, wid):
                total = po[pl.ds(row, n), lo : lo + wid]
                for j in range(3):
                    total += rb[j, pl.ds(row, n), lo : lo + wid].astype(F32)
                return total

            if c == 0:
                zs[:, :EXT] = split_scalar(join_scalar(summed(zpeer, 0, EXT))).astype(BF)
            lo = EXT + c * HC
            zs[:, lo : lo + HC] = summed(zpeer, lo, HC).astype(BF)
            remote(
                zs.at[:, pl.ds(start, width)], zr.at[:, pl.ds(start, width)],
                rz_s.at[phase, c], rz_r.at[phase, c], peer,
            )
        row_scalar = None
        for c in range(CHUNKS):
            start, width = wide_cols(c)
            wait_recv(zr.at[:, pl.ds(start, width)], rz_r.at[phase, c])

            def summed(lo, wid):
                total = po[pl.ds(zmine, n), lo : lo + wid] + zr[:, lo : lo + wid].astype(F32)
                for j in range(3):
                    total += rb[j, pl.ds(zmine, n), lo : lo + wid].astype(F32)
                return total

            if c == 0:
                row_scalar = join_scalar(summed(0, EXT))
            finish(c, summed(EXT + c * HC, HC), row_scalar)

    def gather_rep_own(phase, c, piece):
        remote(piece(r), piece(r), hz_s.at[phase, c], h_r.at[phase, c, r], dev(rr=2 * y + 1 - zh))
        for j in (2, 1, 3):
            yy = lax.rem(y + j, 4)
            remote(piece(r), piece(r), hy_s.at[phase, c, 0, j], h_r.at[phase, c, r], dev(rr=2 * yy + zh))

    def gather_rep_pass(phase, c, piece):
        b = 2 * y + 1 - zh
        wait_recv(piece(b), h_r.at[phase, c, b])
        for j in (2, 1, 3):
            yy = lax.rem(y + j, 4)
            remote(piece(b), piece(b), hy_s.at[phase, c, 1, j], h_r.at[phase, c, b], dev(rr=2 * yy + zh))

    def wait_rep(phase, c, piece, b):
        wait_recv(piece(b), h_r.at[phase, c, b])

    def forward(phase, n, x_rows, gain_row, xg, xg_rows, h, h_rows, up, down, grad, sb, rb, po, zs, zr, ts, tr):
        xg[t, xg_rows, :FEAT] = (x_rows * (gain_row * cond1)).astype(BF)
        xg[t, xg_rows, FEAT:] = split_scalar(jnp.sum(x_rows * x_rows, axis=1, keepdims=True)).astype(BF)
        block_of = lambda b: xg.at[b, xg_rows, :]
        gather_tp(phase, block_of)
        rows_of = lambda yy: xg[pl.ds(2 * yy, 2), xg_rows, :].reshape(2 * n, ROW)
        loads[2 * phase].wait()

        def product(rows, c):
            return jnp.dot(rows, up[:, c * HC : (c + 1) * HC], preferred_element_type=F32)

        def piece_of(c):
            return lambda b: h.at[b, h_rows, pl.ds(c * HC, HC)]

        def finish(c, a, square_sum):
            factor = lax.rsqrt(square_sum * (1.0 / D_ALL) + 1e-6)
            hidden, slope = gelu_both(a * factor)
            h[r, h_rows, c * HC : (c + 1) * HC] = hidden.astype(BF)
            grad[h_rows, c * HC : (c + 1) * HC] = (slope * factor).astype(BF)
            gather_rep_own(phase, c, piece_of(c))

        reduce_rep(phase, n, rows_of, block_of, product, sb, rb, po, zs, zr, finish)
        for c in range(CHUNKS):
            gather_rep_pass(phase, c, piece_of(c))
        loads[2 * phase + 1].wait()
        for j in (0, 1, 3, 2):
            yy = lax.rem(y + j, 4)
            if j:
                for c in range(CHUNKS):
                    wait_rep(phase, c, piece_of(c), 2 * yy + zh)
                    wait_rep(phase, c, piece_of(c), 2 * yy + 1 - zh)
            both = h[pl.ds(2 * yy, 2), h_rows, :].reshape(2 * n, HID)
            part = jnp.dot(both, down[...], preferred_element_type=F32)
            ts[pl.ds(2 * yy, 2)] = part.astype(BF).reshape(2, n, FEAT)
            for k in range(2):
                b = 2 * yy + k
                remote(ts.at[b], tr.at[t], tp_s.at[phase, b], tp_r.at[phase, t], dev(tt=b), when=b != t)
        total = ts[t].astype(F32)
        for k in range(1, 8):
            b = lax.rem(t + k, 8)
            wait_recv(tr.at[b], tp_r.at[phase, b])
            total += tr[b].astype(F32)
        return total

    x0 = xt[:QUARTER, :].astype(F32)
    q_rows = pl.ds(qrow, QUARTER)
    out = forward(
        0, QUARTER, x0, gain[0:1, :], xgs, q_rows, hs, q_rows, upw.at[0], dnw.at[0], gd.at[0],
        sb1, rb1, po1, zs1, zr1, ts1, tr1,
    )
    own = pl.ds(pl.multiple_of(half * HALF + quart * QUARTER, QUARTER), QUARTER)
    pair = pl.ds(pl.multiple_of(half * HALF + (1 - quart) * QUARTER, QUARTER), QUARTER)
    mine = pl.ds(pl.multiple_of(half * HALF, HALF), HALF)
    other = pl.ds(pl.multiple_of((1 - half) * HALF, HALF), HALF)
    gen[own, :] = (x0 + out).astype(BF)
    remote(gen.at[own, :], gen.at[own, :], gsend.at[0], grecv.at[0], dev(gg=g_pair))
    is_late = g >= 2
    is_early = g < 2
    for i, ref in enumerate((xgs.at[:, q_rows, :], hs.at[:, q_rows, :], gd.at[0, q_rows, :])):
        remote(ref, ref, gsend.at[1 + i], grecv.at[1 + i], dev(gg=g_pair), when=is_late)
    wait_recv(gen.at[pair, :], grecv.at[0])
    remote(gen.at[mine, :], gen.at[mine, :], gsend.at[4], grecv.at[4], dev(gg=g_near))

    wait_recv(rt, trecv.at[1], off_diag)
    t_row = xt[QUARTER + 8 : QUARTER + 9, :].astype(F32)
    t_value = t_row[:, 0:1] * 256.0 + t_row[:, EXT : EXT + 1]
    sigma = 0.1 + 0.8 * t_value / 999.0
    gen_f = gen[mine, :].astype(F32)
    x_t = ((1.0 - sigma) * gen_f + sigma * rt[...].astype(F32)).astype(BF).astype(F32)
    all_rows = pl.ds(0, HALF)
    out = forward(
        1, HALF, x_t, gain[pl.ds(model, 1), :], xgf.at[half], all_rows, hf.at[half], all_rows,
        upw.at[1], dnw.at[1], gd.at[1], sb2, rb2, po2, zs2, zr2, ts2, tr2,
    )
    pred = (x_t + out).astype(BF)
    is_2, is_3 = g == 2, g == 3
    for i, ref in enumerate((xgf.at[0], hf.at[0])):
        remote(ref, ref, gsend.at[5 + i], grecv.at[5 + i], dev(gg=g_near), when=is_2)

    wait_recv(gen.at[other, :], grecv.at[4])
    remote(gen, gout, tsend.at[2], trecv.at[2], flip, when=off_diag)

    scale = 1.0 / math.sqrt(TOKENS)
    fk[...] = pred

    def to_pair():
        pltpu.make_async_remote_copy(
            src_ref=fk, dst_ref=dother.at[0], send_sem=gsend.at[7], recv_sem=grecv.at[7],
            device_id=dev(gg=g_pair), device_id_type=MESH,
        ).start()

    pl.when(is_late)(to_pair)
    dy = dyb.at[half]

    @pl.when(is_late)
    def _():
        dy[t, :, :FEAT] = ((fk[...].astype(F32) - gen_f) * scale).astype(BF)
        dy[t, :, FEAT:] = jnp.zeros((HALF, EXT), BF)

    @pl.when(is_early)
    def _():
        real = fk[...].astype(F32)
        distance = jnp.sum(jnp.sum(jnp.abs(gen_f - real), axis=1, keepdims=True), axis=0, keepdims=True)
        dmine[0] = jnp.broadcast_to(distance, (8, EXT))
        cp = pltpu.make_async_remote_copy(
            src_ref=dmine.at[0], dst_ref=dmine.at[1], send_sem=gsend.at[8], recv_sem=grecv.at[8],
            device_id=dev(gg=g_near), device_id_type=MESH,
        )
        cp.start()
        wait_recv(dother.at[0], grecv.at[7])
        fake = dother[0].astype(F32)
        dy[t, :, :FEAT] = ((fake - real) * scale).astype(BF)
        cp.wait()
        both = jnp.broadcast_to(dmine[0, 0:1, 0:1] + dmine[1, 0:1, 0:1], (HALF, 1))
        dy[t, :, FEAT:] = split_scalar(both).astype(BF)

    dy_block = lambda b: dy.at[b]
    gather_tp(2, dy_block)
    da = dab.at[half]
    back = dnw.at[late]
    slope = gd.at[late]

    def product(rows, c):
        return lax.dot_general(
            rows, back[c * HC : (c + 1) * HC, :], (((1,), (1,)), ((), ())), preferred_element_type=F32
        )

    def da_piece(c):
        start, width = wide_cols(c)
        return lambda b: da.at[b, :, pl.ds(start, width)]

    wait_recv(gd.at[0, pl.ds(QUARTER, QUARTER), :], grecv.at[3], is_early)

    def finish(c, dh, distance):
        norm = distance * (1.0 / (IMG_TOK * D_ALL)) + 1e-5
        row_scale = jnp.where(is_late, 1.0, 1.0 / norm)
        lo = EXT + c * HC
        if c == 0:
            da[r, :, :EXT] = split_scalar(row_scale).astype(BF)
        da[r, :, lo : lo + HC] = (dh * row_scale * slope[:, c * HC : (c + 1) * HC].astype(F32)).astype(BF)
        gather_rep_own(2, c, da_piece(c))

    reduce_rep(
        2, HALF, lambda yy: dy[pl.ds(2 * yy, 2)].reshape(2 * HALF, ROW), dy_block, product,
        sb3, rb3, po3, zs3, zr3, finish,
    )
    remote(dyb.at[0], dyb.at[0], gsend.at[9], grecv.at[9], dev(gg=g_near), when=is_2)
    for c in range(CHUNKS):
        gather_rep_pass(2, c, da_piece(c))
    relay = lambda b: remote(dab.at[0, b], dab.at[0, b], gsend.at[10 + b], grecv.at[10 + b], dev(gg=g_near), when=is_2)
    relay(r)
    relay(2 * y + 1 - zh)
    for j in (1, 3, 2):
        yy = lax.rem(y + j, 4)
        for b in (2 * yy + zh, 2 * yy + 1 - zh):
            for c in range(CHUNKS):
                wait_rep(2, c, da_piece(c), b)
            relay(b)

    for i, ref in enumerate((xgs.at[:, pl.ds(QUARTER, QUARTER), :], hs.at[:, pl.ds(QUARTER, QUARTER), :])):
        wait_recv(ref, grecv.at[1 + i], is_early)
    for i, ref in enumerate((xgf.at[0], hf.at[0])):
        wait_recv(ref, grecv.at[5 + i], is_3)
    wait_recv(dyb.at[0], grecv.at[9], is_3)
    for b in range(BLOCKS):
        wait_recv(dab.at[0, b], grecv.at[10 + b], is_3)

    tn = (((0,), (0,)), ((), ()))
    step = 256

    def weight_grads(tokens, u_of, da_of, h_of, dy_of):
        def up_tile(i, _):
            cols = pl.ds(pl.multiple_of(i * step, step), step)
            wide = pl.ds(pl.multiple_of(EXT + i * step, EXT), step)
            upg_out[0, :, cols] = lax.dot_general(u_of(), da_of(wide), tn, preferred_element_type=F32)
            return 0

        lax.fori_loop(0, HID // step, up_tile, 0)
        row_scale = join_scalar(da_of(slice(0, EXT)).astype(F32))
        upstream = (dy_of().astype(F32) * row_scale).astype(BF)

        def down_tile(i, _):
            cols = pl.ds(pl.multiple_of(i * step, step), step)
            dng_out[0, cols, :] = lax.dot_general(h_of(cols), upstream, tn, preferred_element_type=F32)
            return 0

        lax.fori_loop(0, HID // step, down_tile, 0)

    @pl.when(is_early)
    def _():
        n = BLOCKS * HALF
        weight_grads(
            n,
            lambda: xgs[:, :, :FEAT].reshape(n, FEAT),
            lambda cols: da[:, :, cols].reshape(n, -1),
            lambda cols: hs[:, :, cols].reshape(n, -1),
            lambda: dy[:, :, :FEAT].reshape(n, FEAT),
        )

    @pl.when(is_2)
    def _():
        upg_out[...] = jnp.zeros_like(upg_out)
        dng_out[...] = jnp.zeros_like(dng_out)

    @pl.when(is_3)
    def _():
        n = 2 * BLOCKS * HALF
        weight_grads(
            n,
            lambda: xgf[:, :, :, :FEAT].reshape(n, FEAT),
            lambda cols: dab[:, :, :, cols].reshape(n, -1),
            lambda cols: hf[:, :, :, cols].reshape(n, -1),
            lambda: dyb[:, :, :, :FEAT].reshape(n, FEAT),
        )

    wait_recv(gout, trecv.at[2], off_diag)

    @pl.when(off_diag)
    def _():
        gen_out[...] = gout[...]

    @pl.when(jnp.logical_not(off_diag))
    def _():
        gen_out[...] = gen[...]

    for cp, when in sends:
        if when is None:
            cp.wait_send()
        else:
            pl.when(when)(cp.wait_send)

    @pl.when(is_late)
    def _():
        pltpu.make_async_remote_copy(
            src_ref=fk, dst_ref=dother.at[0], send_sem=gsend.at[7], recv_sem=grecv.at[7],
            device_id=dev(gg=g_pair), device_id_type=MESH,
        ).wait_send()


def rep_buffers(n):
    return [
        pltpu.VMEM((3, 2 * n, WIDE), BF),
        pltpu.VMEM((3, 2 * n, WIDE), BF),
        pltpu.VMEM((2 * n, WIDE), F32),
        pltpu.VMEM((n, WIDE), BF),
        pltpu.VMEM((n, WIDE), BF),
    ]


def body(noise_in, noise_renoise, text_cond, t_index, gains, up_weights, down_weights):
    g, r, t = lax.axis_index("grp"), lax.axis_index("rep"), lax.axis_index("tp")
    half, quart = g % 2, g // 2
    x_part = lax.dynamic_slice_in_dim(noise_in, half * HALF + quart * QUARTER, QUARTER, 0)
    r_part = lax.dynamic_slice_in_dim(noise_renoise, half * HALF, HALF, 0)
    cond = lax.dynamic_slice_in_dim(text_cond, t * FEAT, FEAT, 1)
    t_all = t_index.astype(F32)
    t_high = jnp.floor(t_all * (1.0 / 256.0))
    t_low = t_all - 256.0 * t_high
    lane = lax.broadcasted_iota(jnp.int32, (8, FEAT), 1)
    t_rows = jnp.where(lane < EXT, t_high, t_low).astype(BF)
    msgx = jnp.concatenate([x_part, jnp.broadcast_to(cond, (8, FEAT)), t_rows], axis=0)
    gain = jnp.pad(lax.dynamic_slice_in_dim(gains, r * FEAT, FEAT, 1), ((0, 5), (0, 0)))
    vmem = pl.BlockSpec(memory_space=pltpu.VMEM)
    hbm = pl.BlockSpec(memory_space=pl.ANY)
    dma = pltpu.SemaphoreType.DMA
    tp_buffers = lambda n: [pltpu.VMEM((BLOCKS, n, FEAT), BF)] * 2
    out = pl.pallas_call(
        kernel,
        name="step",
        out_shape=(
            jax.ShapeDtypeStruct((IMG_TOK, FEAT), BF),
            jax.ShapeDtypeStruct((1, FEAT, HID), F32),
            jax.ShapeDtypeStruct((1, HID, FEAT), F32),
        ),
        in_specs=[vmem, vmem, vmem, hbm, hbm],
        out_specs=(vmem, vmem, vmem),
        scratch_shapes=[
            pltpu.VMEM((QUARTER + 16, FEAT), BF),
            pltpu.VMEM((HALF, FEAT), BF),
            pltpu.VMEM((IMG_TOK, FEAT), BF),
            pltpu.VMEM((IMG_TOK, FEAT), BF),
            pltpu.VMEM((HALF, FEAT), BF),
            pltpu.VMEM((2, 8, EXT), F32),
            pltpu.VMEM((1, HALF, FEAT), BF),
            pltpu.VMEM((2, FEAT, HID), BF),
            pltpu.VMEM((2, HID, FEAT), BF),
            pltpu.VMEM((BLOCKS, HALF, ROW), BF),
            pltpu.VMEM((BLOCKS, HALF, HID), BF),
            pltpu.VMEM((2, BLOCKS, HALF, ROW), BF),
            pltpu.VMEM((2, BLOCKS, HALF, HID), BF),
            pltpu.VMEM((2, BLOCKS, HALF, ROW), BF),
            pltpu.VMEM((2, BLOCKS, HALF, WIDE), BF),
            pltpu.VMEM((2, HALF, HID), BF),
            *rep_buffers(QUARTER),
            *tp_buffers(QUARTER),
            *rep_buffers(HALF),
            *tp_buffers(HALF),
            *rep_buffers(HALF),
            dma((4,)),
            dma((3,)),
            dma((3,)),
            dma((18,)),
            dma((18,)),
            dma((3, 8)),
            dma((3, 8)),
            dma((3, CHUNKS, 4)),
            dma((3, CHUNKS, 4)),
            dma((3, CHUNKS)),
            dma((3, CHUNKS)),
            dma((3, CHUNKS, 2, 4)),
            dma((3, CHUNKS)),
            dma((3, CHUNKS, 8)),
            dma((2, 8)),
            dma((2, 8)),
        ],
        compiler_params=pltpu.CompilerParams(
            collective_id=0, has_side_effects=True, vmem_limit_bytes=60 * 2**20
        ),
    )(msgx, r_part, gain, up_weights, down_weights)
    return out


def solution(mesh):
    in_specs = (
        P("rep", "tp"),
        P("rep", "tp"),
        P("rep", None),
        P("rep"),
        P(),
        P(None, "rep", "tp"),
        P(None, "tp", "rep"),
    )
    out_specs = (P("rep", "tp"), P("grp", "rep", "tp"), P("grp", "tp", "rep"))
    return jax.shard_map(body, mesh=mesh, in_specs=in_specs, out_specs=out_specs, check_vma=False)
```

```python
import functools
import math

import jax
import jax.numpy as jnp
from jax import lax
from jax.experimental import pallas as pl
from jax.experimental.pallas import tpu as pltpu
from jax.sharding import PartitionSpec as P

MESH = pl.DeviceIdType.MESH
BF = jnp.bfloat16
F32 = jnp.float32
FEAT = 384
HID = 1536
EXT = 128
ROW = FEAT + EXT
WIDE = EXT + HID
CHUNKS = 4
HC = HID // CHUNKS
BLOCKS = 8
HALF = 64
QUARTER = 32
IMG_TOK = 128
D_ALL = 3072
TOKENS = 1024
GELU_C = math.sqrt(2.0 / math.pi)


def split_scalar(value):
    high = value.astype(BF).astype(F32)
    low = value - high
    lane = lax.broadcasted_iota(jnp.int32, (value.shape[0], EXT), 1)
    return jnp.where(lane < EXT // 2, high, low)


def join_scalar(columns):
    return columns[:, 0:1] + columns[:, EXT // 2 : EXT // 2 + 1]


def gelu_both(a):
    a2 = a * a
    th = jnp.tanh(GELU_C * a * (1.0 + 0.044715 * a2))
    half = 0.5 * (1.0 + th)
    grad = half + 0.5 * a * (1.0 - th * th) * (GELU_C * (1.0 + 3.0 * 0.044715 * a2))
    return a * half, grad


def wide_cols(c):
    return (0, EXT + HC) if c == 0 else (EXT + c * HC, HC)


def kernel(
    noise, renoise, cond_in, t_in, gains, up_hbm, down_hbm,
    gen_out, upg_out, dng_out,
    msgc, xt, ct, rt, gen, gout, fk, fother, dmine,
    upw, dnw, xgs, hs, xgf, hf, dyb, dab, gd,
    sb1, rb1, po1, zs1, zr1, acc1, ta1, tb1, tc1, td1,
    sb2, rb2, po2, zs2, zr2, acc2, ta2, tb2, tc2, td2,
    sb3, rb3, po3, zs3, zr3,
    wsem, tsend, trecv, gsend, grecv,
    ag_s, ag_r, ry_s, ry_r, rz_s, rz_r, hy_s, h_r, tp_s, tp_r, xs_s, xs_r,
):
    g, r, t = lax.axis_index("grp"), lax.axis_index("rep"), lax.axis_index("tp")
    y, zh = lax.div(r, 2), lax.rem(r, 2)
    zl, core = lax.div(t, 2), lax.rem(t, 2)
    is_late, is_early = g >= 2, g < 2
    is_2, is_3 = g == 2, g == 3
    late = is_late.astype(jnp.int32)
    quart = late
    low = lax.rem(g, 2)
    half = low + late - 2 * low * late
    g_pair = 3 - g
    g_near = g + 1 - 2 * low
    qrow = pl.multiple_of(quart * QUARTER, QUARTER)
    sends = []

    def dev(gg=None, rr=None, tt=None):
        return (g if gg is None else gg, r if rr is None else rr, t if tt is None else tt)

    def remote(src, dst, ssem, rsem, to, when=None):
        cp = pltpu.make_async_remote_copy(
            src_ref=src, dst_ref=dst, send_sem=ssem, recv_sem=rsem, device_id=to, device_id_type=MESH
        )
        if when is None:
            cp.start()
        else:
            pl.when(when)(cp.start)
        sends.append((cp, when))
        return cp

    def wait_recv(dst, rsem, when=None):
        cp = pltpu.make_async_remote_copy(
            src_ref=dst, dst_ref=dst, send_sem=rsem, recv_sem=rsem, device_id=dev(), device_id_type=MESH
        )
        if when is None:
            cp.wait_recv()
        else:
            pl.when(when)(cp.wait_recv)

    model = 1 + late
    loads = [
        pltpu.make_async_copy(up_hbm.at[0], upw.at[0], wsem.at[0]),
        pltpu.make_async_copy(down_hbm.at[0], dnw.at[0], wsem.at[1]),
        pltpu.make_async_copy(up_hbm.at[model], upw.at[1], wsem.at[2]),
        pltpu.make_async_copy(down_hbm.at[model], dnw.at[1], wsem.at[3]),
    ]
    for cp in loads:
        cp.start()

    barrier = pltpu.get_barrier_semaphore()
    sibling = dev(tt=2 * zl + 1 - core)
    flip = dev(rr=t, tt=r)
    off_diag = r != t
    row_peer = lambda yy: dev(rr=2 * yy + zh)
    z_peer = dev(rr=2 * y + 1 - zh)
    peers = [sibling, z_peer, dev(gg=g_pair), dev(gg=g_near)]
    peers += [dev(tt=2 * lax.rem(zl + d, 4) + core) for d in range(1, 4)]
    peers += [row_peer(lax.rem(y + j, 4)) for j in range(1, 4)]
    for peer in peers:
        pl.semaphore_signal(barrier, inc=1, device_id=peer, device_id_type=MESH)

    cond_row = cond_in[0:1, pl.ds(pl.multiple_of(t * FEAT, EXT), FEAT)].astype(F32)
    t_all = jnp.full((16, FEAT), t_in[0], jnp.int32)
    row = lax.broadcasted_iota(jnp.int32, (16, FEAT), 0)
    lane = lax.broadcasted_iota(jnp.int32, (16, FEAT), 1)
    t_part = jnp.where(lane < EXT, t_all >> 8, t_all & 255).astype(F32)
    msgc[...] = jnp.where(row < 8, jnp.broadcast_to(cond_row, (16, FEAT)), t_part).astype(BF)

    @pl.when(off_diag)
    def _():
        pl.semaphore_signal(barrier, inc=1, device_id=flip, device_id_type=MESH)
        pl.semaphore_wait(barrier, len(peers) + 1)

    @pl.when(jnp.logical_not(off_diag))
    def _():
        pl.semaphore_wait(barrier, len(peers))

    own = pl.ds(pl.multiple_of(half * HALF + quart * QUARTER, QUARTER), QUARTER)
    pair = pl.ds(pl.multiple_of(half * HALF + (1 - quart) * QUARTER, QUARTER), QUARTER)
    mine = pl.ds(pl.multiple_of(half * HALF, HALF), HALF)
    other = pl.ds(pl.multiple_of((1 - half) * HALF, HALF), HALF)
    remote(noise.at[own, :], xt, tsend.at[0], trecv.at[0], flip, when=off_diag)
    remote(msgc, ct, tsend.at[1], trecv.at[1], flip, when=off_diag)
    remote(renoise.at[mine, :], rt, tsend.at[2], trecv.at[2], flip, when=off_diag)

    @pl.when(jnp.logical_not(off_diag))
    def _():
        xt[...] = noise[own, :]
        ct[...] = msgc[...]
        rt[...] = renoise[mine, :]

    wait_recv(xt, trecv.at[0], off_diag)
    wait_recv(ct, trecv.at[1], off_diag)
    cond1 = 1.0 + ct[0:1, :].astype(F32)

    def gather_tp(phase, block_of):
        remote(block_of(t), block_of(t), ag_s.at[phase, 0], ag_r.at[phase, t], sibling)
        for d in (2, 1, 3):
            to = dev(tt=2 * lax.rem(zl + d, 4) + core)
            remote(block_of(t), block_of(t), ag_s.at[phase, d], ag_r.at[phase, t], to)

    def wait_chip(phase, block_of, d):
        yy = lax.rem(zl + d, 4)
        if d:
            b = 2 * yy + core
            wait_recv(block_of(b), ag_r.at[phase, b])
            remote(block_of(b), block_of(b), ag_s.at[phase, 3 + d], ag_r.at[phase, b], sibling)
        b = 2 * yy + 1 - core
        wait_recv(block_of(b), ag_r.at[phase, b])

    def reduce_rep(phase, n, rows_of, block_of, product, bufs, finish, gathered):
        sb, rb, po, zs, zr = bufs
        for c in range(CHUNKS):
            start, width = wide_cols(c)
            lo = EXT + c * HC
            for d in (0, 1, 3, 2):
                yy = lax.rem(zl + d, 4)
                if c == 0:
                    wait_chip(phase, block_of, d)
                rows = rows_of(yy)
                part = product(rows[:, :FEAT], c)

                @pl.when(yy == y)
                def _():
                    if c == 0:
                        po[:, :EXT] = rows[:, FEAT:].astype(F32)
                    po[:, lo : lo + HC] = part

                @pl.when(yy != y)
                def _():
                    if c == 0:
                        sb[yy, :, :EXT] = rows[:, FEAT:]
                    sb[yy, :, lo : lo + HC] = part.astype(BF)

                cols = pl.ds(start, width)
                remote(
                    sb.at[yy, :, cols], rb.at[y, :, cols], ry_s.at[phase, c, d], ry_r.at[phase, c, y],
                    row_peer(yy), when=yy != y,
                )
            if c == 0:
                gathered()

        def to_z(c):
            start, width = wide_cols(c)
            others = [lax.rem(y + j, 4) for j in (1, 3, 2)]
            for yy in others:
                wait_recv(rb.at[yy, :, pl.ds(start, width)], ry_r.at[phase, c, yy])

            def add_up(lo, wid):
                total = po[:, lo : lo + wid]
                for yy in others:
                    total += rb[yy, :, lo : lo + wid].astype(F32)
                po[:, lo : lo + wid] = total
                return total

            if c == 0:
                zs[:, :EXT] = split_scalar(join_scalar(add_up(0, EXT))).astype(BF)
            lo = EXT + c * HC
            zs[:, lo : lo + HC] = add_up(lo, HC).astype(BF)
            cols = pl.ds(start, width)
            remote(zs.at[:, cols], zr.at[:, cols], rz_s.at[phase, c], rz_r.at[phase, c], z_peer)

        state = {}

        def from_z(c):
            start, width = wide_cols(c)
            wait_recv(zr.at[:, pl.ds(start, width)], rz_r.at[phase, c])
            if c == 0:
                state["scalar"] = join_scalar(po[:, :EXT] + zr[:, :EXT].astype(F32))
            lo = EXT + c * HC
            finish(c, po[:, lo : lo + HC] + zr[:, lo : lo + HC].astype(F32), state["scalar"])

        ahead = CHUNKS - 1 if n == HALF else CHUNKS
        for c in range(CHUNKS):
            if c == ahead:
                from_z(0)
            to_z(c)
        for c in range(1 if ahead < CHUNKS else 0, CHUNKS):
            from_z(c)

    def forward(phase, n, x_rows, gain_row, xg, xg_rows, h, h_rows, bufs, gathered, chunk_here):
        acc, ta, tb, tc, td = bufs[5:]
        up, down, grad = upw.at[phase], dnw.at[phase], gd.at[phase]
        xg[t, xg_rows, :FEAT] = (x_rows * (gain_row * cond1)).astype(BF)
        xg[t, xg_rows, FEAT:] = split_scalar(jnp.sum(x_rows * x_rows, axis=1, keepdims=True)).astype(BF)
        block_of = lambda b: xg.at[b, xg_rows, :]
        gather_tp(phase, block_of)
        rows_of = lambda yy: xg[pl.ds(2 * yy, 2), xg_rows, :].reshape(2 * n, ROW)
        loads[2 * phase].wait()

        def product(rows, c):
            return jnp.dot(rows, up[:, c * HC : (c + 1) * HC], preferred_element_type=F32)

        piece = lambda yy, c: h.at[pl.ds(2 * yy, 2), h_rows, pl.ds(c * HC, HC)]

        def finish(c, a, square_sum):
            factor = lax.rsqrt(square_sum * (1.0 / D_ALL) + 1e-6)
            hidden, slope = gelu_both(a * factor)
            cols = slice(c * HC, (c + 1) * HC)
            h[pl.ds(2 * y, 2), h_rows, cols] = hidden.astype(BF).reshape(2, n, HC)
            for j in (2, 1, 3):
                remote(
                    piece(y, c), piece(y, c), hy_s.at[phase, c, j], h_r.at[phase, c, y],
                    row_peer(lax.rem(y + j, 4)),
                )
            grad[:, h_rows, cols] = (slope * factor).astype(BF).reshape(2, n, HC)

        reduce_rep(phase, n, rows_of, block_of, product, bufs[:5], finish, gathered)
        loads[2 * phase + 1].wait()
        for c in range(CHUNKS):
            cols = slice(c * HC, (c + 1) * HC)
            for j in (0, 1, 3, 2):
                yy = lax.rem(y + j, 4)
                if j:
                    wait_recv(piece(yy, c), h_r.at[phase, c, yy])
                both = h[pl.ds(2 * yy, 2), h_rows, cols].reshape(2 * n, HC)
                part = jnp.dot(both, down[cols, :], preferred_element_type=F32).reshape(2, n, FEAT)
                if c:
                    acc[pl.ds(2 * yy, 2)] += part
                else:
                    acc[pl.ds(2 * yy, 2)] = part
            chunk_here(c)
        for d in (2, 1, 3, 0):
            yy = lax.rem(zl + d, 4)
            ta[d] = acc[2 * yy + 1 - core].astype(BF)
            remote(ta.at[d], tb.at[d], tp_s.at[phase, d], tp_r.at[phase, d], sibling)
        total = None
        for d in (2, 1, 3, 0):
            yy = lax.rem(zl + d, 4)
            wait_recv(tb.at[d], tp_r.at[phase, d])
            both = acc[2 * yy + core] + tb[d].astype(F32)
            if d:
                tc[d - 1] = both.astype(BF)
                remote(
                    tc.at[d - 1], td.at[d - 1], tp_s.at[phase, 3 + d], tp_r.at[phase, 3 + d],
                    dev(tt=2 * yy + core),
                )
            else:
                total = both
        for d in (1, 3, 2):
            wait_recv(td.at[d - 1], tp_r.at[phase, 3 + d])
            total += td[d - 1].astype(F32)
        return total

    gain = gains[:, pl.ds(pl.multiple_of(r * FEAT, EXT), FEAT)]
    x0 = xt[...].astype(F32)
    q_rows = pl.ds(qrow, QUARTER)
    out = forward(
        0, QUARTER, x0, gain[0:1, :], xgs, q_rows, hs, q_rows,
        (sb1, rb1, po1, zs1, zr1, acc1, ta1, tb1, tc1, td1), lambda: None, lambda c: None,
    )
    gen[own, :] = (x0 + out).astype(BF)
    remote(gen.at[own, :], gen.at[own, :], gsend.at[0], grecv.at[0], dev(gg=g_pair))
    for i, ref in enumerate((gd.at[0, :, q_rows, :], xgs.at[:, q_rows, :], hs.at[:, q_rows, :])):
        remote(ref, ref, gsend.at[1 + i], grecv.at[1 + i], dev(gg=g_pair), when=is_late)
    wait_recv(rt, trecv.at[2], off_diag)
    t_row = ct[8:9, :].astype(F32)
    sigma = 0.1 + 0.8 * (t_row[:, 0:1] * 256.0 + t_row[:, EXT : EXT + 1]) / 999.0
    wait_recv(gen.at[pair, :], grecv.at[0])
    remote(gen.at[mine, :], gen.at[mine, :], gsend.at[4], grecv.at[4], dev(gg=g_near))

    gen_f = gen[mine, :].astype(F32)
    x_t = ((1.0 - sigma) * gen_f + sigma * rt[...].astype(F32)).astype(BF).astype(F32)
    all_rows = pl.ds(0, HALF)
    xgf_2 = xgf.at[1, :, :, pl.ds(0, FEAT)]
    hf_2 = lambda c: hf.at[1, :, :, pl.ds(c * HC, HC)]
    near = dev(gg=g_near)
    gain_row = jnp.where(is_late, gain[2:3, :], gain[1:2, :])
    out = forward(
        1, HALF, x_t, gain_row, xgf.at[half], all_rows, hf.at[half], all_rows,
        (sb2, rb2, po2, zs2, zr2, acc2, ta2, tb2, tc2, td2),
        lambda: remote(xgf_2, xgf_2, gsend.at[5], grecv.at[5], near, when=is_2),
        lambda c: remote(hf_2(c), hf_2(c), gsend.at[10 + c], grecv.at[10 + c], near, when=is_2),
    )
    fk[...] = (x_t + out).astype(BF)
    remote(fk, fother, gsend.at[6], grecv.at[6], dev(gg=g_pair), when=is_late)

    scale = 1.0 / math.sqrt(TOKENS)
    dy = dyb.at[half]

    @pl.when(is_late)
    def _():
        dy[t, :, :FEAT] = ((fk[...].astype(F32) - gen_f) * scale).astype(BF)
        dy[t, :, FEAT:] = jnp.zeros((HALF, EXT), BF)

    @pl.when(is_early)
    def _():
        real = fk[...].astype(F32)
        distance = jnp.sum(jnp.sum(jnp.abs(gen_f - real), axis=1, keepdims=True), axis=0, keepdims=True)
        dmine[0] = jnp.broadcast_to(distance, (8, EXT))
        cp = pltpu.make_async_remote_copy(
            src_ref=dmine.at[0], dst_ref=dmine.at[1], send_sem=gsend.at[7], recv_sem=grecv.at[7],
            device_id=near, device_id_type=MESH,
        )
        cp.start()
        wait_recv(fother, grecv.at[6])
        dy[t, :, :FEAT] = ((fother[...].astype(F32) - real) * scale).astype(BF)
        cp.wait()
        both = jnp.broadcast_to(dmine[0, 0:1, 0:1] + dmine[1, 0:1, 0:1], (HALF, 1))
        dy[t, :, FEAT:] = split_scalar(both).astype(BF)

    dy_block = lambda b: dy.at[b]
    gather_tp(2, dy_block)

    wait_recv(gen.at[other, :], grecv.at[4])
    remote(gen, gout, tsend.at[3], trecv.at[3], flip, when=off_diag)

    da = dab.at[half]
    back = dnw.at[late]
    slope = gd.at[late]

    def product(rows, c):
        return lax.dot_general(
            rows, back[c * HC : (c + 1) * HC, :], (((1,), (1,)), ((), ())), preferred_element_type=F32
        )

    def da_piece(buf, yy, c):
        start, width = wide_cols(c)
        return buf.at[pl.ds(2 * yy, 2), :, pl.ds(start, width)]

    wait_recv(gd.at[0, :, pl.ds(QUARTER, QUARTER), :], grecv.at[1], is_early)
    not_2 = g != 2
    facing = lax.rem(y + 2, 4)
    da_2 = dab.at[1]

    def pass_on(c):
        wait_recv(da_piece(da_2, facing, c), h_r.at[2, c, facing], is_2)
        remote(
            da_piece(da_2, facing, c), da_piece(da_2, facing, c), xs_s.at[c, 1], xs_r.at[c, facing], near, when=is_2
        )
        wait_recv(da_piece(da_2, y, c), xs_r.at[c, y], is_3)
        for j in (1, 3):
            remote(
                da_piece(da_2, y, c), da_piece(da_2, y, c), xs_s.at[c, 1 + j], xs_r.at[c, y],
                row_peer(lax.rem(y + j, 4)), when=is_3,
            )

    def finish(c, dh, distance):
        norm = distance * (1.0 / (IMG_TOK * D_ALL)) + 1e-5
        row_scale = jnp.where(is_late, 1.0, 1.0 / norm)
        start, width = wide_cols(c)
        lo = EXT + c * HC
        two = pl.ds(2 * y, 2)
        if c == 0:
            da[two, :, :EXT] = split_scalar(row_scale).astype(BF).reshape(2, HALF, EXT)
        slopes = slope[:, :, c * HC : (c + 1) * HC].reshape(2 * HALF, HC).astype(F32)
        da[two, :, lo : lo + HC] = (dh * row_scale * slopes).astype(BF).reshape(2, HALF, HC)
        own_piece = da_piece(da, y, c)
        remote(own_piece, own_piece, xs_s.at[c, 0], xs_r.at[c, y], near, when=is_2)
        for j in (2, 1, 3):
            remote(
                own_piece, own_piece, hy_s.at[2, c, j], h_r.at[2, c, y], row_peer(lax.rem(y + j, 4)),
                when=None if j == 2 else not_2,
            )
        if c:
            pass_on(c - 1)

    dyb_2 = dyb.at[1, :, :, pl.ds(0, FEAT)]
    reduce_rep(
        2, HALF, lambda yy: dy[pl.ds(2 * yy, 2)].reshape(2 * HALF, ROW), dy_block, product,
        (sb3, rb3, po3, zs3, zr3), finish,
        lambda: remote(dyb_2, dyb_2, gsend.at[8], grecv.at[8], near, when=is_2),
    )
    pass_on(CHUNKS - 1)

    for i, ref in enumerate((xgs.at[:, pl.ds(QUARTER, QUARTER), :], hs.at[:, pl.ds(QUARTER, QUARTER), :])):
        wait_recv(ref, grecv.at[2 + i], is_early)
    wait_recv(xgf_2, grecv.at[5], is_3)
    for c in range(CHUNKS):
        wait_recv(hf_2(c), grecv.at[10 + c], is_3)
    wait_recv(dyb_2, grecv.at[8], is_3)

    tn = (((0,), (0,)), ((), ()))
    step = 256

    def up_grad(u_of, da_of):
        def tile(i, _):
            cols = pl.ds(pl.multiple_of(i * step, step), step)
            wide = pl.ds(pl.multiple_of(EXT + i * step, EXT), step)
            upg_out[:, cols] = lax.dot_general(u_of(), da_of(wide), tn, preferred_element_type=F32).astype(BF)
            return 0

        lax.fori_loop(0, HID // step, tile, 0)

    def down_grad(h_of, upstream):
        def tile(i, _):
            cols = pl.ds(pl.multiple_of(i * step, step), step)
            dng_out[cols, :] = lax.dot_general(h_of(cols), upstream, tn, preferred_element_type=F32).astype(BF)
            return 0

        lax.fori_loop(0, HID // step, tile, 0)

    n_half, n_all = BLOCKS * HALF, 2 * BLOCKS * HALF

    @pl.when(is_2)
    def _():
        upg_out[...] = jnp.zeros_like(upg_out)
        dng_out[...] = jnp.zeros_like(dng_out)

    @pl.when(is_3)
    def _():
        down_grad(lambda cols: hf[:, :, :, cols].reshape(n_all, -1), dyb[:, :, :, :FEAT].reshape(n_all, FEAT))

    for c in range(CHUNKS):
        for j in (1, 3, 2):
            yy = lax.rem(y + j, 4)
            wait_recv(da_piece(da, yy, c), h_r.at[2, c, yy], not_2)
            wait_recv(da_piece(da_2, yy, c), xs_r.at[c, yy], is_3)

    @pl.when(is_early)
    def _():
        row_scale = join_scalar(da[:, :, :EXT].reshape(n_half, EXT).astype(F32))
        upstream = (dy[:, :, :FEAT].reshape(n_half, FEAT).astype(F32) * row_scale).astype(BF)
        down_grad(lambda cols: hs[:, :, cols].reshape(n_half, -1), upstream)
        up_grad(lambda: xgs[:, :, :FEAT].reshape(n_half, FEAT), lambda cols: da[:, :, cols].reshape(n_half, -1))

    @pl.when(is_3)
    def _():
        up_grad(
            lambda: xgf[:, :, :, :FEAT].reshape(n_all, FEAT), lambda cols: dab[:, :, :, cols].reshape(n_all, -1)
        )

    wait_recv(gout, trecv.at[3], off_diag)

    @pl.when(off_diag)
    def _():
        gen_out[...] = gout[...].astype(F32)

    @pl.when(jnp.logical_not(off_diag))
    def _():
        gen_out[...] = gen[...].astype(F32)

    for cp, when in sends:
        if when is None:
            cp.wait_send()
        else:
            pl.when(when)(cp.wait_send)


def rep_buffers(n):
    return [
        pltpu.VMEM((4, 2 * n, WIDE), BF),
        pltpu.VMEM((4, 2 * n, WIDE), BF),
        pltpu.VMEM((2 * n, WIDE), F32),
        pltpu.VMEM((2 * n, WIDE), BF),
        pltpu.VMEM((2 * n, WIDE), BF),
    ]


def tp_buffers(n):
    return [
        pltpu.VMEM((BLOCKS, n, FEAT), F32),
        pltpu.VMEM((4, n, FEAT), BF),
        pltpu.VMEM((4, n, FEAT), BF),
        pltpu.VMEM((3, n, FEAT), BF),
        pltpu.VMEM((3, n, FEAT), BF),
    ]


def body(noise_in, noise_renoise, text_cond, t_index, gains, up_weights, down_weights):
    vmem = pl.BlockSpec(memory_space=pltpu.VMEM)
    smem = pl.BlockSpec(memory_space=pltpu.SMEM)
    hbm = pl.BlockSpec(memory_space=pl.ANY)
    dma = pltpu.SemaphoreType.DMA
    generated, up_grad, down_grad = pl.pallas_call(
        kernel,
        name="step",
        out_shape=(
            jax.ShapeDtypeStruct((IMG_TOK, FEAT), F32),
            jax.ShapeDtypeStruct((FEAT, HID), BF),
            jax.ShapeDtypeStruct((HID, FEAT), BF),
        ),
        in_specs=[vmem, vmem, vmem, smem, vmem, hbm, hbm],
        out_specs=(vmem, vmem, vmem),
        scratch_shapes=[
            pltpu.VMEM((16, FEAT), BF),
            pltpu.VMEM((QUARTER, FEAT), BF),
            pltpu.VMEM((16, FEAT), BF),
            pltpu.VMEM((HALF, FEAT), BF),
            pltpu.VMEM((IMG_TOK, FEAT), BF),
            pltpu.VMEM((IMG_TOK, FEAT), BF),
            pltpu.VMEM((HALF, FEAT), BF),
            pltpu.VMEM((HALF, FEAT), BF),
            pltpu.VMEM((2, 8, EXT), F32),
            pltpu.VMEM((2, FEAT, HID), BF),
            pltpu.VMEM((2, HID, FEAT), BF),
            pltpu.VMEM((BLOCKS, HALF, ROW), BF),
            pltpu.VMEM((BLOCKS, HALF, HID), BF),
            pltpu.VMEM((2, BLOCKS, HALF, ROW), BF),
            pltpu.VMEM((2, BLOCKS, HALF, HID), BF),
            pltpu.VMEM((2, BLOCKS, HALF, ROW), BF),
            pltpu.VMEM((2, BLOCKS, HALF, WIDE), BF),
            pltpu.VMEM((2, 2, HALF, HID), BF),
            *rep_buffers(QUARTER),
            *tp_buffers(QUARTER),
            *rep_buffers(HALF),
            *tp_buffers(HALF),
            *rep_buffers(HALF),
            dma((4,)),
            dma((4,)),
            dma((4,)),
            dma((10 + CHUNKS,)),
            dma((10 + CHUNKS,)),
            dma((3, 7)),
            dma((3, 8)),
            dma((3, CHUNKS, 4)),
            dma((3, CHUNKS, 4)),
            dma((3, CHUNKS)),
            dma((3, CHUNKS)),
            dma((3, CHUNKS, 4)),
            dma((3, CHUNKS, 4)),
            dma((2, 7)),
            dma((2, 7)),
            dma((CHUNKS, 5)),
            dma((CHUNKS, 4)),
        ],
        compiler_params=pltpu.CompilerParams(
            collective_id=0, has_side_effects=True, vmem_limit_bytes=60 * 2**20
        ),
    )(noise_in, noise_renoise, text_cond, t_index, gains, up_weights, down_weights)
    return generated.astype(BF), up_grad.astype(F32)[None], down_grad.astype(F32)[None]


def solution(mesh):
    in_specs = (
        P("rep", "tp"),
        P("rep", "tp"),
        P("rep", None),
        P("rep"),
        P(),
        P(None, "rep", "tp"),
        P(None, "tp", "rep"),
    )
    out_specs = (P("rep", "tp"), P("grp", "rep", "tp"), P("grp", "tp", "rep"))
    return jax.shard_map(body, mesh=mesh, in_specs=in_specs, out_specs=out_specs, check_vma=False)
```

```python
import functools
import math

import jax
import jax.numpy as jnp
from jax import lax
from jax.experimental import pallas as pl
from jax.experimental.pallas import tpu as pltpu
from jax.sharding import PartitionSpec as P

MESH = pl.DeviceIdType.MESH
BF = jnp.bfloat16
F32 = jnp.float32
FEAT = 384
HID = 1536
LANES = 128
CHUNKS = 4
HC = HID // CHUNKS
BLOCKS = 8
HALF = 64
QUARTER = 32
IMG_TOK = 128
D_ALL = 3072
TOKENS = 1024
GELU_C = math.sqrt(2.0 / math.pi)


def diagonal(n):
    return lax.broadcasted_iota(jnp.int32, (n, LANES), 0) == lax.broadcasted_iota(jnp.int32, (n, LANES), 1)


def to_lanes(column):
    return jnp.sum(jnp.where(diagonal(column.shape[0]), column, 0.0), axis=0, keepdims=True)


def to_column(lanes, n):
    return jnp.sum(jnp.where(diagonal(n), lanes, 0.0), axis=1, keepdims=True)


def gelu_both(a):
    a2 = a * a
    th = jnp.tanh(GELU_C * a * (1.0 + 0.044715 * a2))
    half = 0.5 * (1.0 + th)
    grad = half + 0.5 * a * (1.0 - th * th) * (GELU_C * (1.0 + 3.0 * 0.044715 * a2))
    return a * half, grad


def kernel(
    noise, renoise, cond_in, t_in, gains, up_hbm, down_hbm,
    gen_out, upg_out, dng_out,
    msgc, xt, ct, rt, gen, gout, fk, fother, dmine,
    upw, dnw, xgs, hs, xgf, hf, dyb, dab, gd, dys, ut,
    sc_own, sc_row, sc_zs, sc_zr, sc_all,
    sb1, rb1, po1, zs1, zr1, acc1, ta1, tb1, tc1, td1,
    sb2, rb2, po2, zs2, zr2, acc2, ta2, tb2, tc2, td2,
    sb3, rb3, po3, zs3, zr3,
    wsem, tsend, trecv, gsend, grecv,
    ag_s, ag_r, ry_s, ry_r, rz_s, rz_r, hy_s, h_r, tp_s, tp_r, xs_s, xs_r,
    sy_s, sy_r, sz_s, sz_r, st_s, st_r,
):
    g, r, t = lax.axis_index("grp"), lax.axis_index("rep"), lax.axis_index("tp")
    y, zh = lax.div(r, 2), lax.rem(r, 2)
    zl, core = lax.div(t, 2), lax.rem(t, 2)
    is_late, is_early = g >= 2, g < 2
    is_2, is_3 = g == 2, g == 3
    late = is_late.astype(jnp.int32)
    quart = late
    low = lax.rem(g, 2)
    half = low + late - 2 * low * late
    g_pair = 3 - g
    g_near = g + 1 - 2 * low
    qrow = pl.multiple_of(quart * QUARTER, QUARTER)
    sends = []

    def dev(gg=None, rr=None, tt=None):
        return (g if gg is None else gg, r if rr is None else rr, t if tt is None else tt)

    def remote(src, dst, ssem, rsem, to, when=None):
        cp = pltpu.make_async_remote_copy(
            src_ref=src, dst_ref=dst, send_sem=ssem, recv_sem=rsem, device_id=to, device_id_type=MESH
        )
        if when is None:
            cp.start()
        else:
            pl.when(when)(cp.start)
        sends.append((cp, when))
        return cp

    def wait_recv(dst, rsem, when=None):
        cp = pltpu.make_async_remote_copy(
            src_ref=dst, dst_ref=dst, send_sem=rsem, recv_sem=rsem, device_id=dev(), device_id_type=MESH
        )
        if when is None:
            cp.wait_recv()
        else:
            pl.when(when)(cp.wait_recv)

    model = 1 + late
    loads = [
        pltpu.make_async_copy(up_hbm.at[0], upw.at[0], wsem.at[0]),
        pltpu.make_async_copy(down_hbm.at[0], dnw.at[0], wsem.at[1]),
        pltpu.make_async_copy(up_hbm.at[model], upw.at[1], wsem.at[2]),
        pltpu.make_async_copy(down_hbm.at[model], dnw.at[1], wsem.at[3]),
    ]
    for cp in loads:
        cp.start()

    barrier = pltpu.get_barrier_semaphore()
    sibling = dev(tt=2 * zl + 1 - core)
    flip = dev(rr=t, tt=r)
    off_diag = r != t
    row_peer = lambda yy: dev(rr=2 * yy + zh)
    z_peer = dev(rr=2 * y + 1 - zh)
    peers = [sibling, z_peer, dev(gg=g_pair), dev(gg=g_near)]
    peers += [dev(tt=2 * lax.rem(zl + d, 4) + core) for d in range(1, 4)]
    peers += [row_peer(lax.rem(y + j, 4)) for j in range(1, 4)]
    for peer in peers:
        pl.semaphore_signal(barrier, inc=1, device_id=peer, device_id_type=MESH)

    cond_row = cond_in[0:1, pl.ds(pl.multiple_of(t * FEAT, LANES), FEAT)].astype(F32)
    t_all = jnp.full((16, FEAT), t_in[0], jnp.int32)
    row = lax.broadcasted_iota(jnp.int32, (16, FEAT), 0)
    lane = lax.broadcasted_iota(jnp.int32, (16, FEAT), 1)
    t_part = jnp.where(lane < LANES, t_all >> 8, t_all & 255).astype(F32)
    msgc[...] = jnp.where(row < 8, jnp.broadcast_to(cond_row, (16, FEAT)), t_part).astype(BF)

    @pl.when(off_diag)
    def _():
        pl.semaphore_signal(barrier, inc=1, device_id=flip, device_id_type=MESH)
        pl.semaphore_wait(barrier, len(peers) + 1)

    @pl.when(jnp.logical_not(off_diag))
    def _():
        pl.semaphore_wait(barrier, len(peers))

    own = pl.ds(pl.multiple_of(half * HALF + quart * QUARTER, QUARTER), QUARTER)
    pair = pl.ds(pl.multiple_of(half * HALF + (1 - quart) * QUARTER, QUARTER), QUARTER)
    mine = pl.ds(pl.multiple_of(half * HALF, HALF), HALF)
    other = pl.ds(pl.multiple_of((1 - half) * HALF, HALF), HALF)
    remote(noise.at[own, :], xt, tsend.at[0], trecv.at[0], flip, when=off_diag)
    remote(msgc, ct, tsend.at[1], trecv.at[1], flip, when=off_diag)
    remote(renoise.at[mine, :], rt, tsend.at[2], trecv.at[2], flip, when=off_diag)

    @pl.when(jnp.logical_not(off_diag))
    def _():
        xt[...] = noise[own, :]
        ct[...] = msgc[...]
        rt[...] = renoise[mine, :]

    wait_recv(xt, trecv.at[0], off_diag)
    wait_recv(ct, trecv.at[1], off_diag)
    cond1 = 1.0 + ct[0:1, :].astype(F32)

    def gather_tp(phase, block_of):
        remote(block_of(t), block_of(t), ag_s.at[phase, 0], ag_r.at[phase, t], sibling)
        for d in (2, 1, 3):
            to = dev(tt=2 * lax.rem(zl + d, 4) + core)
            remote(block_of(t), block_of(t), ag_s.at[phase, d], ag_r.at[phase, t], to)

    def wait_chip(phase, block_of, d):
        yy = lax.rem(zl + d, 4)
        if d:
            b = 2 * yy + core
            wait_recv(block_of(b), ag_r.at[phase, b])
            remote(block_of(b), block_of(b), ag_s.at[phase, 3 + d], ag_r.at[phase, b], sibling)
        b = 2 * yy + 1 - core
        wait_recv(block_of(b), ag_r.at[phase, b])

    def scalar_start(phase, lanes):
        sc_own[phase] = jnp.broadcast_to(lanes, (8, LANES))
        for j in (2, 1, 3):
            remote(
                sc_own.at[phase], sc_row.at[phase, y], sy_s.at[phase, j], sy_r.at[phase, y],
                row_peer(lax.rem(y + j, 4)),
            )

    def scalar_to_z(phase):
        total = sc_own[phase]
        for j in (1, 3, 2):
            yy = lax.rem(y + j, 4)
            wait_recv(sc_row.at[phase, yy], sy_r.at[phase, yy])
            total += sc_row[phase, yy]
        sc_zs[phase] = total
        remote(sc_zs.at[phase], sc_zr.at[phase], sz_s.at[phase], sz_r.at[phase], z_peer)

    def scalar_to_tp(phase):
        wait_recv(sc_zr.at[phase], sz_r.at[phase])
        sc_all[phase, t] = sc_zs[phase] + sc_zr[phase]
        tile = sc_all.at[phase, t]
        remote(tile, tile, st_s.at[phase, 0], st_r.at[phase, t], sibling)
        for d in (2, 1, 3):
            remote(tile, tile, st_s.at[phase, d], st_r.at[phase, t], dev(tt=2 * lax.rem(zl + d, 4) + core))

    def scalar_end(phase):
        for d in (1, 3, 2):
            b = 2 * lax.rem(zl + d, 4) + core
            tile = sc_all.at[phase, b]
            wait_recv(tile, st_r.at[phase, b])
            remote(tile, tile, st_s.at[phase, 3 + d], st_r.at[phase, b], sibling)
        for d in range(4):
            b = 2 * lax.rem(zl + d, 4) + 1 - core
            wait_recv(sc_all.at[phase, b], st_r.at[phase, b])

    def reduce_rep(phase, n, rows_of, block_of, product, bufs, finish, gathered):
        sb, rb, po, zs, zr = bufs
        span = lambda c: pl.ds(c * HC, HC)
        for c in range(CHUNKS):
            lo = c * HC
            for d in (0, 1, 3, 2):
                yy = lax.rem(zl + d, 4)
                if c == 0:
                    wait_chip(phase, block_of, d)
                part = product(rows_of(yy), c)

                @pl.when(yy == y)
                def _():
                    po[:, lo : lo + HC] = part

                @pl.when(yy != y)
                def _():
                    sb[yy, :, lo : lo + HC] = part.astype(BF)

                remote(
                    sb.at[yy, :, span(c)], rb.at[y, :, span(c)], ry_s.at[phase, c, d], ry_r.at[phase, c, y],
                    row_peer(yy), when=yy != y,
                )
                if c == 0 and d == 0:
                    scalar_to_z(phase)
            if c == 0:
                gathered()
        scalar_to_tp(phase)

        def to_z(c):
            lo = c * HC
            total = po[:, lo : lo + HC]
            for j in (1, 3, 2):
                yy = lax.rem(y + j, 4)
                wait_recv(rb.at[yy, :, span(c)], ry_r.at[phase, c, yy])
                total += rb[yy, :, lo : lo + HC].astype(F32)
            po[:, lo : lo + HC] = total
            zs[:, lo : lo + HC] = total.astype(BF)
            remote(zs.at[:, span(c)], zr.at[:, span(c)], rz_s.at[phase, c], rz_r.at[phase, c], z_peer)

        def from_z(c):
            lo = c * HC
            if c == 0:
                scalar_end(phase)
            wait_recv(zr.at[:, span(c)], rz_r.at[phase, c])
            finish(c, po[:, lo : lo + HC] + zr[:, lo : lo + HC].astype(F32))

        ahead = CHUNKS - 1 if n == HALF else CHUNKS
        for c in range(CHUNKS):
            if c == ahead:
                from_z(0)
            to_z(c)
        for c in range(1 if ahead < CHUNKS else 0, CHUNKS):
            from_z(c)

    def forward(phase, n, x_rows, gain_row, xg, xg_rows, h, h_rows, bufs, gathered, chunk_here):
        acc, ta, tb, tc, td = bufs[5:]
        up, down, grad = upw.at[phase], dnw.at[phase], gd.at[phase]
        xg[t, xg_rows, :] = (x_rows * (gain_row * cond1)).astype(BF)
        block_of = lambda b: xg.at[b, xg_rows, :]
        gather_tp(phase, block_of)
        scalar_start(phase, to_lanes(jnp.sum(x_rows * x_rows, axis=1, keepdims=True)))
        rows_of = lambda yy: xg[pl.ds(2 * yy, 2), xg_rows, :].reshape(2 * n, FEAT)
        loads[2 * phase].wait()

        def product(rows, c):
            return jnp.dot(rows, up[:, c * HC : (c + 1) * HC], preferred_element_type=F32)

        piece = lambda yy, c: h.at[pl.ds(2 * yy, 2), h_rows, pl.ds(c * HC, HC)]

        state = {}

        def finish(c, a):
            if c == 0:
                squares = [to_column(sc_all[phase, 2 * y + k, 0:1, :], n) for k in range(2)]
                state["factor"] = lax.rsqrt(jnp.concatenate(squares, axis=0) * (1.0 / D_ALL) + 1e-6)
            factor = state["factor"]
            hidden, slope = gelu_both(a * factor)
            cols = slice(c * HC, (c + 1) * HC)
            h[pl.ds(2 * y, 2), h_rows, cols] = hidden.astype(BF).reshape(2, n, HC)
            for j in (2, 1, 3):
                remote(
                    piece(y, c), piece(y, c), hy_s.at[phase, c, j], h_r.at[phase, c, y],
                    row_peer(lax.rem(y + j, 4)),
                )
            grad[:, h_rows, cols] = (slope * factor).astype(BF).reshape(2, n, HC)

        reduce_rep(phase, n, rows_of, block_of, product, bufs[:5], finish, gathered)
        loads[2 * phase + 1].wait()
        for c in range(CHUNKS):
            cols = slice(c * HC, (c + 1) * HC)
            for j in (0, 1, 3, 2):
                yy = lax.rem(y + j, 4)
                if j:
                    wait_recv(piece(yy, c), h_r.at[phase, c, yy])
                both = h[pl.ds(2 * yy, 2), h_rows, cols].reshape(2 * n, HC)
                part = jnp.dot(both, down[cols, :], preferred_element_type=F32).reshape(2, n, FEAT)
                if c:
                    part += acc[pl.ds(2 * yy, 2)]
                acc[pl.ds(2 * yy, 2)] = part
                if c == CHUNKS - 1:
                    ta[yy] = acc[2 * yy + 1 - core].astype(BF)
                    remote(ta.at[yy], tb.at[yy], tp_s.at[phase, yy], tp_r.at[phase, yy], sibling)
            chunk_here(c)
        total = None
        for d in (2, 1, 3, 0):
            yy = lax.rem(zl + d, 4)
            wait_recv(tb.at[yy], tp_r.at[phase, yy])
            both = acc[2 * yy + core] + tb[yy].astype(F32)
            if d:
                tc[d - 1] = both.astype(BF)
                remote(
                    tc.at[d - 1], td.at[d - 1], tp_s.at[phase, 3 + d], tp_r.at[phase, 3 + d],
                    dev(tt=2 * yy + core),
                )
            else:
                total = both
        for d in (1, 3, 2):
            wait_recv(td.at[d - 1], tp_r.at[phase, 3 + d])
            total += td[d - 1].astype(F32)
        return total

    gain = gains[:, pl.ds(pl.multiple_of(r * FEAT, LANES), FEAT)]
    x0 = xt[...].astype(F32)
    q_rows = pl.ds(qrow, QUARTER)
    out = forward(
        0, QUARTER, x0, gain[0:1, :], xgs, q_rows, hs, q_rows,
        (sb1, rb1, po1, zs1, zr1, acc1, ta1, tb1, tc1, td1), lambda: None, lambda c: None,
    )
    gen[own, :] = (x0 + out).astype(BF)
    remote(gen.at[own, :], gen.at[own, :], gsend.at[0], grecv.at[0], dev(gg=g_pair))
    for i, ref in enumerate((gd.at[0, :, q_rows, :], xgs.at[:, q_rows, :], hs.at[:, q_rows, :])):
        remote(ref, ref, gsend.at[1 + i], grecv.at[1 + i], dev(gg=g_pair), when=is_late)
    wait_recv(rt, trecv.at[2], off_diag)
    t_row = ct[8:9, :].astype(F32)
    sigma = 0.1 + 0.8 * (t_row[:, 0:1] * 256.0 + t_row[:, LANES : LANES + 1]) / 999.0
    wait_recv(gen.at[pair, :], grecv.at[0])
    remote(gen.at[mine, :], gen.at[mine, :], gsend.at[4], grecv.at[4], dev(gg=g_near))

    gen_f = gen[mine, :].astype(F32)
    x_t = ((1.0 - sigma) * gen_f + sigma * rt[...].astype(F32)).astype(BF).astype(F32)
    all_rows = pl.ds(0, HALF)
    xgf_2 = xgf.at[1]
    hf_2 = lambda c: hf.at[1, :, :, pl.ds(c * HC, HC)]
    near = dev(gg=g_near)

    def inputs_here():
        wait_recv(gen.at[other, :], grecv.at[4])
        remote(gen, gout, tsend.at[3], trecv.at[3], flip, when=off_diag)
        remote(xgf_2, xgf_2, gsend.at[5], grecv.at[5], near, when=is_2)

    gain_row = jnp.where(is_late, gain[2:3, :], gain[1:2, :])
    out = forward(
        1, HALF, x_t, gain_row, xgf.at[half], all_rows, hf.at[half], all_rows,
        (sb2, rb2, po2, zs2, zr2, acc2, ta2, tb2, tc2, td2),
        inputs_here,
        lambda c: remote(hf_2(c), hf_2(c), gsend.at[10 + c], grecv.at[10 + c], near, when=is_2),
    )
    fk[...] = (x_t + out).astype(BF)
    remote(fk, fother, gsend.at[6], grecv.at[6], dev(gg=g_pair), when=is_late)

    scale = 1.0 / math.sqrt(TOKENS)
    dy = dyb.at[half]

    @pl.when(is_late)
    def _():
        dy[t] = ((fk[...].astype(F32) - gen_f) * scale).astype(BF)
        dmine[...] = jnp.zeros_like(dmine)

    @pl.when(is_early)
    def _():
        real = fk[...].astype(F32)
        distance = jnp.sum(jnp.sum(jnp.abs(gen_f - real), axis=1, keepdims=True), axis=0, keepdims=True)
        dmine[0] = jnp.broadcast_to(distance, (8, LANES))
        cp = pltpu.make_async_remote_copy(
            src_ref=dmine.at[0], dst_ref=dmine.at[1], send_sem=gsend.at[7], recv_sem=grecv.at[7],
            device_id=near, device_id_type=MESH,
        )
        cp.start()
        wait_recv(fother, grecv.at[6])
        dy[t] = ((fother[...].astype(F32) - real) * scale).astype(BF)
        cp.wait()

    dy_block = lambda b: dy.at[b]
    gather_tp(2, dy_block)
    scalar_start(2, dmine[0, 0:1, :] + dmine[1, 0:1, :])

    da = dab.at[half]
    back = dnw.at[late]
    slope = gd.at[late]

    def product(rows, c):
        return lax.dot_general(
            rows, back[c * HC : (c + 1) * HC, :], (((1,), (1,)), ((), ())), preferred_element_type=F32
        )

    def da_piece(buf, yy, c):
        return buf.at[pl.ds(2 * yy, 2), :, pl.ds(c * HC, HC)]

    def image_scale(b):
        norm = sc_all[2, b, 0:1, 0:1] * (1.0 / (IMG_TOK * D_ALL)) + 1e-5
        return jnp.where(is_late, 1.0, 1.0 / norm)

    wait_recv(gd.at[0, :, pl.ds(QUARTER, QUARTER), :], grecv.at[1], is_early)
    not_2 = g != 2
    facing = lax.rem(y + 2, 4)
    da_2 = dab.at[1]

    def pass_on(c):
        behind, ahead = lax.rem(y + (1 if c % 2 else 3), 4), lax.rem(y + (3 if c % 2 else 1), 4)
        passed = da_piece(da, behind, c)
        wait_recv(passed, h_r.at[2, c, behind], not_2)
        remote(passed, passed, hy_s.at[2, c, 0], h_r.at[2, c, behind], row_peer(ahead), when=not_2)
        wait_recv(da_piece(da_2, facing, c), h_r.at[2, c, facing], is_2)
        remote(
            da_piece(da_2, facing, c), da_piece(da_2, facing, c), xs_s.at[c, 1], xs_r.at[c, facing], near, when=is_2
        )
        wait_recv(da_piece(da_2, y, c), xs_r.at[c, y], is_3)
        for j in (1, 3):
            remote(
                da_piece(da_2, y, c), da_piece(da_2, y, c), xs_s.at[c, 1 + j], xs_r.at[c, y],
                row_peer(lax.rem(y + j, 4)), when=is_3,
            )

    row_state = {}

    def finish(c, dh):
        if c == 0:
            scales = [jnp.broadcast_to(image_scale(2 * y + k), (HALF, 1)) for k in range(2)]
            row_state["scale"] = jnp.concatenate(scales, axis=0)
        cols = slice(c * HC, (c + 1) * HC)
        slopes = slope[:, :, cols].reshape(2 * HALF, HC).astype(F32)
        da[pl.ds(2 * y, 2), :, cols] = (dh * row_state["scale"] * slopes).astype(BF).reshape(2, HALF, HC)
        own_piece = da_piece(da, y, c)
        remote(own_piece, own_piece, xs_s.at[c, 0], xs_r.at[c, y], near, when=is_2)
        for j in (2, 1, 3):
            remote(
                own_piece, own_piece, hy_s.at[2, c, j], h_r.at[2, c, y], row_peer(lax.rem(y + j, 4)),
                when=is_2 if j == 2 else not_2,
            )
        if c:
            pass_on(c - 1)

    dyb_2 = dyb.at[1]
    reduce_rep(
        2, HALF, lambda yy: dy[pl.ds(2 * yy, 2)].reshape(2 * HALF, FEAT), dy_block, product,
        (sb3, rb3, po3, zs3, zr3), finish,
        lambda: remote(dyb_2, dyb_2, gsend.at[8], grecv.at[8], near, when=is_2),
    )
    pass_on(CHUNKS - 1)

    for i, ref in enumerate((xgs.at[:, pl.ds(QUARTER, QUARTER), :], hs.at[:, pl.ds(QUARTER, QUARTER), :])):
        wait_recv(ref, grecv.at[2 + i], is_early)
    wait_recv(xgf_2, grecv.at[5], is_3)
    for c in range(CHUNKS):
        wait_recv(hf_2(c), grecv.at[10 + c], is_3)
    wait_recv(dyb_2, grecv.at[8], is_3)

    tn = (((0,), (0,)), ((), ()))
    step = 256

    def down_grad(h_of, upstream_of):
        def tile(i, _):
            cols = pl.ds(pl.multiple_of(i * step, step), step)
            dng_out[cols, :] = lax.dot_general(h_of(cols), upstream_of(), tn, preferred_element_type=F32).astype(BF)
            return 0

        lax.fori_loop(0, HID // step, tile, 0)

    n_half, n_all = BLOCKS * HALF, 2 * BLOCKS * HALF

    @pl.when(is_2)
    def _():
        upg_out[...] = jnp.zeros_like(upg_out)
        dng_out[...] = jnp.zeros_like(dng_out)

    @pl.when(is_early)
    def _():
        for k in range(BLOCKS // 2):
            two = xgs[2 * k : 2 * k + 2].reshape(2 * HALF, FEAT)
            ut[:, k * LANES : (k + 1) * LANES] = two.T
        for b in range(BLOCKS):
            dys[b] = (dy[b].astype(F32) * image_scale(b)).astype(BF)
        down_grad(lambda cols: hs[:, :, cols].reshape(n_half, -1), lambda: dys[...].reshape(n_half, FEAT))

    @pl.when(is_3)
    def _():
        for k in range(BLOCKS):
            two = xgf[k // 4, 2 * (k % 4) : 2 * (k % 4) + 2].reshape(2 * HALF, FEAT)
            ut[:, k * LANES : (k + 1) * LANES] = two.T
        down_grad(lambda cols: hf[:, :, :, cols].reshape(n_all, -1), lambda: dyb[...].reshape(n_all, FEAT))

    for c in range(CHUNKS):
        cols = slice(c * HC, (c + 1) * HC)
        for j in (1, 3, 2):
            yy = lax.rem(y + j, 4)
            if j != (1 if c % 2 else 3):
                wait_recv(da_piece(da, yy, c), h_r.at[2, c, yy], not_2)
            wait_recv(da_piece(da_2, yy, c), xs_r.at[c, yy], is_3)

        @pl.when(is_early)
        def _():
            upg_out[:, cols] = jnp.dot(
                ut[:, :n_half], da[:, :, cols].reshape(n_half, HC), preferred_element_type=F32
            ).astype(BF)

        @pl.when(is_3)
        def _():
            upg_out[:, cols] = jnp.dot(
                ut[...], dab[:, :, :, cols].reshape(n_all, HC), preferred_element_type=F32
            ).astype(BF)

    wait_recv(gout, trecv.at[3], off_diag)

    @pl.when(off_diag)
    def _():
        gen_out[...] = gout[...].astype(F32)

    @pl.when(jnp.logical_not(off_diag))
    def _():
        gen_out[...] = gen[...].astype(F32)

    for cp, when in sends:
        if when is None:
            cp.wait_send()
        else:
            pl.when(when)(cp.wait_send)


def rep_buffers(n):
    return [
        pltpu.VMEM((4, 2 * n, HID), BF),
        pltpu.VMEM((4, 2 * n, HID), BF),
        pltpu.VMEM((2 * n, HID), F32),
        pltpu.VMEM((2 * n, HID), BF),
        pltpu.VMEM((2 * n, HID), BF),
    ]


def tp_buffers(n):
    return [
        pltpu.VMEM((BLOCKS, n, FEAT), F32),
        pltpu.VMEM((4, n, FEAT), BF),
        pltpu.VMEM((4, n, FEAT), BF),
        pltpu.VMEM((3, n, FEAT), BF),
        pltpu.VMEM((3, n, FEAT), BF),
    ]


def body(noise_in, noise_renoise, text_cond, t_index, gains, up_weights, down_weights):
    vmem = pl.BlockSpec(memory_space=pltpu.VMEM)
    smem = pl.BlockSpec(memory_space=pltpu.SMEM)
    hbm = pl.BlockSpec(memory_space=pl.ANY)
    dma = pltpu.SemaphoreType.DMA
    generated, up_grad, down_grad = pl.pallas_call(
        kernel,
        name="step",
        out_shape=(
            jax.ShapeDtypeStruct((IMG_TOK, FEAT), F32),
            jax.ShapeDtypeStruct((FEAT, HID), BF),
            jax.ShapeDtypeStruct((HID, FEAT), BF),
        ),
        in_specs=[vmem, vmem, vmem, smem, vmem, hbm, hbm],
        out_specs=(vmem, vmem, vmem),
        scratch_shapes=[
            pltpu.VMEM((16, FEAT), BF),
            pltpu.VMEM((QUARTER, FEAT), BF),
            pltpu.VMEM((16, FEAT), BF),
            pltpu.VMEM((HALF, FEAT), BF),
            pltpu.VMEM((IMG_TOK, FEAT), BF),
            pltpu.VMEM((IMG_TOK, FEAT), BF),
            pltpu.VMEM((HALF, FEAT), BF),
            pltpu.VMEM((HALF, FEAT), BF),
            pltpu.VMEM((2, 8, LANES), F32),
            pltpu.VMEM((2, FEAT, HID), BF),
            pltpu.VMEM((2, HID, FEAT), BF),
            pltpu.VMEM((BLOCKS, HALF, FEAT), BF),
            pltpu.VMEM((BLOCKS, HALF, HID), BF),
            pltpu.VMEM((2, BLOCKS, HALF, FEAT), BF),
            pltpu.VMEM((2, BLOCKS, HALF, HID), BF),
            pltpu.VMEM((2, BLOCKS, HALF, FEAT), BF),
            pltpu.VMEM((2, BLOCKS, HALF, HID), BF),
            pltpu.VMEM((2, 2, HALF, HID), BF),
            pltpu.VMEM((BLOCKS, HALF, FEAT), BF),
            pltpu.VMEM((FEAT, 2 * BLOCKS * HALF), BF),
            pltpu.VMEM((3, 8, LANES), F32),
            pltpu.VMEM((3, 4, 8, LANES), F32),
            pltpu.VMEM((3, 8, LANES), F32),
            pltpu.VMEM((3, 8, LANES), F32),
            pltpu.VMEM((3, BLOCKS, 8, LANES), F32),
            *rep_buffers(QUARTER),
            *tp_buffers(QUARTER),
            *rep_buffers(HALF),
            *tp_buffers(HALF),
            *rep_buffers(HALF),
            dma((4,)),
            dma((4,)),
            dma((4,)),
            dma((10 + CHUNKS,)),
            dma((10 + CHUNKS,)),
            dma((3, 7)),
            dma((3, 8)),
            dma((3, CHUNKS, 4)),
            dma((3, CHUNKS, 4)),
            dma((3, CHUNKS)),
            dma((3, CHUNKS)),
            dma((3, CHUNKS, 4)),
            dma((3, CHUNKS, 4)),
            dma((2, 7)),
            dma((2, 7)),
            dma((CHUNKS, 5)),
            dma((CHUNKS, 4)),
            dma((3, 4)),
            dma((3, 4)),
            dma((3,)),
            dma((3,)),
            dma((3, 7)),
            dma((3, 8)),
        ],
        compiler_params=pltpu.CompilerParams(
            collective_id=0, has_side_effects=True, vmem_limit_bytes=60 * 2**20
        ),
    )(noise_in, noise_renoise, text_cond, t_index, gains, up_weights, down_weights)
    return generated.astype(BF), up_grad.astype(F32)[None], down_grad.astype(F32)[None]


def solution(mesh):
    in_specs = (
        P("rep", "tp"),
        P("rep", "tp"),
        P("rep", None),
        P("rep"),
        P(),
        P(None, "rep", "tp"),
        P(None, "tp", "rep"),
    )
    out_specs = (P("rep", "tp"), P("grp", "rep", "tp"), P("grp", "tp", "rep"))
    return jax.shard_map(body, mesh=mesh, in_specs=in_specs, out_specs=out_specs, check_vma=False)
```

```python
import functools
import math

import jax
import jax.numpy as jnp
from jax import lax
from jax.experimental import pallas as pl
from jax.experimental.pallas import tpu as pltpu
from jax.sharding import PartitionSpec as P

MESH = pl.DeviceIdType.MESH
BF = jnp.bfloat16
F32 = jnp.float32
FEAT = 384
HID = 1536
LANES = 128
CHUNKS = 4
HC = HID // CHUNKS
BLOCKS = 8
HALF = 64
QUARTER = 32
IMG_TOK = 128
D_ALL = 3072
TOKENS = 1024
GELU_C = math.sqrt(2.0 / math.pi)


def diagonal(n):
    return lax.broadcasted_iota(jnp.int32, (n, LANES), 0) == lax.broadcasted_iota(jnp.int32, (n, LANES), 1)


def to_lanes(column):
    return jnp.sum(jnp.where(diagonal(column.shape[0]), column, 0.0), axis=0, keepdims=True)


def to_column(lanes, n):
    return jnp.sum(jnp.where(diagonal(n), lanes, 0.0), axis=1, keepdims=True)


def gelu_both(a):
    a2 = a * a
    th = jnp.tanh(GELU_C * a * (1.0 + 0.044715 * a2))
    half = 0.5 * (1.0 + th)
    grad = half + 0.5 * a * (1.0 - th * th) * (GELU_C * (1.0 + 3.0 * 0.044715 * a2))
    return a * half, grad


def kernel(
    noise_hbm, renoise_hbm, cond_in, t_in, gains_hbm, up_hbm, down_hbm,
    gen_hbm, upg_hbm, dng_hbm,
    noise, renoise, gain, upg_out, dng_out, isem, osem,
    msgc, xt, ct, rt, gen, gout, fk, fother, dmine,
    upw, dnw, xgs, hs, xgf, hf, dyb, dab, gd, dys, ut,
    sc_own, sc_row, sc_zs, sc_zr, sc_all,
    sb1, rb1, po1, zs1, zr1, acc1, ta1, tb1, tc1, td1,
    sb2, rb2, po2, zs2, zr2, acc2, ta2, tb2, tc2, td2,
    sb3, rb3, po3, zs3, zr3,
    wsem, tsend, trecv, gsend, grecv,
    ag_s, ag_r, ry_s, ry_r, rz_s, rz_r, hy_s, h_r, tp_s, tp_r, xs_s, xs_r,
    sy_s, sy_r, sz_s, sz_r, st_s, st_r,
):
    g, r, t = lax.axis_index("grp"), lax.axis_index("rep"), lax.axis_index("tp")
    y, zh = lax.div(r, 2), lax.rem(r, 2)
    zl, core = lax.div(t, 2), lax.rem(t, 2)
    is_late, is_early = g >= 2, g < 2
    is_2, is_3 = g == 2, g == 3
    late = is_late.astype(jnp.int32)
    quart = late
    low = lax.rem(g, 2)
    half = low + late - 2 * low * late
    g_pair = 3 - g
    g_near = g + 1 - 2 * low
    qrow = pl.multiple_of(quart * QUARTER, QUARTER)
    sends = []

    def dev(gg=None, rr=None, tt=None):
        return (g if gg is None else gg, r if rr is None else rr, t if tt is None else tt)

    def remote(src, dst, ssem, rsem, to, when=None):
        cp = pltpu.make_async_remote_copy(
            src_ref=src, dst_ref=dst, send_sem=ssem, recv_sem=rsem, device_id=to, device_id_type=MESH
        )
        if when is None:
            cp.start()
        else:
            pl.when(when)(cp.start)
        sends.append((cp, when))
        return cp

    def wait_recv(dst, rsem, when=None):
        cp = pltpu.make_async_remote_copy(
            src_ref=dst, dst_ref=dst, send_sem=rsem, recv_sem=rsem, device_id=dev(), device_id_type=MESH
        )
        if when is None:
            cp.wait_recv()
        else:
            pl.when(when)(cp.wait_recv)

    own = pl.ds(pl.multiple_of(half * HALF + quart * QUARTER, QUARTER), QUARTER)
    pair = pl.ds(pl.multiple_of(half * HALF + (1 - quart) * QUARTER, QUARTER), QUARTER)
    mine = pl.ds(pl.multiple_of(half * HALF, HALF), HALF)
    other = pl.ds(pl.multiple_of((1 - half) * HALF, HALF), HALF)
    inputs = [
        pltpu.make_async_copy(noise_hbm.at[own, :], noise, isem.at[0]),
        pltpu.make_async_copy(renoise_hbm.at[mine, :], renoise, isem.at[1]),
        pltpu.make_async_copy(gains_hbm.at[:, pl.ds(pl.multiple_of(r * FEAT, LANES), FEAT)], gain, isem.at[2]),
    ]

    model = 1 + late
    loads = [
        pltpu.make_async_copy(up_hbm.at[0], upw.at[0], wsem.at[0]),
        pltpu.make_async_copy(down_hbm.at[0], dnw.at[0], wsem.at[1]),
        pltpu.make_async_copy(up_hbm.at[model], upw.at[1], wsem.at[2]),
        pltpu.make_async_copy(down_hbm.at[model], dnw.at[1], wsem.at[3]),
    ]
    barrier = pltpu.get_barrier_semaphore()
    sibling = dev(tt=2 * zl + 1 - core)
    flip = dev(rr=t, tt=r)
    off_diag = r != t
    row_peer = lambda yy: dev(rr=2 * yy + zh)
    z_peer = dev(rr=2 * y + 1 - zh)
    peers = [sibling, z_peer, dev(gg=g_pair), dev(gg=g_near)]
    peers += [dev(tt=2 * lax.rem(zl + d, 4) + core) for d in range(1, 4)]
    peers += [row_peer(lax.rem(y + j, 4)) for j in range(1, 4)]
    for peer in peers:
        pl.semaphore_signal(barrier, inc=1, device_id=peer, device_id_type=MESH)

    for cp in inputs + loads:
        cp.start()

    cond_row = cond_in[0:1, pl.ds(pl.multiple_of(t * FEAT, LANES), FEAT)].astype(F32)
    t_all = jnp.full((16, FEAT), t_in[0], jnp.int32)
    row = lax.broadcasted_iota(jnp.int32, (16, FEAT), 0)
    lane = lax.broadcasted_iota(jnp.int32, (16, FEAT), 1)
    t_part = jnp.where(lane < LANES, t_all >> 8, t_all & 255).astype(F32)
    msgc[...] = jnp.where(row < 8, jnp.broadcast_to(cond_row, (16, FEAT)), t_part).astype(BF)

    @pl.when(off_diag)
    def _():
        pl.semaphore_signal(barrier, inc=1, device_id=flip, device_id_type=MESH)
        pl.semaphore_wait(barrier, len(peers) + 1)

    @pl.when(jnp.logical_not(off_diag))
    def _():
        pl.semaphore_wait(barrier, len(peers))

    for cp in inputs:
        cp.wait()
    remote(noise, xt, tsend.at[0], trecv.at[0], flip, when=off_diag)
    remote(msgc, ct, tsend.at[1], trecv.at[1], flip, when=off_diag)
    remote(renoise, rt, tsend.at[2], trecv.at[2], flip, when=off_diag)

    @pl.when(jnp.logical_not(off_diag))
    def _():
        xt[...] = noise[...]
        ct[...] = msgc[...]
        rt[...] = renoise[...]

    wait_recv(xt, trecv.at[0], off_diag)
    wait_recv(ct, trecv.at[1], off_diag)
    cond1 = 1.0 + ct[0:1, :].astype(F32)

    def gather_tp(phase, block_of):
        remote(block_of(t), block_of(t), ag_s.at[phase, 0], ag_r.at[phase, t], sibling)
        for d in (2, 1, 3):
            to = dev(tt=2 * lax.rem(zl + d, 4) + core)
            remote(block_of(t), block_of(t), ag_s.at[phase, d], ag_r.at[phase, t], to)

    def wait_chip(phase, block_of, d):
        yy = lax.rem(zl + d, 4)
        if d:
            b = 2 * yy + core
            wait_recv(block_of(b), ag_r.at[phase, b])
            remote(block_of(b), block_of(b), ag_s.at[phase, 3 + d], ag_r.at[phase, b], sibling)
        b = 2 * yy + 1 - core
        wait_recv(block_of(b), ag_r.at[phase, b])

    def scalar_start(phase, lanes):
        sc_own[phase] = jnp.broadcast_to(lanes, (8, LANES))
        for j in (2, 1, 3):
            remote(
                sc_own.at[phase], sc_row.at[phase, y], sy_s.at[phase, j], sy_r.at[phase, y],
                row_peer(lax.rem(y + j, 4)),
            )

    def scalar_to_z(phase):
        total = sc_own[phase]
        for j in (1, 3, 2):
            yy = lax.rem(y + j, 4)
            wait_recv(sc_row.at[phase, yy], sy_r.at[phase, yy])
            total += sc_row[phase, yy]
        sc_zs[phase] = total
        remote(sc_zs.at[phase], sc_zr.at[phase], sz_s.at[phase], sz_r.at[phase], z_peer)

    def scalar_to_tp(phase):
        wait_recv(sc_zr.at[phase], sz_r.at[phase])
        sc_all[phase, t] = sc_zs[phase] + sc_zr[phase]
        tile = sc_all.at[phase, t]
        remote(tile, tile, st_s.at[phase, 0], st_r.at[phase, t], sibling)
        for d in (2, 1, 3):
            remote(tile, tile, st_s.at[phase, d], st_r.at[phase, t], dev(tt=2 * lax.rem(zl + d, 4) + core))

    def scalar_end(phase):
        for d in (1, 3, 2):
            b = 2 * lax.rem(zl + d, 4) + core
            tile = sc_all.at[phase, b]
            wait_recv(tile, st_r.at[phase, b])
            remote(tile, tile, st_s.at[phase, 3 + d], st_r.at[phase, b], sibling)
        for d in range(4):
            b = 2 * lax.rem(zl + d, 4) + 1 - core
            wait_recv(sc_all.at[phase, b], st_r.at[phase, b])

    def reduce_rep(phase, n, rows_of, block_of, product, bufs, finish, gathered):
        sb, rb, po, zs, zr = bufs
        span = lambda c: pl.ds(c * HC, HC)
        for c in range(CHUNKS):
            lo = c * HC
            for d in (0, 1, 3, 2):
                yy = lax.rem(zl + d, 4)
                if c == 0:
                    wait_chip(phase, block_of, d)
                part = product(rows_of(yy), c)

                @pl.when(yy == y)
                def _():
                    po[:, lo : lo + HC] = part

                @pl.when(yy != y)
                def _():
                    sb[yy, :, lo : lo + HC] = part.astype(BF)

                remote(
                    sb.at[yy, :, span(c)], rb.at[y, :, span(c)], ry_s.at[phase, c, d], ry_r.at[phase, c, y],
                    row_peer(yy), when=yy != y,
                )
                if c == 0 and d == 1:
                    scalar_to_z(phase)
            if c == 0:
                gathered()
        scalar_to_tp(phase)

        def to_z(c):
            lo = c * HC
            total = po[:, lo : lo + HC]
            for j in (1, 3, 2):
                yy = lax.rem(y + j, 4)
                wait_recv(rb.at[yy, :, span(c)], ry_r.at[phase, c, yy])
                total += rb[yy, :, lo : lo + HC].astype(F32)
            po[:, lo : lo + HC] = total
            zs[:, lo : lo + HC] = total.astype(BF)
            remote(zs.at[:, span(c)], zr.at[:, span(c)], rz_s.at[phase, c], rz_r.at[phase, c], z_peer)

        def from_z(c):
            lo = c * HC
            if c == 0:
                scalar_end(phase)
            wait_recv(zr.at[:, span(c)], rz_r.at[phase, c])
            finish(c, po[:, lo : lo + HC] + zr[:, lo : lo + HC].astype(F32))

        ahead = CHUNKS - 1 if n == HALF else CHUNKS
        for c in range(CHUNKS):
            if c == ahead:
                from_z(0)
            to_z(c)
        for c in range(1 if ahead < CHUNKS else 0, CHUNKS):
            from_z(c)

    def forward(phase, n, x_rows, gain_row, xg, xg_rows, h, h_rows, bufs, gathered, chunk_here):
        acc, ta, tb, tc, td = bufs[5:]
        up, down, grad = upw.at[phase], dnw.at[phase], gd.at[phase]
        xg[t, xg_rows, :] = (x_rows * (gain_row * cond1)).astype(BF)
        block_of = lambda b: xg.at[b, xg_rows, :]
        gather_tp(phase, block_of)
        scalar_start(phase, to_lanes(jnp.sum(x_rows * x_rows, axis=1, keepdims=True)))
        rows_of = lambda yy: xg[pl.ds(2 * yy, 2), xg_rows, :].reshape(2 * n, FEAT)
        loads[2 * phase].wait()

        def product(rows, c):
            return jnp.dot(rows, up[:, c * HC : (c + 1) * HC], preferred_element_type=F32)

        piece = lambda yy, c: h.at[pl.ds(2 * yy, 2), h_rows, pl.ds(c * HC, HC)]

        state = {}
        relayed = n == HALF

        def pass_on(c):
            behind, ahead = lax.rem(y + (1 if c % 2 else 3), 4), lax.rem(y + (3 if c % 2 else 1), 4)
            passed = piece(behind, c)
            wait_recv(passed, h_r.at[phase, c, behind])
            remote(passed, passed, hy_s.at[phase, c, 2], h_r.at[phase, c, behind], row_peer(ahead))

        def finish(c, a):
            if c == 0:
                squares = [to_column(sc_all[phase, 2 * y + k, 0:1, :], n) for k in range(2)]
                state["factor"] = lax.rsqrt(jnp.concatenate(squares, axis=0) * (1.0 / D_ALL) + 1e-6)
            factor = state["factor"]
            hidden, slope = gelu_both(a * factor)
            cols = slice(c * HC, (c + 1) * HC)
            h[pl.ds(2 * y, 2), h_rows, cols] = hidden.astype(BF).reshape(2, n, HC)
            for j in (1, 3) if relayed else (2, 1, 3):
                remote(
                    piece(y, c), piece(y, c), hy_s.at[phase, c, j], h_r.at[phase, c, y],
                    row_peer(lax.rem(y + j, 4)),
                )
            if relayed and c:
                pass_on(c - 1)
            grad[:, h_rows, cols] = (slope * factor).astype(BF).reshape(2, n, HC)

        reduce_rep(phase, n, rows_of, block_of, product, bufs[:5], finish, gathered)
        if relayed:
            pass_on(CHUNKS - 1)
        loads[2 * phase + 1].wait()
        for c in range(CHUNKS):
            cols = slice(c * HC, (c + 1) * HC)
            for j in (0, 1, 3, 2):
                yy = lax.rem(y + j, 4)
                if j and not (relayed and j == (1 if c % 2 else 3)):
                    wait_recv(piece(yy, c), h_r.at[phase, c, yy])
                both = h[pl.ds(2 * yy, 2), h_rows, cols].reshape(2 * n, HC)
                part = jnp.dot(both, down[cols, :], preferred_element_type=F32).reshape(2, n, FEAT)
                if c:
                    part += acc[pl.ds(2 * yy, 2)]
                acc[pl.ds(2 * yy, 2)] = part
                if c == CHUNKS - 1:
                    ta[yy] = acc[2 * yy + 1 - core].astype(BF)
                    remote(ta.at[yy], tb.at[yy], tp_s.at[phase, yy], tp_r.at[phase, yy], sibling)
            chunk_here(c)
        total = None
        for d in (2, 1, 3, 0):
            yy = lax.rem(zl + d, 4)
            wait_recv(tb.at[yy], tp_r.at[phase, yy])
            both = acc[2 * yy + core] + tb[yy].astype(F32)
            if d:
                tc[d - 1] = both.astype(BF)
                remote(
                    tc.at[d - 1], td.at[d - 1], tp_s.at[phase, 3 + d], tp_r.at[phase, 3 + d],
                    dev(tt=2 * yy + core),
                )
            else:
                total = both
        for d in (1, 3, 2):
            wait_recv(td.at[d - 1], tp_r.at[phase, 3 + d])
            total += td[d - 1].astype(F32)
        return total

    x0 = xt[...].astype(F32)
    q_rows = pl.ds(qrow, QUARTER)
    out = forward(
        0, QUARTER, x0, gain[0:1, :], xgs, q_rows, hs, q_rows,
        (sb1, rb1, po1, zs1, zr1, acc1, ta1, tb1, tc1, td1), lambda: None, lambda c: None,
    )
    gen[own, :] = (x0 + out).astype(BF)
    remote(gen.at[own, :], gen.at[own, :], gsend.at[0], grecv.at[0], dev(gg=g_pair))
    for i, ref in enumerate((gd.at[0, :, q_rows, :], xgs.at[:, q_rows, :], hs.at[:, q_rows, :])):
        remote(ref, ref, gsend.at[1 + i], grecv.at[1 + i], dev(gg=g_pair), when=is_late)
    wait_recv(rt, trecv.at[2], off_diag)
    t_row = ct[8:9, :].astype(F32)
    sigma = 0.1 + 0.8 * (t_row[:, 0:1] * 256.0 + t_row[:, LANES : LANES + 1]) / 999.0
    wait_recv(gen.at[pair, :], grecv.at[0])
    remote(gen.at[mine, :], gen.at[mine, :], gsend.at[4], grecv.at[4], dev(gg=g_near))

    gen_f = gen[mine, :].astype(F32)
    x_t = ((1.0 - sigma) * gen_f + sigma * rt[...].astype(F32)).astype(BF).astype(F32)
    all_rows = pl.ds(0, HALF)
    xgf_2 = xgf.at[1]
    hf_2 = lambda c: hf.at[1, :, :, pl.ds(c * HC, HC)]
    near = dev(gg=g_near)

    def inputs_here():
        wait_recv(gen.at[other, :], grecv.at[4])
        remote(gen, gout, tsend.at[3], trecv.at[3], flip, when=off_diag)
        remote(xgf_2, xgf_2, gsend.at[5], grecv.at[5], near, when=is_2)

    gain_row = jnp.where(is_late, gain[2:3, :], gain[1:2, :])
    out = forward(
        1, HALF, x_t, gain_row, xgf.at[half], all_rows, hf.at[half], all_rows,
        (sb2, rb2, po2, zs2, zr2, acc2, ta2, tb2, tc2, td2),
        inputs_here,
        lambda c: remote(hf_2(c), hf_2(c), gsend.at[10 + c], grecv.at[10 + c], near, when=is_2),
    )
    fk[...] = (x_t + out).astype(BF)
    remote(fk, fother, gsend.at[6], grecv.at[6], dev(gg=g_pair), when=is_late)

    scale = 1.0 / math.sqrt(TOKENS)
    dy = dyb.at[half]

    @pl.when(is_late)
    def _():
        dy[t] = ((fk[...].astype(F32) - gen_f) * scale).astype(BF)
        dmine[...] = jnp.zeros_like(dmine)

    @pl.when(is_early)
    def _():
        real = fk[...].astype(F32)
        distance = jnp.sum(jnp.sum(jnp.abs(gen_f - real), axis=1, keepdims=True), axis=0, keepdims=True)
        dmine[0] = jnp.broadcast_to(distance, (8, LANES))
        cp = pltpu.make_async_remote_copy(
            src_ref=dmine.at[0], dst_ref=dmine.at[1], send_sem=gsend.at[7], recv_sem=grecv.at[7],
            device_id=near, device_id_type=MESH,
        )
        cp.start()
        wait_recv(fother, grecv.at[6])
        dy[t] = ((fother[...].astype(F32) - real) * scale).astype(BF)
        cp.wait()

    dy_block = lambda b: dy.at[b]
    gather_tp(2, dy_block)
    scalar_start(2, dmine[0, 0:1, :] + dmine[1, 0:1, :])

    da = dab.at[half]
    back = dnw.at[late]
    slope = gd.at[late]

    def product(rows, c):
        return lax.dot_general(
            rows, back[c * HC : (c + 1) * HC, :], (((1,), (1,)), ((), ())), preferred_element_type=F32
        )

    def da_piece(buf, yy, c):
        return buf.at[pl.ds(2 * yy, 2), :, pl.ds(c * HC, HC)]

    def image_scale(b):
        norm = sc_all[2, b, 0:1, 0:1] * (1.0 / (IMG_TOK * D_ALL)) + 1e-5
        return jnp.where(is_late, 1.0, 1.0 / norm)

    wait_recv(gd.at[0, :, pl.ds(QUARTER, QUARTER), :], grecv.at[1], is_early)
    not_2 = g != 2
    da_2 = dab.at[1]

    def pass_on(c):
        behind, ahead = lax.rem(y + (1 if c % 2 else 3), 4), lax.rem(y + (3 if c % 2 else 1), 4)
        passed = da_piece(da, behind, c)
        wait_recv(passed, h_r.at[2, c, behind], not_2)
        remote(passed, passed, hy_s.at[2, c, 0], h_r.at[2, c, behind], row_peer(ahead), when=not_2)
        last = c == CHUNKS - 1
        for j in (1, 3, 2) if last else (2,):
            pair_2 = lax.rem(y + j, 4)
            crossing = da_piece(da_2, pair_2, c)
            wait_recv(crossing, h_r.at[2, c, pair_2], is_2)
            remote(crossing, crossing, xs_s.at[c, j], xs_r.at[c, pair_2], near, when=is_2)
        wait_recv(da_piece(da_2, y, c), xs_r.at[c, y], is_3)
        if not last:
            for j in (1, 3):
                remote(
                    da_piece(da_2, y, c), da_piece(da_2, y, c), xs_s.at[c, 3 + j], xs_r.at[c, y],
                    row_peer(lax.rem(y + j, 4)), when=is_3,
                )

    row_state = {}

    def finish(c, dh):
        if c == 0:
            scales = [jnp.broadcast_to(image_scale(2 * y + k), (HALF, 1)) for k in range(2)]
            row_state["scale"] = jnp.concatenate(scales, axis=0)
        cols = slice(c * HC, (c + 1) * HC)
        slopes = slope[:, :, cols].reshape(2 * HALF, HC).astype(F32)
        da[pl.ds(2 * y, 2), :, cols] = (dh * row_state["scale"] * slopes).astype(BF).reshape(2, HALF, HC)
        own_piece = da_piece(da, y, c)
        remote(own_piece, own_piece, xs_s.at[c, 0], xs_r.at[c, y], near, when=is_2)
        for j in (2, 1, 3):
            remote(
                own_piece, own_piece, hy_s.at[2, c, j], h_r.at[2, c, y], row_peer(lax.rem(y + j, 4)),
                when=is_2 if j == 2 else None if c == CHUNKS - 1 else not_2,
            )
        if c:
            pass_on(c - 1)

    dyb_2 = dyb.at[1]
    reduce_rep(
        2, HALF, lambda yy: dy[pl.ds(2 * yy, 2)].reshape(2 * HALF, FEAT), dy_block, product,
        (sb3, rb3, po3, zs3, zr3), finish,
        lambda: remote(dyb_2, dyb_2, gsend.at[8], grecv.at[8], near, when=is_2),
    )
    pass_on(CHUNKS - 1)

    for i, ref in enumerate((xgs.at[:, pl.ds(QUARTER, QUARTER), :], hs.at[:, pl.ds(QUARTER, QUARTER), :])):
        wait_recv(ref, grecv.at[2 + i], is_early)
    wait_recv(xgf_2, grecv.at[5], is_3)
    for c in range(CHUNKS):
        wait_recv(hf_2(c), grecv.at[10 + c], is_3)
    wait_recv(dyb_2, grecv.at[8], is_3)

    tn = (((0,), (0,)), ((), ()))
    step = 256

    def down_grad(h_of, upstream_of):
        def tile(i, _):
            cols = pl.ds(pl.multiple_of(i * step, step), step)
            dng_out[cols, :] = lax.dot_general(h_of(cols), upstream_of(), tn, preferred_element_type=F32).astype(BF)
            return 0

        lax.fori_loop(0, HID // step, tile, 0)

    n_half, n_all = BLOCKS * HALF, 2 * BLOCKS * HALF
    outs = [pltpu.make_async_copy(gout, gen_hbm, osem.at[0]), pltpu.make_async_copy(dng_out, dng_hbm, osem.at[1])]
    wait_recv(gout, trecv.at[3], off_diag)

    @pl.when(jnp.logical_not(off_diag))
    def _():
        gout[...] = gen[...]

    outs[0].start()

    @pl.when(is_2)
    def _():
        upg_out[...] = jnp.zeros_like(upg_out)
        dng_out[...] = jnp.zeros_like(dng_out)

    @pl.when(is_early)
    def _():
        for k in range(BLOCKS // 2):
            two = xgs[2 * k : 2 * k + 2].reshape(2 * HALF, FEAT)
            ut[:, k * LANES : (k + 1) * LANES] = two.T
        for b in range(BLOCKS):
            dys[b] = (dy[b].astype(F32) * image_scale(b)).astype(BF)
        down_grad(lambda cols: hs[:, :, cols].reshape(n_half, -1), lambda: dys[...].reshape(n_half, FEAT))

    @pl.when(is_3)
    def _():
        for k in range(BLOCKS):
            two = xgf[k // 4, 2 * (k % 4) : 2 * (k % 4) + 2].reshape(2 * HALF, FEAT)
            ut[:, k * LANES : (k + 1) * LANES] = two.T
        down_grad(lambda cols: hf[:, :, :, cols].reshape(n_all, -1), lambda: dyb[...].reshape(n_all, FEAT))

    outs[1].start()
    for c in range(CHUNKS):
        cols = slice(c * HC, (c + 1) * HC)
        for j in (1, 3, 2):
            yy = lax.rem(y + j, 4)
            if j != (1 if c % 2 else 3):
                wait_recv(da_piece(da, yy, c), h_r.at[2, c, yy], not_2)
            wait_recv(da_piece(da_2, yy, c), xs_r.at[c, yy], is_3)

        @pl.when(is_early)
        def _():
            upg_out[:, cols] = jnp.dot(
                ut[:, :n_half], da[:, :, cols].reshape(n_half, HC), preferred_element_type=F32
            ).astype(BF)

        @pl.when(is_3)
        def _():
            upg_out[:, cols] = jnp.dot(
                ut[...], dab[:, :, :, cols].reshape(n_all, HC), preferred_element_type=F32
            ).astype(BF)

        outs.append(pltpu.make_async_copy(upg_out.at[:, cols], upg_hbm.at[:, cols], osem.at[2 + c]))
        outs[-1].start()

    for cp, when in sends:
        if when is None:
            cp.wait_send()
        else:
            pl.when(when)(cp.wait_send)
    for cp in outs:
        cp.wait()


def widen(gen, up, down, gen_out, up_out, down_out):
    gen_out[...] = gen[...]
    up_out[0] = up[...].astype(F32)
    down_out[0] = down[...].astype(F32)


def rep_buffers(n):
    return [
        pltpu.VMEM((4, 2 * n, HID), BF),
        pltpu.VMEM((4, 2 * n, HID), BF),
        pltpu.VMEM((2 * n, HID), F32),
        pltpu.VMEM((2 * n, HID), BF),
        pltpu.VMEM((2 * n, HID), BF),
    ]


def tp_buffers(n):
    return [
        pltpu.VMEM((BLOCKS, n, FEAT), F32),
        pltpu.VMEM((4, n, FEAT), BF),
        pltpu.VMEM((4, n, FEAT), BF),
        pltpu.VMEM((3, n, FEAT), BF),
        pltpu.VMEM((3, n, FEAT), BF),
    ]


def body(noise_in, noise_renoise, text_cond, t_index, gains, up_weights, down_weights):
    vmem = pl.BlockSpec(memory_space=pltpu.VMEM)
    smem = pl.BlockSpec(memory_space=pltpu.SMEM)
    hbm = pl.BlockSpec(memory_space=pl.ANY)
    dma = pltpu.SemaphoreType.DMA
    generated, up_grad, down_grad = pl.pallas_call(
        kernel,
        name="step",
        out_shape=(
            jax.ShapeDtypeStruct((IMG_TOK, FEAT), BF),
            jax.ShapeDtypeStruct((FEAT, HID), BF),
            jax.ShapeDtypeStruct((HID, FEAT), BF),
        ),
        in_specs=[hbm, hbm, vmem, smem, hbm, hbm, hbm],
        out_specs=(hbm, hbm, hbm),
        scratch_shapes=[
            pltpu.VMEM((QUARTER, FEAT), BF),
            pltpu.VMEM((HALF, FEAT), BF),
            pltpu.VMEM((3, FEAT), F32),
            pltpu.VMEM((FEAT, HID), BF),
            pltpu.VMEM((HID, FEAT), BF),
            dma((3,)),
            dma((2 + CHUNKS,)),
            pltpu.VMEM((16, FEAT), BF),
            pltpu.VMEM((QUARTER, FEAT), BF),
            pltpu.VMEM((16, FEAT), BF),
            pltpu.VMEM((HALF, FEAT), BF),
            pltpu.VMEM((IMG_TOK, FEAT), BF),
            pltpu.VMEM((IMG_TOK, FEAT), BF),
            pltpu.VMEM((HALF, FEAT), BF),
            pltpu.VMEM((HALF, FEAT), BF),
            pltpu.VMEM((2, 8, LANES), F32),
            pltpu.VMEM((2, FEAT, HID), BF),
            pltpu.VMEM((2, HID, FEAT), BF),
            pltpu.VMEM((BLOCKS, HALF, FEAT), BF),
            pltpu.VMEM((BLOCKS, HALF, HID), BF),
            pltpu.VMEM((2, BLOCKS, HALF, FEAT), BF),
            pltpu.VMEM((2, BLOCKS, HALF, HID), BF),
            pltpu.VMEM((2, BLOCKS, HALF, FEAT), BF),
            pltpu.VMEM((2, BLOCKS, HALF, HID), BF),
            pltpu.VMEM((2, 2, HALF, HID), BF),
            pltpu.VMEM((BLOCKS, HALF, FEAT), BF),
            pltpu.VMEM((FEAT, 2 * BLOCKS * HALF), BF),
            pltpu.VMEM((3, 8, LANES), F32),
            pltpu.VMEM((3, 4, 8, LANES), F32),
            pltpu.VMEM((3, 8, LANES), F32),
            pltpu.VMEM((3, 8, LANES), F32),
            pltpu.VMEM((3, BLOCKS, 8, LANES), F32),
            *rep_buffers(QUARTER),
            *tp_buffers(QUARTER),
            *rep_buffers(HALF),
            *tp_buffers(HALF),
            *rep_buffers(HALF),
            dma((4,)),
            dma((4,)),
            dma((4,)),
            dma((10 + CHUNKS,)),
            dma((10 + CHUNKS,)),
            dma((3, 7)),
            dma((3, 8)),
            dma((3, CHUNKS, 4)),
            dma((3, CHUNKS, 4)),
            dma((3, CHUNKS)),
            dma((3, CHUNKS)),
            dma((3, CHUNKS, 4)),
            dma((3, CHUNKS, 4)),
            dma((2, 7)),
            dma((2, 7)),
            dma((CHUNKS, 7)),
            dma((CHUNKS, 4)),
            dma((3, 4)),
            dma((3, 4)),
            dma((3,)),
            dma((3,)),
            dma((3, 7)),
            dma((3, 8)),
        ],
        compiler_params=pltpu.CompilerParams(
            collective_id=0, has_side_effects=True, vmem_limit_bytes=60 * 2**20
        ),
    )(noise_in, noise_renoise, text_cond, t_index, gains, up_weights, down_weights)
    parts = 4
    rows = [
        pl.BlockSpec((IMG_TOK // parts, FEAT), lambda i: (i, 0)),
        pl.BlockSpec((FEAT // parts, HID), lambda i: (i, 0)),
        pl.BlockSpec((HID // parts, FEAT), lambda i: (i, 0)),
    ]
    wide = [
        rows[0],
        pl.BlockSpec((1, FEAT // parts, HID), lambda i: (0, i, 0)),
        pl.BlockSpec((1, HID // parts, FEAT), lambda i: (0, i, 0)),
    ]
    return pl.pallas_call(
        widen,
        name="widen",
        grid=(parts,),
        out_shape=(
            jax.ShapeDtypeStruct((IMG_TOK, FEAT), BF),
            jax.ShapeDtypeStruct((1, FEAT, HID), F32),
            jax.ShapeDtypeStruct((1, HID, FEAT), F32),
        ),
        in_specs=rows,
        out_specs=wide,
    )(generated, up_grad, down_grad)


def solution(mesh):
    in_specs = (
        P("rep", "tp"),
        P("rep", "tp"),
        P("rep", None),
        P("rep"),
        P(),
        P(None, "rep", "tp"),
        P(None, "tp", "rep"),
    )
    out_specs = (P("rep", "tp"), P("grp", "rep", "tp"), P("grp", "tp", "rep"))
    return jax.shard_map(body, mesh=mesh, in_specs=in_specs, out_specs=out_specs, check_vma=False)
```

```python
import functools
import math

import jax
import jax.numpy as jnp
from jax import lax
from jax.experimental import pallas as pl
from jax.experimental.pallas import tpu as pltpu
from jax.sharding import PartitionSpec as P

MESH = pl.DeviceIdType.MESH
BF = jnp.bfloat16
F32 = jnp.float32
FEAT = 384
HID = 1536
LANES = 128
CHUNKS = 4
HC = HID // CHUNKS
BLOCKS = 8
HALF = 64
QUARTER = 32
IMG_TOK = 128
D_ALL = 3072
TOKENS = 1024
GELU_C = math.sqrt(2.0 / math.pi)


def diagonal(n):
    return lax.broadcasted_iota(jnp.int32, (n, LANES), 0) == lax.broadcasted_iota(jnp.int32, (n, LANES), 1)


def to_lanes(column):
    return jnp.sum(jnp.where(diagonal(column.shape[0]), column, 0.0), axis=0, keepdims=True)


def to_column(lanes, n):
    return jnp.sum(jnp.where(diagonal(n), lanes, 0.0), axis=1, keepdims=True)


def gelu_both(a):
    a2 = a * a
    th = jnp.tanh(GELU_C * a * (1.0 + 0.044715 * a2))
    half = 0.5 * (1.0 + th)
    grad = half + 0.5 * a * (1.0 - th * th) * (GELU_C * (1.0 + 3.0 * 0.044715 * a2))
    return a * half, grad


def kernel(
    noise_hbm, renoise_hbm, cond_in, t_in, gains_hbm, up_hbm, down_hbm,
    gen_hbm, upg_hbm, dng_hbm,
    noise, renoise, gain, upg_out, dng_out, isem, osem,
    msgc, xt, ct, rt, gen, gout, fk, fother, dmine,
    upw, dnw, xgs, hs, xgf, hf, dyb, dab, gd, dys, ut,
    sc_own, sc_row, sc_zs, sc_zr, sc_all,
    sb1, rb1, po1, zs1, zr1, acc1, ta1, tb1, tc1, td1,
    sb2, rb2, po2, zs2, zr2, acc2, ta2, tb2, tc2, td2,
    sb3, rb3, po3, zs3, zr3,
    wsem, tsend, trecv, gsend, grecv,
    ag_s, ag_r, ry_s, ry_r, rz_s, rz_r, hy_s, h_r, tp_s, tp_r, xs_s, xs_r, hx_s, hx_r,
    sy_s, sy_r, sz_s, sz_r, st_s, st_r,
):
    g, r, t = lax.axis_index("grp"), lax.axis_index("rep"), lax.axis_index("tp")
    y, zh = lax.div(r, 2), lax.rem(r, 2)
    zl, core = lax.div(t, 2), lax.rem(t, 2)
    is_late, is_early = g >= 2, g < 2
    is_2, is_3 = g == 2, g == 3
    late = is_late.astype(jnp.int32)
    quart = late
    low = lax.rem(g, 2)
    half = low + late - 2 * low * late
    g_pair = 3 - g
    g_near = g + 1 - 2 * low
    qrow = pl.multiple_of(quart * QUARTER, QUARTER)
    sends = []

    def dev(gg=None, rr=None, tt=None):
        return (g if gg is None else gg, r if rr is None else rr, t if tt is None else tt)

    def remote(src, dst, ssem, rsem, to, when=None):
        cp = pltpu.make_async_remote_copy(
            src_ref=src, dst_ref=dst, send_sem=ssem, recv_sem=rsem, device_id=to, device_id_type=MESH
        )
        if when is None:
            cp.start()
        else:
            pl.when(when)(cp.start)
        sends.append((cp, when))
        return cp

    near = dev(gg=g_near)

    def wait_recv(dst, rsem, when=None):
        cp = pltpu.make_async_remote_copy(
            src_ref=dst, dst_ref=dst, send_sem=rsem, recv_sem=rsem, device_id=dev(), device_id_type=MESH
        )
        if when is None:
            cp.wait_recv()
        else:
            pl.when(when)(cp.wait_recv)

    own = pl.ds(pl.multiple_of(half * HALF + quart * QUARTER, QUARTER), QUARTER)
    pair = pl.ds(pl.multiple_of(half * HALF + (1 - quart) * QUARTER, QUARTER), QUARTER)
    mine = pl.ds(pl.multiple_of(half * HALF, HALF), HALF)
    other = pl.ds(pl.multiple_of((1 - half) * HALF, HALF), HALF)
    inputs = [
        pltpu.make_async_copy(noise_hbm.at[own, :], noise, isem.at[0]),
        pltpu.make_async_copy(renoise_hbm.at[mine, :], renoise, isem.at[1]),
        pltpu.make_async_copy(gains_hbm.at[:, pl.ds(pl.multiple_of(r * FEAT, LANES), FEAT)], gain, isem.at[2]),
    ]

    model = 1 + late
    loads = [
        pltpu.make_async_copy(up_hbm.at[0], upw.at[0], wsem.at[0]),
        pltpu.make_async_copy(down_hbm.at[0], dnw.at[0], wsem.at[1]),
        pltpu.make_async_copy(up_hbm.at[model], upw.at[1], wsem.at[2]),
        pltpu.make_async_copy(down_hbm.at[model], dnw.at[1], wsem.at[3]),
    ]
    barrier = pltpu.get_barrier_semaphore()
    sibling = dev(tt=2 * zl + 1 - core)
    flip = dev(rr=t, tt=r)
    off_diag = r != t
    row_peer = lambda yy: dev(rr=2 * yy + zh)
    z_peer = dev(rr=2 * y + 1 - zh)
    peers = [sibling, z_peer, dev(gg=g_pair), dev(gg=g_near)]
    peers += [dev(tt=2 * lax.rem(zl + d, 4) + core) for d in range(1, 4)]
    peers += [row_peer(lax.rem(y + j, 4)) for j in range(1, 4)]
    for peer in peers:
        pl.semaphore_signal(barrier, inc=1, device_id=peer, device_id_type=MESH)

    for cp in inputs + loads:
        cp.start()

    cond_row = cond_in[0:1, pl.ds(pl.multiple_of(t * FEAT, LANES), FEAT)].astype(F32)
    t_all = jnp.full((16, FEAT), t_in[0], jnp.int32)
    row = lax.broadcasted_iota(jnp.int32, (16, FEAT), 0)
    lane = lax.broadcasted_iota(jnp.int32, (16, FEAT), 1)
    t_part = jnp.where(lane < LANES, t_all >> 8, t_all & 255).astype(F32)
    msgc[...] = jnp.where(row < 8, jnp.broadcast_to(cond_row, (16, FEAT)), t_part).astype(BF)

    @pl.when(off_diag)
    def _():
        pl.semaphore_signal(barrier, inc=1, device_id=flip, device_id_type=MESH)
        pl.semaphore_wait(barrier, len(peers) + 1)

    @pl.when(jnp.logical_not(off_diag))
    def _():
        pl.semaphore_wait(barrier, len(peers))

    for cp in inputs:
        cp.wait()
    remote(noise, xt, tsend.at[0], trecv.at[0], flip, when=off_diag)
    remote(msgc, ct, tsend.at[1], trecv.at[1], flip, when=off_diag)
    remote(renoise, rt, tsend.at[2], trecv.at[2], flip, when=off_diag)

    @pl.when(jnp.logical_not(off_diag))
    def _():
        xt[...] = noise[...]
        ct[...] = msgc[...]
        rt[...] = renoise[...]

    wait_recv(xt, trecv.at[0], off_diag)
    wait_recv(ct, trecv.at[1], off_diag)
    cond1 = 1.0 + ct[0:1, :].astype(F32)

    def gather_tp(phase, block_of):
        remote(block_of(t), block_of(t), ag_s.at[phase, 0], ag_r.at[phase, t], sibling)
        for d in (2, 1, 3):
            to = dev(tt=2 * lax.rem(zl + d, 4) + core)
            remote(block_of(t), block_of(t), ag_s.at[phase, d], ag_r.at[phase, t], to)

    def wait_chip(phase, block_of, d):
        yy = lax.rem(zl + d, 4)
        if d:
            b = 2 * yy + core
            wait_recv(block_of(b), ag_r.at[phase, b])
            remote(block_of(b), block_of(b), ag_s.at[phase, 3 + d], ag_r.at[phase, b], sibling)
        b = 2 * yy + 1 - core
        wait_recv(block_of(b), ag_r.at[phase, b])

    def scalar_start(phase, lanes):
        sc_own[phase] = jnp.broadcast_to(lanes, (8, LANES))
        for j in (2, 1, 3):
            remote(
                sc_own.at[phase], sc_row.at[phase, y], sy_s.at[phase, j], sy_r.at[phase, y],
                row_peer(lax.rem(y + j, 4)),
            )

    def scalar_to_z(phase):
        total = sc_own[phase]
        for j in (1, 3, 2):
            yy = lax.rem(y + j, 4)
            wait_recv(sc_row.at[phase, yy], sy_r.at[phase, yy])
            total += sc_row[phase, yy]
        sc_zs[phase] = total
        remote(sc_zs.at[phase], sc_zr.at[phase], sz_s.at[phase], sz_r.at[phase], z_peer)

    def scalar_to_tp(phase):
        wait_recv(sc_zr.at[phase], sz_r.at[phase])
        sc_all[phase, t] = sc_zs[phase] + sc_zr[phase]
        tile = sc_all.at[phase, t]
        remote(tile, tile, st_s.at[phase, 0], st_r.at[phase, t], sibling)
        for d in (2, 1, 3):
            remote(tile, tile, st_s.at[phase, d], st_r.at[phase, t], dev(tt=2 * lax.rem(zl + d, 4) + core))

    def scalar_end(phase):
        for d in (1, 3, 2):
            b = 2 * lax.rem(zl + d, 4) + core
            tile = sc_all.at[phase, b]
            wait_recv(tile, st_r.at[phase, b])
            remote(tile, tile, st_s.at[phase, 3 + d], st_r.at[phase, b], sibling)
        for d in range(4):
            b = 2 * lax.rem(zl + d, 4) + 1 - core
            wait_recv(sc_all.at[phase, b], st_r.at[phase, b])

    def reduce_rep(phase, n, rows_of, block_of, product, bufs, finish, gathered, sent, after):
        sb, rb, po, zs, zr = bufs
        span = lambda c: pl.ds(c * HC, HC)
        for c in range(CHUNKS):
            lo = c * HC
            for d in (0, 1, 3, 2):
                yy = lax.rem(zl + d, 4)
                if c == 0:
                    wait_chip(phase, block_of, d)
                part = product(rows_of(yy), c)

                @pl.when(yy == y)
                def _():
                    po[:, lo : lo + HC] = part

                @pl.when(yy != y)
                def _():
                    sb[yy, :, lo : lo + HC] = part.astype(BF)

                remote(
                    sb.at[yy, :, span(c)], rb.at[y, :, span(c)], ry_s.at[phase, c, d], ry_r.at[phase, c, y],
                    row_peer(yy), when=yy != y,
                )
                if c == 0 and d == 1:
                    scalar_to_z(phase)
            if c == 0:
                gathered()
        scalar_to_tp(phase)
        sent()

        def to_z(c):
            lo = c * HC
            total = po[:, lo : lo + HC]
            for j in (1, 3, 2):
                yy = lax.rem(y + j, 4)
                wait_recv(rb.at[yy, :, span(c)], ry_r.at[phase, c, yy])
                total += rb[yy, :, lo : lo + HC].astype(F32)
            po[:, lo : lo + HC] = total
            zs[:, lo : lo + HC] = total.astype(BF)
            remote(zs.at[:, span(c)], zr.at[:, span(c)], rz_s.at[phase, c], rz_r.at[phase, c], z_peer)

        def from_z(c):
            lo = c * HC
            if c == 0:
                scalar_end(phase)
            wait_recv(zr.at[:, span(c)], rz_r.at[phase, c])
            finish(c, po[:, lo : lo + HC] + zr[:, lo : lo + HC].astype(F32))

        early = n == HALF
        for c in range(CHUNKS):
            if early and c == CHUNKS - 1:
                from_z(0)
            to_z(c)
        for c in range(1 if early else 0, CHUNKS):
            from_z(c)
            if c >= 2:
                after(c - 2)
        for c in (CHUNKS - 2, CHUNKS - 1):
            after(c)

    def forward(phase, n, x_rows, gain_row, xg, xg_rows, h, h_rows, bufs, gathered):
        acc, ta, tb, tc, td = bufs[5:]
        up, down, grad = upw.at[phase], dnw.at[phase], gd.at[phase]
        xg[t, xg_rows, :] = (x_rows * (gain_row * cond1)).astype(BF)
        block_of = lambda b: xg.at[b, xg_rows, :]
        gather_tp(phase, block_of)
        scalar_start(phase, to_lanes(jnp.sum(x_rows * x_rows, axis=1, keepdims=True)))
        rows_of = lambda yy: xg[pl.ds(2 * yy, 2), xg_rows, :].reshape(2 * n, FEAT)
        loads[2 * phase].wait()

        def product(rows, c):
            return jnp.dot(rows, up[:, c * HC : (c + 1) * HC], preferred_element_type=F32)

        piece = lambda yy, c: h.at[pl.ds(2 * yy, 2), h_rows, pl.ds(c * HC, HC)]

        state = {}
        relayed = n == HALF

        def pass_on(c):
            behind, ahead = lax.rem(y + (1 if c % 2 else 3), 4), lax.rem(y + (3 if c % 2 else 1), 4)
            passed = piece(behind, c)
            wait_recv(passed, h_r.at[phase, c, behind])
            remote(passed, passed, hy_s.at[phase, c, 2], h_r.at[phase, c, behind], row_peer(ahead))
            remote(passed, passed, hx_s.at[c, 1 if c % 2 else 3], hx_r.at[c, behind], near, when=is_2)

        def finish(c, a):
            if c == 0:
                squares = [to_column(sc_all[phase, 2 * y + k, 0:1, :], n) for k in range(2)]
                state["factor"] = lax.rsqrt(jnp.concatenate(squares, axis=0) * (1.0 / D_ALL) + 1e-6)
            factor = state["factor"]
            hidden, slope = gelu_both(a * factor)
            cols = slice(c * HC, (c + 1) * HC)
            h[pl.ds(2 * y, 2), h_rows, cols] = hidden.astype(BF).reshape(2, n, HC)
            for j in (1, 3) if relayed else (2, 1, 3):
                remote(
                    piece(y, c), piece(y, c), hy_s.at[phase, c, j], h_r.at[phase, c, y],
                    row_peer(lax.rem(y + j, 4)),
                )
            remote(piece(y, c), piece(y, c), hx_s.at[c, 0], hx_r.at[c, y], near, when=is_2) if relayed else None
            grad[:, h_rows, cols] = (slope * factor).astype(BF).reshape(2, n, HC)

        def project(c):
            if c == 0:
                loads[2 * phase + 1].wait()
            cols = slice(c * HC, (c + 1) * HC)
            for j in (0, 1, 3, 2):
                yy = lax.rem(y + j, 4)
                if j and not (relayed and j == (1 if c % 2 else 3)):
                    wait_recv(piece(yy, c), h_r.at[phase, c, yy])
                    if relayed:
                        remote(piece(yy, c), piece(yy, c), hx_s.at[c, j], hx_r.at[c, yy], near, when=is_2)
                both = h[pl.ds(2 * yy, 2), h_rows, cols].reshape(2 * n, HC)
                part = jnp.dot(both, down[cols, :], preferred_element_type=F32).reshape(2, n, FEAT)
                if c:
                    part += acc[pl.ds(2 * yy, 2)]
                acc[pl.ds(2 * yy, 2)] = part
                if c == CHUNKS - 1:
                    ta[yy] = acc[2 * yy + 1 - core].astype(BF)
                    remote(ta.at[yy], tb.at[yy], tp_s.at[phase, yy], tp_r.at[phase, yy], sibling)

        def after(c):
            if relayed:
                pass_on(c)
                if c:
                    project(c - 1)

        reduce_rep(phase, n, rows_of, block_of, product, bufs[:5], finish, gathered, lambda: None, after)
        for c in range(CHUNKS - 1 if relayed else 0, CHUNKS):
            project(c)
        total = None
        for d in (2, 1, 3, 0):
            yy = lax.rem(zl + d, 4)
            wait_recv(tb.at[yy], tp_r.at[phase, yy])
            both = acc[2 * yy + core] + tb[yy].astype(F32)
            if d:
                tc[d - 1] = both.astype(BF)
                remote(
                    tc.at[d - 1], td.at[d - 1], tp_s.at[phase, 3 + d], tp_r.at[phase, 3 + d],
                    dev(tt=2 * yy + core),
                )
            else:
                total = both
        for d in (1, 3, 2):
            wait_recv(td.at[d - 1], tp_r.at[phase, 3 + d])
            total += td[d - 1].astype(F32)
        return total

    x0 = xt[...].astype(F32)
    q_rows = pl.ds(qrow, QUARTER)
    out = forward(
        0, QUARTER, x0, gain[0:1, :], xgs, q_rows, hs, q_rows,
        (sb1, rb1, po1, zs1, zr1, acc1, ta1, tb1, tc1, td1), lambda: None,
    )
    gen[own, :] = (x0 + out).astype(BF)
    remote(gen.at[own, :], gen.at[own, :], gsend.at[0], grecv.at[0], dev(gg=g_pair))
    for i, ref in enumerate((gd.at[0, :, q_rows, :], xgs.at[:, q_rows, :], hs.at[:, q_rows, :])):
        remote(ref, ref, gsend.at[1 + i], grecv.at[1 + i], dev(gg=g_pair), when=is_late)
    wait_recv(rt, trecv.at[2], off_diag)
    t_row = ct[8:9, :].astype(F32)
    sigma = 0.1 + 0.8 * (t_row[:, 0:1] * 256.0 + t_row[:, LANES : LANES + 1]) / 999.0
    wait_recv(gen.at[pair, :], grecv.at[0])
    remote(gen.at[mine, :], gen.at[mine, :], gsend.at[4], grecv.at[4], dev(gg=g_near))

    gen_f = gen[mine, :].astype(F32)
    x_t = ((1.0 - sigma) * gen_f + sigma * rt[...].astype(F32)).astype(BF).astype(F32)
    all_rows = pl.ds(0, HALF)
    xgf_2 = xgf.at[1]

    def inputs_here():
        wait_recv(gen.at[other, :], grecv.at[4])
        remote(gen, gout, tsend.at[3], trecv.at[3], flip, when=off_diag)
        remote(xgf_2, xgf_2, gsend.at[5], grecv.at[5], near, when=is_2)

    gain_row = jnp.where(is_late, gain[2:3, :], gain[1:2, :])
    out = forward(
        1, HALF, x_t, gain_row, xgf.at[half], all_rows, hf.at[half], all_rows,
        (sb2, rb2, po2, zs2, zr2, acc2, ta2, tb2, tc2, td2),
        inputs_here,
    )
    fk[...] = (x_t + out).astype(BF)
    remote(fk, fother, gsend.at[6], grecv.at[6], dev(gg=g_pair), when=is_late)

    scale = 1.0 / math.sqrt(TOKENS)
    dy = dyb.at[half]

    @pl.when(is_late)
    def _():
        dy[t] = ((fk[...].astype(F32) - gen_f) * scale).astype(BF)
        dmine[...] = jnp.zeros_like(dmine)

    @pl.when(is_early)
    def _():
        real = fk[...].astype(F32)
        distance = jnp.sum(jnp.sum(jnp.abs(gen_f - real), axis=1, keepdims=True), axis=0, keepdims=True)
        dmine[0] = jnp.broadcast_to(distance, (8, LANES))
        cp = pltpu.make_async_remote_copy(
            src_ref=dmine.at[0], dst_ref=dmine.at[1], send_sem=gsend.at[7], recv_sem=grecv.at[7],
            device_id=near, device_id_type=MESH,
        )
        cp.start()
        wait_recv(fother, grecv.at[6])
        dy[t] = ((fother[...].astype(F32) - real) * scale).astype(BF)
        cp.wait()

    dy_block = lambda b: dy.at[b]
    gather_tp(2, dy_block)
    scalar_start(2, dmine[0, 0:1, :] + dmine[1, 0:1, :])

    da = dab.at[half]
    back = dnw.at[late]
    slope = gd.at[late]

    def product(rows, c):
        return lax.dot_general(
            rows, back[c * HC : (c + 1) * HC, :], (((1,), (1,)), ((), ())), preferred_element_type=F32
        )

    def da_piece(buf, yy, c):
        return buf.at[pl.ds(2 * yy, 2), :, pl.ds(c * HC, HC)]

    def image_scale(b):
        norm = sc_all[2, b, 0:1, 0:1] * (1.0 / (IMG_TOK * D_ALL)) + 1e-5
        return jnp.where(is_late, 1.0, 1.0 / norm)

    wait_recv(gd.at[0, :, pl.ds(QUARTER, QUARTER), :], grecv.at[1], is_early)
    not_2 = g != 2
    da_2 = dab.at[1]

    def pass_on(c):
        behind, ahead = lax.rem(y + (1 if c % 2 else 3), 4), lax.rem(y + (3 if c % 2 else 1), 4)
        passed = da_piece(da, behind, c)
        wait_recv(passed, h_r.at[2, c, behind], not_2)
        remote(passed, passed, hy_s.at[2, c, 0], h_r.at[2, c, behind], row_peer(ahead), when=not_2)
        last = c == CHUNKS - 1
        for j in (1, 3, 2) if last else (2,):
            pair_2 = lax.rem(y + j, 4)
            crossing = da_piece(da_2, pair_2, c)
            wait_recv(crossing, h_r.at[2, c, pair_2], is_2)
            remote(crossing, crossing, xs_s.at[c, j], xs_r.at[c, pair_2], near, when=is_2)
        wait_recv(da_piece(da_2, y, c), xs_r.at[c, y], is_3)
        if not last:
            for j in (1, 3):
                remote(
                    da_piece(da_2, y, c), da_piece(da_2, y, c), xs_s.at[c, 3 + j], xs_r.at[c, y],
                    row_peer(lax.rem(y + j, 4)), when=is_3,
                )

    row_state = {}

    def finish(c, dh):
        if c == 0:
            scales = [jnp.broadcast_to(image_scale(2 * y + k), (HALF, 1)) for k in range(2)]
            row_state["scale"] = jnp.concatenate(scales, axis=0)
        cols = slice(c * HC, (c + 1) * HC)
        slopes = slope[:, :, cols].reshape(2 * HALF, HC).astype(F32)
        da[pl.ds(2 * y, 2), :, cols] = (dh * row_state["scale"] * slopes).astype(BF).reshape(2, HALF, HC)
        own_piece = da_piece(da, y, c)
        remote(own_piece, own_piece, xs_s.at[c, 0], xs_r.at[c, y], near, when=is_2)
        for j in (2, 1, 3):
            remote(
                own_piece, own_piece, hy_s.at[2, c, j], h_r.at[2, c, y], row_peer(lax.rem(y + j, 4)),
                when=is_2 if j == 2 else None if c == CHUNKS - 1 else not_2,
            )

    dyb_2 = dyb.at[1]
    n_half, n_all = BLOCKS * HALF, 2 * BLOCKS * HALF

    def turned():
        @pl.when(is_early)
        def _():
            wait_recv(xgs_other, grecv.at[2])
            for k in range(BLOCKS // 2):
                two = xgs[2 * k : 2 * k + 2].reshape(2 * HALF, FEAT)
                ut[:, k * LANES : (k + 1) * LANES] = two.T

        @pl.when(is_3)
        def _():
            wait_recv(xgf_2, grecv.at[5])
            for k in range(BLOCKS):
                two = xgf[k // 4, 2 * (k % 4) : 2 * (k % 4) + 2].reshape(2 * HALF, FEAT)
                ut[:, k * LANES : (k + 1) * LANES] = two.T

    tn = (((0,), (0,)), ((), ()))
    step = 256

    def down_tiles(first, last):
        for i in range(first, last):
            cols = slice(i * step, (i + 1) * step)

            @pl.when(is_early)
            def _():
                dng_out[cols, :] = lax.dot_general(
                    hs[:, :, cols].reshape(n_half, step), dys[...].reshape(n_half, FEAT), tn,
                    preferred_element_type=F32,
                ).astype(BF)

            @pl.when(is_3)
            def _():
                dng_out[cols, :] = lax.dot_general(
                    hf[:, :, :, cols].reshape(n_all, step), dyb[...].reshape(n_all, FEAT), tn,
                    preferred_element_type=F32,
                ).astype(BF)

    def after(c):
        pass_on(c)
        if c == 0:

            @pl.when(is_early)
            def _():
                wait_recv(hs_other, grecv.at[3])
                for b in range(BLOCKS):
                    dys[b] = (dy[b].astype(F32) * image_scale(b)).astype(BF)

            @pl.when(is_3)
            def _():
                for k in range(CHUNKS):
                    for yy in range(4):
                        wait_recv(hf.at[1, 2 * yy : 2 * yy + 2, :, pl.ds(k * HC, HC)], hx_r.at[k, yy])
                wait_recv(dyb_2, grecv.at[8])

        if c < 3:
            down_tiles(2 * c, 2 * c + 2)

    xgs_other, hs_other = xgs.at[:, pl.ds(QUARTER, QUARTER), :], hs.at[:, pl.ds(QUARTER, QUARTER), :]
    reduce_rep(
        2, HALF, lambda yy: dy[pl.ds(2 * yy, 2)].reshape(2 * HALF, FEAT), dy_block, product,
        (sb3, rb3, po3, zs3, zr3), finish,
        lambda: remote(dyb_2, dyb_2, gsend.at[8], grecv.at[8], near, when=is_2), turned, after,
    )

    outs = [pltpu.make_async_copy(gout, gen_hbm, osem.at[0]), pltpu.make_async_copy(dng_out, dng_hbm, osem.at[1])]
    wait_recv(gout, trecv.at[3], off_diag)

    @pl.when(jnp.logical_not(off_diag))
    def _():
        gout[...] = gen[...]

    @pl.when(is_2)
    def _():
        upg_out[...] = jnp.zeros_like(upg_out)
        dng_out[...] = jnp.zeros_like(dng_out)

    outs[0].start()
    outs[1].start()
    for c in range(CHUNKS):
        cols = slice(c * HC, (c + 1) * HC)
        for j in (1, 3, 2):
            yy = lax.rem(y + j, 4)
            if j != (1 if c % 2 else 3):
                wait_recv(da_piece(da, yy, c), h_r.at[2, c, yy], not_2)
            wait_recv(da_piece(da_2, yy, c), xs_r.at[c, yy], is_3)

        @pl.when(is_early)
        def _():
            upg_out[:, cols] = jnp.dot(
                ut[:, :n_half], da[:, :, cols].reshape(n_half, HC), preferred_element_type=F32
            ).astype(BF)

        @pl.when(is_3)
        def _():
            upg_out[:, cols] = jnp.dot(
                ut[...], dab[:, :, :, cols].reshape(n_all, HC), preferred_element_type=F32
            ).astype(BF)

        outs.append(pltpu.make_async_copy(upg_out.at[:, cols], upg_hbm.at[:, cols], osem.at[2 + c]))
        outs[-1].start()

    for cp, when in sends:
        if when is None:
            cp.wait_send()
        else:
            pl.when(when)(cp.wait_send)
    for cp in outs:
        cp.wait()


def widen(gen, up, down, gen_out, up_out, down_out):
    gen_out[...] = gen[...]
    up_out[0] = up[...].astype(F32)
    down_out[0] = down[...].astype(F32)


def rep_buffers(n):
    return [
        pltpu.VMEM((4, 2 * n, HID), BF),
        pltpu.VMEM((4, 2 * n, HID), BF),
        pltpu.VMEM((2 * n, HID), F32),
        pltpu.VMEM((2 * n, HID), BF),
        pltpu.VMEM((2 * n, HID), BF),
    ]


def tp_buffers(n):
    return [
        pltpu.VMEM((BLOCKS, n, FEAT), F32),
        pltpu.VMEM((4, n, FEAT), BF),
        pltpu.VMEM((4, n, FEAT), BF),
        pltpu.VMEM((3, n, FEAT), BF),
        pltpu.VMEM((3, n, FEAT), BF),
    ]


def body(noise_in, noise_renoise, text_cond, t_index, gains, up_weights, down_weights):
    vmem = pl.BlockSpec(memory_space=pltpu.VMEM)
    smem = pl.BlockSpec(memory_space=pltpu.SMEM)
    hbm = pl.BlockSpec(memory_space=pl.ANY)
    dma = pltpu.SemaphoreType.DMA
    generated, up_grad, down_grad = pl.pallas_call(
        kernel,
        name="step",
        out_shape=(
            jax.ShapeDtypeStruct((IMG_TOK, FEAT), BF),
            jax.ShapeDtypeStruct((FEAT, HID), BF),
            jax.ShapeDtypeStruct((HID, FEAT), BF),
        ),
        in_specs=[hbm, hbm, vmem, smem, hbm, hbm, hbm],
        out_specs=(hbm, hbm, hbm),
        scratch_shapes=[
            pltpu.VMEM((QUARTER, FEAT), BF),
            pltpu.VMEM((HALF, FEAT), BF),
            pltpu.VMEM((3, FEAT), F32),
            pltpu.VMEM((FEAT, HID), BF),
            pltpu.VMEM((HID, FEAT), BF),
            dma((3,)),
            dma((2 + CHUNKS,)),
            pltpu.VMEM((16, FEAT), BF),
            pltpu.VMEM((QUARTER, FEAT), BF),
            pltpu.VMEM((16, FEAT), BF),
            pltpu.VMEM((HALF, FEAT), BF),
            pltpu.VMEM((IMG_TOK, FEAT), BF),
            pltpu.VMEM((IMG_TOK, FEAT), BF),
            pltpu.VMEM((HALF, FEAT), BF),
            pltpu.VMEM((HALF, FEAT), BF),
            pltpu.VMEM((2, 8, LANES), F32),
            pltpu.VMEM((2, FEAT, HID), BF),
            pltpu.VMEM((2, HID, FEAT), BF),
            pltpu.VMEM((BLOCKS, HALF, FEAT), BF),
            pltpu.VMEM((BLOCKS, HALF, HID), BF),
            pltpu.VMEM((2, BLOCKS, HALF, FEAT), BF),
            pltpu.VMEM((2, BLOCKS, HALF, HID), BF),
            pltpu.VMEM((2, BLOCKS, HALF, FEAT), BF),
            pltpu.VMEM((2, BLOCKS, HALF, HID), BF),
            pltpu.VMEM((2, 2, HALF, HID), BF),
            pltpu.VMEM((BLOCKS, HALF, FEAT), BF),
            pltpu.VMEM((FEAT, 2 * BLOCKS * HALF), BF),
            pltpu.VMEM((3, 8, LANES), F32),
            pltpu.VMEM((3, 4, 8, LANES), F32),
            pltpu.VMEM((3, 8, LANES), F32),
            pltpu.VMEM((3, 8, LANES), F32),
            pltpu.VMEM((3, BLOCKS, 8, LANES), F32),
            *rep_buffers(QUARTER),
            *tp_buffers(QUARTER),
            *rep_buffers(HALF),
            *tp_buffers(HALF),
            *rep_buffers(HALF),
            dma((4,)),
            dma((4,)),
            dma((4,)),
            dma((10,)),
            dma((10,)),
            dma((3, 7)),
            dma((3, 8)),
            dma((3, CHUNKS, 4)),
            dma((3, CHUNKS, 4)),
            dma((3, CHUNKS)),
            dma((3, CHUNKS)),
            dma((3, CHUNKS, 4)),
            dma((3, CHUNKS, 4)),
            dma((2, 7)),
            dma((2, 7)),
            dma((CHUNKS, 7)),
            dma((CHUNKS, 4)),
            dma((CHUNKS, 4)),
            dma((CHUNKS, 4)),
            dma((3, 4)),
            dma((3, 4)),
            dma((3,)),
            dma((3,)),
            dma((3, 7)),
            dma((3, 8)),
        ],
        compiler_params=pltpu.CompilerParams(
            collective_id=0, has_side_effects=True, vmem_limit_bytes=60 * 2**20
        ),
    )(noise_in, noise_renoise, text_cond, t_index, gains, up_weights, down_weights)
    parts = 4
    rows = [
        pl.BlockSpec((IMG_TOK // parts, FEAT), lambda i: (i, 0)),
        pl.BlockSpec((FEAT // parts, HID), lambda i: (i, 0)),
        pl.BlockSpec((HID // parts, FEAT), lambda i: (i, 0)),
    ]
    wide = [
        rows[0],
        pl.BlockSpec((1, FEAT // parts, HID), lambda i: (0, i, 0)),
        pl.BlockSpec((1, HID // parts, FEAT), lambda i: (0, i, 0)),
    ]
    return pl.pallas_call(
        widen,
        name="widen",
        grid=(parts,),
        out_shape=(
            jax.ShapeDtypeStruct((IMG_TOK, FEAT), BF),
            jax.ShapeDtypeStruct((1, FEAT, HID), F32),
            jax.ShapeDtypeStruct((1, HID, FEAT), F32),
        ),
        in_specs=rows,
        out_specs=wide,
    )(generated, up_grad, down_grad)


def solution(mesh):
    in_specs = (
        P("rep", "tp"),
        P("rep", "tp"),
        P("rep", None),
        P("rep"),
        P(),
        P(None, "rep", "tp"),
        P(None, "tp", "rep"),
    )
    out_specs = (P("rep", "tp"), P("grp", "rep", "tp"), P("grp", "tp", "rep"))
    return jax.shard_map(body, mesh=mesh, in_specs=in_specs, out_specs=out_specs, check_vma=False)
```

```python
import functools
import math

import jax
import jax.numpy as jnp
from jax import lax
from jax.experimental import pallas as pl
from jax.experimental.pallas import tpu as pltpu
from jax.sharding import PartitionSpec as P

MESH = pl.DeviceIdType.MESH
BF = jnp.bfloat16
F32 = jnp.float32
FEAT = 384
HID = 1536
LANES = 128
CHUNKS = 6
HC = HID // CHUNKS
BLOCKS = 8
HALF = 64
QUARTER = 32
IMG_TOK = 128
D_ALL = 3072
TOKENS = 1024
GELU_C = math.sqrt(2.0 / math.pi)


def diagonal(n):
    return lax.broadcasted_iota(jnp.int32, (n, LANES), 0) == lax.broadcasted_iota(jnp.int32, (n, LANES), 1)


def to_lanes(column):
    return jnp.sum(jnp.where(diagonal(column.shape[0]), column, 0.0), axis=0, keepdims=True)


def to_column(lanes, n):
    return jnp.sum(jnp.where(diagonal(n), lanes, 0.0), axis=1, keepdims=True)


def gelu_both(a):
    a2 = a * a
    th = jnp.tanh(GELU_C * a * (1.0 + 0.044715 * a2))
    half = 0.5 * (1.0 + th)
    grad = half + 0.5 * a * (1.0 - th * th) * (GELU_C * (1.0 + 3.0 * 0.044715 * a2))
    return a * half, grad


def kernel(
    noise_hbm, renoise_hbm, cond_in, t_in, gains_hbm, up_hbm, down_hbm,
    gen_hbm, upg_hbm, dng_hbm,
    noise, renoise, gain, upg_out, dng_out, isem, osem,
    msgc, xt, ct, rt, gen, gout, fk, fother, dmine,
    upw, dnw, xgs, hs, xgf, hf, dyb, dab, gd, dys, ut,
    sc_own, sc_row, sc_zs, sc_zr, sc_all,
    sb1, rb1, po1, zs1, zr1, acc1, ta1, tb1, tc1, td1,
    sb2, rb2, po2, zs2, zr2, acc2, ta2, tb2, tc2, td2,
    sb3, rb3, po3, zs3, zr3,
    wsem, tsend, trecv, gsend, grecv,
    ag_s, ag_r, ry_s, ry_r, rz_s, rz_r, hy_s, h_r, tp_s, tp_r, xs_s, xs_r, hx_s, hx_r,
    sy_s, sy_r, sz_s, sz_r, st_s, st_r,
):
    g, r, t = lax.axis_index("grp"), lax.axis_index("rep"), lax.axis_index("tp")
    y, zh = lax.div(r, 2), lax.rem(r, 2)
    zl, core = lax.div(t, 2), lax.rem(t, 2)
    is_late, is_early = g >= 2, g < 2
    is_2, is_3 = g == 2, g == 3
    late = is_late.astype(jnp.int32)
    quart = late
    low = lax.rem(g, 2)
    half = low + late - 2 * low * late
    g_pair = 3 - g
    g_near = g + 1 - 2 * low
    qrow = pl.multiple_of(quart * QUARTER, QUARTER)
    sends = []

    def dev(gg=None, rr=None, tt=None):
        return (g if gg is None else gg, r if rr is None else rr, t if tt is None else tt)

    def remote(src, dst, ssem, rsem, to, when=None):
        cp = pltpu.make_async_remote_copy(
            src_ref=src, dst_ref=dst, send_sem=ssem, recv_sem=rsem, device_id=to, device_id_type=MESH
        )
        if when is None:
            cp.start()
        else:
            pl.when(when)(cp.start)
        sends.append((cp, when))
        return cp

    near = dev(gg=g_near)

    def wait_recv(dst, rsem, when=None):
        cp = pltpu.make_async_remote_copy(
            src_ref=dst, dst_ref=dst, send_sem=rsem, recv_sem=rsem, device_id=dev(), device_id_type=MESH
        )
        if when is None:
            cp.wait_recv()
        else:
            pl.when(when)(cp.wait_recv)

    own = pl.ds(pl.multiple_of(half * HALF + quart * QUARTER, QUARTER), QUARTER)
    pair = pl.ds(pl.multiple_of(half * HALF + (1 - quart) * QUARTER, QUARTER), QUARTER)
    mine = pl.ds(pl.multiple_of(half * HALF, HALF), HALF)
    other = pl.ds(pl.multiple_of((1 - half) * HALF, HALF), HALF)
    inputs = [
        pltpu.make_async_copy(noise_hbm.at[own, :], noise, isem.at[0]),
        pltpu.make_async_copy(renoise_hbm.at[mine, :], renoise, isem.at[1]),
        pltpu.make_async_copy(gains_hbm.at[:, pl.ds(pl.multiple_of(r * FEAT, LANES), FEAT)], gain, isem.at[2]),
    ]

    model = 1 + late
    loads = [
        pltpu.make_async_copy(up_hbm.at[0], upw.at[0], wsem.at[0]),
        pltpu.make_async_copy(down_hbm.at[0], dnw.at[0], wsem.at[1]),
        pltpu.make_async_copy(up_hbm.at[model], upw.at[1], wsem.at[2]),
        pltpu.make_async_copy(down_hbm.at[model], dnw.at[1], wsem.at[3]),
    ]
    barrier = pltpu.get_barrier_semaphore()
    sibling = dev(tt=2 * zl + 1 - core)
    flip = dev(rr=t, tt=r)
    off_diag = r != t
    row_peer = lambda yy: dev(rr=2 * yy + zh)
    z_peer = dev(rr=2 * y + 1 - zh)
    peers = [sibling, z_peer, dev(gg=g_pair), dev(gg=g_near)]
    peers += [dev(tt=2 * lax.rem(zl + d, 4) + core) for d in range(1, 4)]
    peers += [row_peer(lax.rem(y + j, 4)) for j in range(1, 4)]
    for peer in peers:
        pl.semaphore_signal(barrier, inc=1, device_id=peer, device_id_type=MESH)

    for cp in inputs + loads:
        cp.start()

    cond_row = cond_in[0:1, pl.ds(pl.multiple_of(t * FEAT, LANES), FEAT)].astype(F32)
    t_all = jnp.full((16, FEAT), t_in[0], jnp.int32)
    row = lax.broadcasted_iota(jnp.int32, (16, FEAT), 0)
    lane = lax.broadcasted_iota(jnp.int32, (16, FEAT), 1)
    t_part = jnp.where(lane < LANES, t_all >> 8, t_all & 255).astype(F32)
    msgc[...] = jnp.where(row < 8, jnp.broadcast_to(cond_row, (16, FEAT)), t_part).astype(BF)

    @pl.when(off_diag)
    def _():
        pl.semaphore_signal(barrier, inc=1, device_id=flip, device_id_type=MESH)
        pl.semaphore_wait(barrier, len(peers) + 1)

    @pl.when(jnp.logical_not(off_diag))
    def _():
        pl.semaphore_wait(barrier, len(peers))

    for cp in inputs:
        cp.wait()
    remote(noise, xt, tsend.at[0], trecv.at[0], flip, when=off_diag)
    remote(msgc, ct, tsend.at[1], trecv.at[1], flip, when=off_diag)
    remote(renoise, rt, tsend.at[2], trecv.at[2], flip, when=off_diag)

    @pl.when(jnp.logical_not(off_diag))
    def _():
        xt[...] = noise[...]
        ct[...] = msgc[...]
        rt[...] = renoise[...]

    wait_recv(xt, trecv.at[0], off_diag)
    wait_recv(ct, trecv.at[1], off_diag)
    cond1 = 1.0 + ct[0:1, :].astype(F32)

    def gather_tp(phase, block_of):
        remote(block_of(t), block_of(t), ag_s.at[phase, 0], ag_r.at[phase, t], sibling)
        for d in (2, 1, 3):
            to = dev(tt=2 * lax.rem(zl + d, 4) + core)
            remote(block_of(t), block_of(t), ag_s.at[phase, d], ag_r.at[phase, t], to)

    def wait_chip(phase, block_of, d):
        yy = lax.rem(zl + d, 4)
        if d:
            b = 2 * yy + core
            wait_recv(block_of(b), ag_r.at[phase, b])
            remote(block_of(b), block_of(b), ag_s.at[phase, 3 + d], ag_r.at[phase, b], sibling)
        b = 2 * yy + 1 - core
        wait_recv(block_of(b), ag_r.at[phase, b])

    def scalar_start(phase, lanes):
        sc_own[phase] = jnp.broadcast_to(lanes, (8, LANES))
        for j in (2, 1, 3):
            remote(
                sc_own.at[phase], sc_row.at[phase, y], sy_s.at[phase, j], sy_r.at[phase, y],
                row_peer(lax.rem(y + j, 4)),
            )

    def scalar_to_z(phase):
        total = sc_own[phase]
        for j in (1, 3, 2):
            yy = lax.rem(y + j, 4)
            wait_recv(sc_row.at[phase, yy], sy_r.at[phase, yy])
            total += sc_row[phase, yy]
        sc_zs[phase] = total
        remote(sc_zs.at[phase], sc_zr.at[phase], sz_s.at[phase], sz_r.at[phase], z_peer)

    def scalar_to_tp(phase):
        wait_recv(sc_zr.at[phase], sz_r.at[phase])
        sc_all[phase, t] = sc_zs[phase] + sc_zr[phase]
        tile = sc_all.at[phase, t]
        remote(tile, tile, st_s.at[phase, 0], st_r.at[phase, t], sibling)
        for d in (2, 1, 3):
            remote(tile, tile, st_s.at[phase, d], st_r.at[phase, t], dev(tt=2 * lax.rem(zl + d, 4) + core))

    def scalar_end(phase):
        for d in (1, 3, 2):
            b = 2 * lax.rem(zl + d, 4) + core
            tile = sc_all.at[phase, b]
            wait_recv(tile, st_r.at[phase, b])
            remote(tile, tile, st_s.at[phase, 3 + d], st_r.at[phase, b], sibling)
        for d in range(4):
            b = 2 * lax.rem(zl + d, 4) + 1 - core
            wait_recv(sc_all.at[phase, b], st_r.at[phase, b])

    def reduce_rep(phase, n, rows_of, block_of, product, bufs, finish, gathered, sent, after):
        sb, rb, po, zs, zr = bufs
        span = lambda c: pl.ds(c * HC, HC)
        for c in range(CHUNKS):
            lo = c * HC
            for d in (0, 1, 3, 2):
                yy = lax.rem(zl + d, 4)
                if c == 0:
                    wait_chip(phase, block_of, d)
                part = product(rows_of(yy), c)

                @pl.when(yy == y)
                def _():
                    po[:, lo : lo + HC] = part

                @pl.when(yy != y)
                def _():
                    sb[yy, :, lo : lo + HC] = part.astype(BF)

                remote(
                    sb.at[yy, :, span(c)], rb.at[y, :, span(c)], ry_s.at[phase, c, d], ry_r.at[phase, c, y],
                    row_peer(yy), when=yy != y,
                )
                if c == 0 and d == 1:
                    scalar_to_z(phase)
            if c == 0:
                gathered()
        scalar_to_tp(phase)
        sent()

        def to_z(c):
            lo = c * HC
            total = po[:, lo : lo + HC]
            for j in (1, 3, 2):
                yy = lax.rem(y + j, 4)
                wait_recv(rb.at[yy, :, span(c)], ry_r.at[phase, c, yy])
                total += rb[yy, :, lo : lo + HC].astype(F32)
            po[:, lo : lo + HC] = total
            zs[:, lo : lo + HC] = total.astype(BF)
            remote(zs.at[:, span(c)], zr.at[:, span(c)], rz_s.at[phase, c], rz_r.at[phase, c], z_peer)

        def from_z(c):
            lo = c * HC
            if c == 0:
                scalar_end(phase)
            wait_recv(zr.at[:, span(c)], rz_r.at[phase, c])
            finish(c, po[:, lo : lo + HC] + zr[:, lo : lo + HC].astype(F32))

        early = n == HALF
        for c in range(CHUNKS):
            if early and c == CHUNKS - 1:
                from_z(0)
            to_z(c)
        for c in range(1 if early else 0, CHUNKS):
            from_z(c)
            if c >= 2:
                after(c - 2)
        for c in (CHUNKS - 2, CHUNKS - 1):
            after(c)

    def forward(phase, n, x_rows, gain_row, xg, xg_rows, h, h_rows, bufs, gathered):
        acc, ta, tb, tc, td = bufs[5:]
        up, down, grad = upw.at[phase], dnw.at[phase], gd.at[phase]
        xg[t, xg_rows, :] = (x_rows * (gain_row * cond1)).astype(BF)
        block_of = lambda b: xg.at[b, xg_rows, :]
        gather_tp(phase, block_of)
        scalar_start(phase, to_lanes(jnp.sum(x_rows * x_rows, axis=1, keepdims=True)))
        rows_of = lambda yy: xg[pl.ds(2 * yy, 2), xg_rows, :].reshape(2 * n, FEAT)
        loads[2 * phase].wait()

        def product(rows, c):
            return jnp.dot(rows, up[:, c * HC : (c + 1) * HC], preferred_element_type=F32)

        piece = lambda yy, c: h.at[pl.ds(2 * yy, 2), h_rows, pl.ds(c * HC, HC)]

        state = {}
        relayed = n == HALF
        passing = lambda c: relayed and c < CHUNKS - 2

        def pass_on(c):
            behind, ahead = lax.rem(y + (1 if c % 2 else 3), 4), lax.rem(y + (3 if c % 2 else 1), 4)
            passed = piece(behind, c)
            wait_recv(passed, h_r.at[phase, c, behind])
            remote(passed, passed, hy_s.at[phase, c, 2], h_r.at[phase, c, behind], row_peer(ahead))
            remote(passed, passed, hx_s.at[c, 1 if c % 2 else 3], hx_r.at[c, behind], near, when=is_2)

        def finish(c, a):
            if c == 0:
                squares = [to_column(sc_all[phase, 2 * y + k, 0:1, :], n) for k in range(2)]
                state["factor"] = lax.rsqrt(jnp.concatenate(squares, axis=0) * (1.0 / D_ALL) + 1e-6)
            factor = state["factor"]
            hidden, slope = gelu_both(a * factor)
            cols = slice(c * HC, (c + 1) * HC)
            h[pl.ds(2 * y, 2), h_rows, cols] = hidden.astype(BF).reshape(2, n, HC)
            for j in (1, 3) if passing(c) else (2, 1, 3):
                remote(
                    piece(y, c), piece(y, c), hy_s.at[phase, c, j], h_r.at[phase, c, y],
                    row_peer(lax.rem(y + j, 4)),
                )
            remote(piece(y, c), piece(y, c), hx_s.at[c, 0], hx_r.at[c, y], near, when=is_2) if relayed else None
            grad[:, h_rows, cols] = (slope * factor).astype(BF).reshape(2, n, HC)

        def project(c):
            if c == 0:
                loads[2 * phase + 1].wait()
            cols = slice(c * HC, (c + 1) * HC)
            for j in (0, 1, 3, 2):
                yy = lax.rem(y + j, 4)
                if j and not (passing(c) and j == (1 if c % 2 else 3)):
                    wait_recv(piece(yy, c), h_r.at[phase, c, yy])
                    if relayed:
                        remote(piece(yy, c), piece(yy, c), hx_s.at[c, j], hx_r.at[c, yy], near, when=is_2)
                both = h[pl.ds(2 * yy, 2), h_rows, cols].reshape(2 * n, HC)
                part = jnp.dot(both, down[cols, :], preferred_element_type=F32).reshape(2, n, FEAT)
                if c:
                    part += acc[pl.ds(2 * yy, 2)]
                acc[pl.ds(2 * yy, 2)] = part
                if c == CHUNKS - 1:
                    ta[yy] = acc[2 * yy + 1 - core].astype(BF)
                    remote(ta.at[yy], tb.at[yy], tp_s.at[phase, yy], tp_r.at[phase, yy], sibling)

        def after(c):
            if passing(c):
                pass_on(c)
            if relayed and c >= 3:
                project(c - 3)

        reduce_rep(phase, n, rows_of, block_of, product, bufs[:5], finish, gathered, lambda: None, after)
        for c in range(CHUNKS - 3 if relayed else 0, CHUNKS):
            project(c)
        total = None
        for d in (2, 1, 3, 0):
            yy = lax.rem(zl + d, 4)
            wait_recv(tb.at[yy], tp_r.at[phase, yy])
            both = acc[2 * yy + core] + tb[yy].astype(F32)
            if d:
                tc[d - 1] = both.astype(BF)
                remote(
                    tc.at[d - 1], td.at[d - 1], tp_s.at[phase, 3 + d], tp_r.at[phase, 3 + d],
                    dev(tt=2 * yy + core),
                )
            else:
                total = both
        for d in (1, 3, 2):
            wait_recv(td.at[d - 1], tp_r.at[phase, 3 + d])
            total += td[d - 1].astype(F32)
        return total

    x0 = xt[...].astype(F32)
    q_rows = pl.ds(qrow, QUARTER)
    out = forward(
        0, QUARTER, x0, gain[0:1, :], xgs, q_rows, hs, q_rows,
        (sb1, rb1, po1, zs1, zr1, acc1, ta1, tb1, tc1, td1), lambda: None,
    )
    gen[own, :] = (x0 + out).astype(BF)
    remote(gen.at[own, :], gen.at[own, :], gsend.at[0], grecv.at[0], dev(gg=g_pair))
    for i, ref in enumerate((gd.at[0, :, q_rows, :], xgs.at[:, q_rows, :], hs.at[:, q_rows, :])):
        remote(ref, ref, gsend.at[1 + i], grecv.at[1 + i], dev(gg=g_pair), when=is_late)
    wait_recv(rt, trecv.at[2], off_diag)
    t_row = ct[8:9, :].astype(F32)
    sigma = 0.1 + 0.8 * (t_row[:, 0:1] * 256.0 + t_row[:, LANES : LANES + 1]) / 999.0
    wait_recv(gen.at[pair, :], grecv.at[0])
    remote(gen.at[mine, :], gen.at[mine, :], gsend.at[4], grecv.at[4], dev(gg=g_near))

    gen_f = gen[mine, :].astype(F32)
    x_t = ((1.0 - sigma) * gen_f + sigma * rt[...].astype(F32)).astype(BF).astype(F32)
    all_rows = pl.ds(0, HALF)
    xgf_2 = xgf.at[1]

    def inputs_here():
        wait_recv(gen.at[other, :], grecv.at[4])
        remote(gen, gout, tsend.at[3], trecv.at[3], flip, when=off_diag)
        remote(xgf_2, xgf_2, gsend.at[5], grecv.at[5], near, when=is_2)

    gain_row = jnp.where(is_late, gain[2:3, :], gain[1:2, :])
    out = forward(
        1, HALF, x_t, gain_row, xgf.at[half], all_rows, hf.at[half], all_rows,
        (sb2, rb2, po2, zs2, zr2, acc2, ta2, tb2, tc2, td2),
        inputs_here,
    )
    fk[...] = (x_t + out).astype(BF)
    remote(fk, fother, gsend.at[6], grecv.at[6], dev(gg=g_pair), when=is_late)

    scale = 1.0 / math.sqrt(TOKENS)
    dy = dyb.at[half]

    @pl.when(is_late)
    def _():
        dy[t] = ((fk[...].astype(F32) - gen_f) * scale).astype(BF)
        dmine[...] = jnp.zeros_like(dmine)

    @pl.when(is_early)
    def _():
        real = fk[...].astype(F32)
        distance = jnp.sum(jnp.sum(jnp.abs(gen_f - real), axis=1, keepdims=True), axis=0, keepdims=True)
        dmine[0] = jnp.broadcast_to(distance, (8, LANES))
        cp = pltpu.make_async_remote_copy(
            src_ref=dmine.at[0], dst_ref=dmine.at[1], send_sem=gsend.at[7], recv_sem=grecv.at[7],
            device_id=near, device_id_type=MESH,
        )
        cp.start()
        wait_recv(fother, grecv.at[6])
        dy[t] = ((fother[...].astype(F32) - real) * scale).astype(BF)
        cp.wait()

    dy_block = lambda b: dy.at[b]
    gather_tp(2, dy_block)
    scalar_start(2, dmine[0, 0:1, :] + dmine[1, 0:1, :])

    da = dab.at[half]
    back = dnw.at[late]
    slope = gd.at[late]

    def product(rows, c):
        return lax.dot_general(
            rows, back[c * HC : (c + 1) * HC, :], (((1,), (1,)), ((), ())), preferred_element_type=F32
        )

    def da_piece(buf, yy, c):
        return buf.at[pl.ds(2 * yy, 2), :, pl.ds(c * HC, HC)]

    def image_scale(b):
        norm = sc_all[2, b, 0:1, 0:1] * (1.0 / (IMG_TOK * D_ALL)) + 1e-5
        return jnp.where(is_late, 1.0, 1.0 / norm)

    wait_recv(gd.at[0, :, pl.ds(QUARTER, QUARTER), :], grecv.at[1], is_early)
    not_2 = g != 2
    da_2 = dab.at[1]

    def pass_on(c):
        behind, ahead = lax.rem(y + (1 if c % 2 else 3), 4), lax.rem(y + (3 if c % 2 else 1), 4)
        passed = da_piece(da, behind, c)
        if c < CHUNKS - 1:
            wait_recv(passed, h_r.at[2, c, behind], not_2)
            remote(passed, passed, hy_s.at[2, c, 0], h_r.at[2, c, behind], row_peer(ahead), when=not_2)
        last = c >= CHUNKS - 2
        for j in (1, 3, 2) if last else (2,):
            pair_2 = lax.rem(y + j, 4)
            crossing = da_piece(da_2, pair_2, c)
            wait_recv(crossing, h_r.at[2, c, pair_2], is_2)
            remote(crossing, crossing, xs_s.at[c, j], xs_r.at[c, pair_2], near, when=is_2)
        wait_recv(da_piece(da_2, y, c), xs_r.at[c, y], is_3)
        if not last:
            for j in (1, 3):
                remote(
                    da_piece(da_2, y, c), da_piece(da_2, y, c), xs_s.at[c, 3 + j], xs_r.at[c, y],
                    row_peer(lax.rem(y + j, 4)), when=is_3,
                )

    def when_sent(c, j):
        if j == 2:
            return None if c == CHUNKS - 1 else is_2
        return None if c >= CHUNKS - 2 else not_2

    row_state = {}

    def finish(c, dh):
        if c == 0:
            scales = [jnp.broadcast_to(image_scale(2 * y + k), (HALF, 1)) for k in range(2)]
            row_state["scale"] = jnp.concatenate(scales, axis=0)
        cols = slice(c * HC, (c + 1) * HC)
        slopes = slope[:, :, cols].reshape(2 * HALF, HC).astype(F32)
        da[pl.ds(2 * y, 2), :, cols] = (dh * row_state["scale"] * slopes).astype(BF).reshape(2, HALF, HC)
        own_piece = da_piece(da, y, c)
        remote(own_piece, own_piece, xs_s.at[c, 0], xs_r.at[c, y], near, when=is_2)
        for j in (2, 1, 3):
            remote(
                own_piece, own_piece, hy_s.at[2, c, j], h_r.at[2, c, y], row_peer(lax.rem(y + j, 4)),
                when=when_sent(c, j),
            )

    dyb_2 = dyb.at[1]
    n_half, n_all = BLOCKS * HALF, 2 * BLOCKS * HALF

    def turned():
        @pl.when(is_early)
        def _():
            wait_recv(xgs_other, grecv.at[2])
            for k in range(BLOCKS // 2):
                two = xgs[2 * k : 2 * k + 2].reshape(2 * HALF, FEAT)
                ut[:, k * LANES : (k + 1) * LANES] = two.T

        @pl.when(is_3)
        def _():
            wait_recv(xgf_2, grecv.at[5])
            for k in range(BLOCKS):
                two = xgf[k // 4, 2 * (k % 4) : 2 * (k % 4) + 2].reshape(2 * HALF, FEAT)
                ut[:, k * LANES : (k + 1) * LANES] = two.T

    tn = (((0,), (0,)), ((), ()))
    step = 256

    def down_tiles(first, last):
        for i in range(first, last):
            cols = slice(i * step, (i + 1) * step)

            @pl.when(is_early)
            def _():
                dng_out[cols, :] = lax.dot_general(
                    hs[:, :, cols].reshape(n_half, step), dys[...].reshape(n_half, FEAT), tn,
                    preferred_element_type=F32,
                ).astype(BF)

            @pl.when(is_3)
            def _():
                dng_out[cols, :] = lax.dot_general(
                    hf[:, :, :, cols].reshape(n_all, step), dyb[...].reshape(n_all, FEAT), tn,
                    preferred_element_type=F32,
                ).astype(BF)

    def after(c):
        pass_on(c)
        if c == 0:

            @pl.when(is_early)
            def _():
                wait_recv(hs_other, grecv.at[3])
                for b in range(BLOCKS):
                    dys[b] = (dy[b].astype(F32) * image_scale(b)).astype(BF)

            @pl.when(is_3)
            def _():
                for k in range(CHUNKS):
                    for yy in range(4):
                        wait_recv(hf.at[1, 2 * yy : 2 * yy + 2, :, pl.ds(k * HC, HC)], hx_r.at[k, yy])
                wait_recv(dyb_2, grecv.at[8])

        if c < 3:
            down_tiles(2 * c, 2 * c + 2)

    xgs_other, hs_other = xgs.at[:, pl.ds(QUARTER, QUARTER), :], hs.at[:, pl.ds(QUARTER, QUARTER), :]
    reduce_rep(
        2, HALF, lambda yy: dy[pl.ds(2 * yy, 2)].reshape(2 * HALF, FEAT), dy_block, product,
        (sb3, rb3, po3, zs3, zr3), finish,
        lambda: remote(dyb_2, dyb_2, gsend.at[8], grecv.at[8], near, when=is_2), turned, after,
    )

    outs = [pltpu.make_async_copy(gout, gen_hbm, osem.at[0]), pltpu.make_async_copy(dng_out, dng_hbm, osem.at[1])]
    wait_recv(gout, trecv.at[3], off_diag)

    @pl.when(jnp.logical_not(off_diag))
    def _():
        gout[...] = gen[...]

    @pl.when(is_2)
    def _():
        upg_out[...] = jnp.zeros_like(upg_out)
        dng_out[...] = jnp.zeros_like(dng_out)

    outs[0].start()
    outs[1].start()
    for c in range(CHUNKS):
        cols = slice(c * HC, (c + 1) * HC)
        for j in (1, 3, 2):
            yy = lax.rem(y + j, 4)
            if c == CHUNKS - 1 or j != (1 if c % 2 else 3):
                wait_recv(da_piece(da, yy, c), h_r.at[2, c, yy], not_2)
            wait_recv(da_piece(da_2, yy, c), xs_r.at[c, yy], is_3)

        @pl.when(is_early)
        def _():
            upg_out[:, cols] = jnp.dot(
                ut[:, :n_half], da[:, :, cols].reshape(n_half, HC), preferred_element_type=F32
            ).astype(BF)

        @pl.when(is_3)
        def _():
            upg_out[:, cols] = jnp.dot(
                ut[...], dab[:, :, :, cols].reshape(n_all, HC), preferred_element_type=F32
            ).astype(BF)

        outs.append(pltpu.make_async_copy(upg_out.at[:, cols], upg_hbm.at[:, cols], osem.at[2 + c]))
        outs[-1].start()

    for cp, when in sends:
        if when is None:
            cp.wait_send()
        else:
            pl.when(when)(cp.wait_send)
    for cp in outs:
        cp.wait()


def widen(gen, up, down, gen_out, up_out, down_out):
    gen_out[...] = gen[...]
    up_out[0] = up[...].astype(F32)
    down_out[0] = down[...].astype(F32)


def rep_buffers(n):
    return [
        pltpu.VMEM((4, 2 * n, HID), BF),
        pltpu.VMEM((4, 2 * n, HID), BF),
        pltpu.VMEM((2 * n, HID), F32),
        pltpu.VMEM((2 * n, HID), BF),
        pltpu.VMEM((2 * n, HID), BF),
    ]


def tp_buffers(n):
    return [
        pltpu.VMEM((BLOCKS, n, FEAT), F32),
        pltpu.VMEM((4, n, FEAT), BF),
        pltpu.VMEM((4, n, FEAT), BF),
        pltpu.VMEM((3, n, FEAT), BF),
        pltpu.VMEM((3, n, FEAT), BF),
    ]


def body(noise_in, noise_renoise, text_cond, t_index, gains, up_weights, down_weights):
    vmem = pl.BlockSpec(memory_space=pltpu.VMEM)
    smem = pl.BlockSpec(memory_space=pltpu.SMEM)
    hbm = pl.BlockSpec(memory_space=pl.ANY)
    dma = pltpu.SemaphoreType.DMA
    generated, up_grad, down_grad = pl.pallas_call(
        kernel,
        name="step",
        out_shape=(
            jax.ShapeDtypeStruct((IMG_TOK, FEAT), BF),
            jax.ShapeDtypeStruct((FEAT, HID), BF),
            jax.ShapeDtypeStruct((HID, FEAT), BF),
        ),
        in_specs=[hbm, hbm, vmem, smem, hbm, hbm, hbm],
        out_specs=(hbm, hbm, hbm),
        scratch_shapes=[
            pltpu.VMEM((QUARTER, FEAT), BF),
            pltpu.VMEM((HALF, FEAT), BF),
            pltpu.VMEM((3, FEAT), F32),
            pltpu.VMEM((FEAT, HID), BF),
            pltpu.VMEM((HID, FEAT), BF),
            dma((3,)),
            dma((2 + CHUNKS,)),
            pltpu.VMEM((16, FEAT), BF),
            pltpu.VMEM((QUARTER, FEAT), BF),
            pltpu.VMEM((16, FEAT), BF),
            pltpu.VMEM((HALF, FEAT), BF),
            pltpu.VMEM((IMG_TOK, FEAT), BF),
            pltpu.VMEM((IMG_TOK, FEAT), BF),
            pltpu.VMEM((HALF, FEAT), BF),
            pltpu.VMEM((HALF, FEAT), BF),
            pltpu.VMEM((2, 8, LANES), F32),
            pltpu.VMEM((2, FEAT, HID), BF),
            pltpu.VMEM((2, HID, FEAT), BF),
            pltpu.VMEM((BLOCKS, HALF, FEAT), BF),
            pltpu.VMEM((BLOCKS, HALF, HID), BF),
            pltpu.VMEM((2, BLOCKS, HALF, FEAT), BF),
            pltpu.VMEM((2, BLOCKS, HALF, HID), BF),
            pltpu.VMEM((2, BLOCKS, HALF, FEAT), BF),
            pltpu.VMEM((2, BLOCKS, HALF, HID), BF),
            pltpu.VMEM((2, 2, HALF, HID), BF),
            pltpu.VMEM((BLOCKS, HALF, FEAT), BF),
            pltpu.VMEM((FEAT, 2 * BLOCKS * HALF), BF),
            pltpu.VMEM((3, 8, LANES), F32),
            pltpu.VMEM((3, 4, 8, LANES), F32),
            pltpu.VMEM((3, 8, LANES), F32),
            pltpu.VMEM((3, 8, LANES), F32),
            pltpu.VMEM((3, BLOCKS, 8, LANES), F32),
            *rep_buffers(QUARTER),
            *tp_buffers(QUARTER),
            *rep_buffers(HALF),
            *tp_buffers(HALF),
            *rep_buffers(HALF),
            dma((4,)),
            dma((4,)),
            dma((4,)),
            dma((10,)),
            dma((10,)),
            dma((3, 7)),
            dma((3, 8)),
            dma((3, CHUNKS, 4)),
            dma((3, CHUNKS, 4)),
            dma((3, CHUNKS)),
            dma((3, CHUNKS)),
            dma((3, CHUNKS, 4)),
            dma((3, CHUNKS, 4)),
            dma((2, 7)),
            dma((2, 7)),
            dma((CHUNKS, 7)),
            dma((CHUNKS, 4)),
            dma((CHUNKS, 4)),
            dma((CHUNKS, 4)),
            dma((3, 4)),
            dma((3, 4)),
            dma((3,)),
            dma((3,)),
            dma((3, 7)),
            dma((3, 8)),
        ],
        compiler_params=pltpu.CompilerParams(
            collective_id=0, has_side_effects=True, vmem_limit_bytes=60 * 2**20
        ),
    )(noise_in, noise_renoise, text_cond, t_index, gains, up_weights, down_weights)
    parts = 4
    rows = [
        pl.BlockSpec((IMG_TOK // parts, FEAT), lambda i: (i, 0)),
        pl.BlockSpec((FEAT // parts, HID), lambda i: (i, 0)),
        pl.BlockSpec((HID // parts, FEAT), lambda i: (i, 0)),
    ]
    wide = [
        rows[0],
        pl.BlockSpec((1, FEAT // parts, HID), lambda i: (0, i, 0)),
        pl.BlockSpec((1, HID // parts, FEAT), lambda i: (0, i, 0)),
    ]
    return pl.pallas_call(
        widen,
        name="widen",
        grid=(parts,),
        out_shape=(
            jax.ShapeDtypeStruct((IMG_TOK, FEAT), BF),
            jax.ShapeDtypeStruct((1, FEAT, HID), F32),
            jax.ShapeDtypeStruct((1, HID, FEAT), F32),
        ),
        in_specs=rows,
        out_specs=wide,
    )(generated, up_grad, down_grad)


def solution(mesh):
    in_specs = (
        P("rep", "tp"),
        P("rep", "tp"),
        P("rep", None),
        P("rep"),
        P(),
        P(None, "rep", "tp"),
        P(None, "tp", "rep"),
    )
    out_specs = (P("rep", "tp"), P("grp", "rep", "tp"), P("grp", "tp", "rep"))
    return jax.shard_map(body, mesh=mesh, in_specs=in_specs, out_specs=out_specs, check_vma=False)
```

```python
import functools
import math

import jax
import jax.numpy as jnp
from jax import lax
from jax.experimental import pallas as pl
from jax.experimental.pallas import tpu as pltpu
from jax.sharding import PartitionSpec as P

MESH = pl.DeviceIdType.MESH
BF = jnp.bfloat16
F32 = jnp.float32
FEAT = 384
HID = 1536
LANES = 128
CHUNKS = 4
HC = HID // CHUNKS
BLOCKS = 8
HALF = 64
QUARTER = 32
IMG_TOK = 128
D_ALL = 3072
TOKENS = 1024
GELU_C = math.sqrt(2.0 / math.pi)


def diagonal(n):
    return lax.broadcasted_iota(jnp.int32, (n, LANES), 0) == lax.broadcasted_iota(jnp.int32, (n, LANES), 1)


def to_lanes(column):
    return jnp.sum(jnp.where(diagonal(column.shape[0]), column, 0.0), axis=0, keepdims=True)


def to_column(lanes, n):
    return jnp.sum(jnp.where(diagonal(n), lanes, 0.0), axis=1, keepdims=True)


def gelu_both(a):
    a2 = a * a
    th = jnp.tanh(GELU_C * a * (1.0 + 0.044715 * a2))
    half = 0.5 * (1.0 + th)
    grad = half + 0.5 * a * (1.0 - th * th) * (GELU_C * (1.0 + 3.0 * 0.044715 * a2))
    return a * half, grad


def kernel(
    noise_hbm, renoise_hbm, cond_in, t_in, gains_hbm, up_hbm, down_hbm,
    gen_hbm, upg_hbm, dng_hbm,
    noise, renoise, gain, upg_out, dng_out, isem, osem,
    msgc, xt, ct, rt, gen, gout, fk, fother, dmine,
    upw, dnw, xgs, hs, xgf, hf, dyb, dab, gd, dys, ut,
    sc_own, sc_row, sc_zs, sc_zr, sc_all,
    sb1, rb1, po1, zs1, zr1, acc1, ta1, tb1, tc1, td1,
    sb2, rb2, po2, zs2, zr2, acc2, ta2, tb2, tc2, td2,
    sb3, rb3, po3, zs3, zr3,
    wsem, tsend, trecv, gsend, grecv,
    ag_s, ag_r, ry_s, ry_r, rz_s, rz_r, hy_s, h_r, tp_s, tp_r, xs_s, xs_r, hx_s, hx_r,
    sy_s, sy_r, sz_s, sz_r, st_s, st_r,
):
    g, r, t = lax.axis_index("grp"), lax.axis_index("rep"), lax.axis_index("tp")
    y, zh = lax.div(r, 2), lax.rem(r, 2)
    zl, core = lax.div(t, 2), lax.rem(t, 2)
    is_late, is_early = g >= 2, g < 2
    is_2, is_3 = g == 2, g == 3
    late = is_late.astype(jnp.int32)
    quart = late
    low = lax.rem(g, 2)
    half = low + late - 2 * low * late
    g_pair = 3 - g
    g_near = g + 1 - 2 * low
    qrow = pl.multiple_of(quart * QUARTER, QUARTER)
    sends = []

    def dev(gg=None, rr=None, tt=None):
        return (g if gg is None else gg, r if rr is None else rr, t if tt is None else tt)

    def remote(src, dst, ssem, rsem, to, when=None):
        cp = pltpu.make_async_remote_copy(
            src_ref=src, dst_ref=dst, send_sem=ssem, recv_sem=rsem, device_id=to, device_id_type=MESH
        )
        if when is None:
            cp.start()
        else:
            pl.when(when)(cp.start)
        sends.append((cp, when))
        return cp

    near = dev(gg=g_near)

    def wait_recv(dst, rsem, when=None):
        cp = pltpu.make_async_remote_copy(
            src_ref=dst, dst_ref=dst, send_sem=rsem, recv_sem=rsem, device_id=dev(), device_id_type=MESH
        )
        if when is None:
            cp.wait_recv()
        else:
            pl.when(when)(cp.wait_recv)

    own = pl.ds(pl.multiple_of(half * HALF + quart * QUARTER, QUARTER), QUARTER)
    pair = pl.ds(pl.multiple_of(half * HALF + (1 - quart) * QUARTER, QUARTER), QUARTER)
    mine = pl.ds(pl.multiple_of(half * HALF, HALF), HALF)
    other = pl.ds(pl.multiple_of((1 - half) * HALF, HALF), HALF)
    inputs = [
        pltpu.make_async_copy(noise_hbm.at[own, :], noise, isem.at[0]),
        pltpu.make_async_copy(renoise_hbm.at[mine, :], renoise, isem.at[1]),
        pltpu.make_async_copy(gains_hbm.at[:, pl.ds(pl.multiple_of(r * FEAT, LANES), FEAT)], gain, isem.at[2]),
    ]

    model = 1 + late
    loads = [
        pltpu.make_async_copy(up_hbm.at[0], upw.at[0], wsem.at[0]),
        pltpu.make_async_copy(down_hbm.at[0], dnw.at[0], wsem.at[1]),
        pltpu.make_async_copy(up_hbm.at[model], upw.at[1], wsem.at[2]),
        pltpu.make_async_copy(down_hbm.at[model], dnw.at[1], wsem.at[3]),
    ]
    barrier = pltpu.get_barrier_semaphore()
    sibling = dev(tt=2 * zl + 1 - core)
    flip = dev(rr=t, tt=r)
    off_diag = r != t
    row_peer = lambda yy: dev(rr=2 * yy + zh)
    z_peer = dev(rr=2 * y + 1 - zh)
    peers = [sibling, z_peer, dev(gg=g_pair), dev(gg=g_near)]
    peers += [dev(tt=2 * lax.rem(zl + d, 4) + core) for d in range(1, 4)]
    peers += [row_peer(lax.rem(y + j, 4)) for j in range(1, 4)]
    for peer in peers:
        pl.semaphore_signal(barrier, inc=1, device_id=peer, device_id_type=MESH)

    for cp in inputs + loads:
        cp.start()

    cond_row = cond_in[0:1, pl.ds(pl.multiple_of(t * FEAT, LANES), FEAT)].astype(F32)
    t_all = jnp.full((16, FEAT), t_in[0], jnp.int32)
    row = lax.broadcasted_iota(jnp.int32, (16, FEAT), 0)
    lane = lax.broadcasted_iota(jnp.int32, (16, FEAT), 1)
    t_part = jnp.where(lane < LANES, t_all >> 8, t_all & 255).astype(F32)
    msgc[...] = jnp.where(row < 8, jnp.broadcast_to(cond_row, (16, FEAT)), t_part).astype(BF)

    @pl.when(off_diag)
    def _():
        pl.semaphore_signal(barrier, inc=1, device_id=flip, device_id_type=MESH)
        pl.semaphore_wait(barrier, len(peers) + 1)

    @pl.when(jnp.logical_not(off_diag))
    def _():
        pl.semaphore_wait(barrier, len(peers))

    for cp in inputs:
        cp.wait()
    remote(noise, xt, tsend.at[0], trecv.at[0], flip, when=off_diag)
    remote(msgc, ct, tsend.at[1], trecv.at[1], flip, when=off_diag)
    remote(renoise, rt, tsend.at[2], trecv.at[2], flip, when=off_diag)

    @pl.when(jnp.logical_not(off_diag))
    def _():
        xt[...] = noise[...]
        ct[...] = msgc[...]
        rt[...] = renoise[...]

    wait_recv(xt, trecv.at[0], off_diag)
    wait_recv(ct, trecv.at[1], off_diag)
    cond1 = 1.0 + ct[0:1, :].astype(F32)

    def gather_tp(phase, block_of):
        remote(block_of(t), block_of(t), ag_s.at[phase, 0], ag_r.at[phase, t], sibling)
        for d in (2, 1, 3):
            to = dev(tt=2 * lax.rem(zl + d, 4) + core)
            remote(block_of(t), block_of(t), ag_s.at[phase, d], ag_r.at[phase, t], to)

    def wait_link(phase, block_of, d):
        b = 2 * lax.rem(zl + d, 4) + core
        wait_recv(block_of(b), ag_r.at[phase, b])
        remote(block_of(b), block_of(b), ag_s.at[phase, 3 + d], ag_r.at[phase, b], sibling)

    def wait_chip(phase, block_of, d):
        for nearest in {1: (1, 3), 3: (2,)}.get(d, ()):
            wait_link(phase, block_of, nearest)
        b = 2 * lax.rem(zl + d, 4) + 1 - core
        wait_recv(block_of(b), ag_r.at[phase, b])

    def scalar_start(phase, lanes):
        sc_own[phase] = jnp.broadcast_to(lanes, (8, LANES))
        for j in (2, 1, 3):
            remote(
                sc_own.at[phase], sc_row.at[phase, y], sy_s.at[phase, j], sy_r.at[phase, y],
                row_peer(lax.rem(y + j, 4)),
            )

    def scalar_to_z(phase):
        total = sc_own[phase]
        for j in (1, 3, 2):
            yy = lax.rem(y + j, 4)
            wait_recv(sc_row.at[phase, yy], sy_r.at[phase, yy])
            total += sc_row[phase, yy]
        sc_zs[phase] = total
        remote(sc_zs.at[phase], sc_zr.at[phase], sz_s.at[phase], sz_r.at[phase], z_peer)

    def scalar_to_tp(phase):
        wait_recv(sc_zr.at[phase], sz_r.at[phase])
        sc_all[phase, t] = sc_zs[phase] + sc_zr[phase]
        tile = sc_all.at[phase, t]
        remote(tile, tile, st_s.at[phase, 0], st_r.at[phase, t], sibling)
        for d in (2, 1, 3):
            remote(tile, tile, st_s.at[phase, d], st_r.at[phase, t], dev(tt=2 * lax.rem(zl + d, 4) + core))

    def scalar_end(phase):
        for d in (1, 3, 2):
            b = 2 * lax.rem(zl + d, 4) + core
            tile = sc_all.at[phase, b]
            wait_recv(tile, st_r.at[phase, b])
            remote(tile, tile, st_s.at[phase, 3 + d], st_r.at[phase, b], sibling)
        for d in range(4):
            b = 2 * lax.rem(zl + d, 4) + 1 - core
            wait_recv(sc_all.at[phase, b], st_r.at[phase, b])

    def reduce_rep(phase, n, rows_of, block_of, product, bufs, finish, gathered, sent, after):
        sb, rb, po, zs, zr = bufs
        span = lambda c: pl.ds(c * HC, HC)
        for c in range(CHUNKS):
            lo = c * HC
            for d in (0, 1, 3, 2):
                yy = lax.rem(zl + d, 4)
                if c == 0:
                    wait_chip(phase, block_of, d)
                part = product(rows_of(yy), c)

                @pl.when(yy == y)
                def _():
                    po[:, lo : lo + HC] = part

                @pl.when(yy != y)
                def _():
                    sb[yy, :, lo : lo + HC] = part.astype(BF)

                remote(
                    sb.at[yy, :, span(c)], rb.at[y, :, span(c)], ry_s.at[phase, c, d], ry_r.at[phase, c, y],
                    row_peer(yy), when=yy != y,
                )
                if c == 0 and d == 1:
                    scalar_to_z(phase)
            if c == 0:
                gathered()
        scalar_to_tp(phase)
        sent()

        def to_z(c):
            lo = c * HC
            total = po[:, lo : lo + HC]
            for j in (1, 3, 2):
                yy = lax.rem(y + j, 4)
                wait_recv(rb.at[yy, :, span(c)], ry_r.at[phase, c, yy])
                total += rb[yy, :, lo : lo + HC].astype(F32)
            po[:, lo : lo + HC] = total
            zs[:, lo : lo + HC] = total.astype(BF)
            remote(zs.at[:, span(c)], zr.at[:, span(c)], rz_s.at[phase, c], rz_r.at[phase, c], z_peer)

        def from_z(c):
            lo = c * HC
            if c == 0:
                scalar_end(phase)
            wait_recv(zr.at[:, span(c)], rz_r.at[phase, c])
            finish(c, po[:, lo : lo + HC] + zr[:, lo : lo + HC].astype(F32))

        early = n == HALF
        for c in range(CHUNKS):
            if early and c == CHUNKS - 1:
                from_z(0)
            to_z(c)
        for c in range(1 if early else 0, CHUNKS):
            from_z(c)
            if c >= 2:
                after(c - 2)
        for c in (CHUNKS - 2, CHUNKS - 1):
            after(c)

    def forward(phase, n, x_rows, gain_row, xg, xg_rows, h, h_rows, bufs, gathered):
        acc, ta, tb, tc, td = bufs[5:]
        up, down, grad = upw.at[phase], dnw.at[phase], gd.at[phase]
        xg[t, xg_rows, :] = (x_rows * (gain_row * cond1)).astype(BF)
        block_of = lambda b: xg.at[b, xg_rows, :]
        gather_tp(phase, block_of)
        scalar_start(phase, to_lanes(jnp.sum(x_rows * x_rows, axis=1, keepdims=True)))
        rows_of = lambda yy: xg[pl.ds(2 * yy, 2), xg_rows, :].reshape(2 * n, FEAT)
        loads[2 * phase].wait()

        def product(rows, c):
            return jnp.dot(rows, up[:, c * HC : (c + 1) * HC], preferred_element_type=F32)

        piece = lambda yy, c: h.at[pl.ds(2 * yy, 2), h_rows, pl.ds(c * HC, HC)]

        state = {}
        relayed = n == HALF
        passing = lambda c: relayed and c < CHUNKS - 2

        def pass_on(c):
            behind, ahead = lax.rem(y + (1 if c % 2 else 3), 4), lax.rem(y + (3 if c % 2 else 1), 4)
            passed = piece(behind, c)
            wait_recv(passed, h_r.at[phase, c, behind])
            remote(passed, passed, hy_s.at[phase, c, 2], h_r.at[phase, c, behind], row_peer(ahead))
            remote(passed, passed, hx_s.at[c, 1 if c % 2 else 3], hx_r.at[c, behind], near, when=is_2)

        def finish(c, a):
            if c == 0:
                squares = [to_column(sc_all[phase, 2 * y + k, 0:1, :], n) for k in range(2)]
                state["factor"] = lax.rsqrt(jnp.concatenate(squares, axis=0) * (1.0 / D_ALL) + 1e-6)
            factor = state["factor"]
            hidden, slope = gelu_both(a * factor)
            cols = slice(c * HC, (c + 1) * HC)
            h[pl.ds(2 * y, 2), h_rows, cols] = hidden.astype(BF).reshape(2, n, HC)
            for j in (1, 3) if passing(c) else (2, 1, 3):
                remote(
                    piece(y, c), piece(y, c), hy_s.at[phase, c, j], h_r.at[phase, c, y],
                    row_peer(lax.rem(y + j, 4)),
                )
            remote(piece(y, c), piece(y, c), hx_s.at[c, 0], hx_r.at[c, y], near, when=is_2) if relayed else None
            grad[:, h_rows, cols] = (slope * factor).astype(BF).reshape(2, n, HC)

        def project(c):
            if c == 0:
                loads[2 * phase + 1].wait()
            cols = slice(c * HC, (c + 1) * HC)
            for j in (0, 1, 3, 2):
                yy = lax.rem(y + j, 4)
                if j and not (passing(c) and j == (1 if c % 2 else 3)):
                    wait_recv(piece(yy, c), h_r.at[phase, c, yy])
                    if relayed:
                        remote(piece(yy, c), piece(yy, c), hx_s.at[c, j], hx_r.at[c, yy], near, when=is_2)
                both = h[pl.ds(2 * yy, 2), h_rows, cols].reshape(2 * n, HC)
                part = jnp.dot(both, down[cols, :], preferred_element_type=F32).reshape(2, n, FEAT)
                if c:
                    part += acc[pl.ds(2 * yy, 2)]
                acc[pl.ds(2 * yy, 2)] = part
                if c == CHUNKS - 1:
                    ta[yy] = acc[2 * yy + 1 - core].astype(BF)
                    remote(ta.at[yy], tb.at[yy], tp_s.at[phase, yy], tp_r.at[phase, yy], sibling)

        def after(c):
            if passing(c):
                pass_on(c)
            if relayed and c >= 3:
                project(c - 3)

        reduce_rep(phase, n, rows_of, block_of, product, bufs[:5], finish, gathered, lambda: None, after)
        for c in range(CHUNKS - 3 if relayed else 0, CHUNKS):
            project(c)
        total = None
        for d in (2, 1, 3, 0):
            yy = lax.rem(zl + d, 4)
            wait_recv(tb.at[yy], tp_r.at[phase, yy])
            both = acc[2 * yy + core] + tb[yy].astype(F32)
            if d:
                tc[d - 1] = both.astype(BF)
                remote(
                    tc.at[d - 1], td.at[d - 1], tp_s.at[phase, 3 + d], tp_r.at[phase, 3 + d],
                    dev(tt=2 * yy + core),
                )
            else:
                total = both
        for d in (1, 3, 2):
            wait_recv(td.at[d - 1], tp_r.at[phase, 3 + d])
            total += td[d - 1].astype(F32)
        return total

    x0 = xt[...].astype(F32)
    q_rows = pl.ds(qrow, QUARTER)
    out = forward(
        0, QUARTER, x0, gain[0:1, :], xgs, q_rows, hs, q_rows,
        (sb1, rb1, po1, zs1, zr1, acc1, ta1, tb1, tc1, td1), lambda: None,
    )
    gen[own, :] = (x0 + out).astype(BF)
    remote(gen.at[own, :], gen.at[own, :], gsend.at[0], grecv.at[0], dev(gg=g_pair))
    for i, ref in enumerate((gd.at[0, :, q_rows, :], xgs.at[:, q_rows, :], hs.at[:, q_rows, :])):
        remote(ref, ref, gsend.at[1 + i], grecv.at[1 + i], dev(gg=g_pair), when=is_late)
    wait_recv(rt, trecv.at[2], off_diag)
    t_row = ct[8:9, :].astype(F32)
    sigma = 0.1 + 0.8 * (t_row[:, 0:1] * 256.0 + t_row[:, LANES : LANES + 1]) / 999.0
    wait_recv(gen.at[pair, :], grecv.at[0])
    remote(gen.at[mine, :], gen.at[mine, :], gsend.at[4], grecv.at[4], dev(gg=g_near))

    gen_f = gen[mine, :].astype(F32)
    x_t = ((1.0 - sigma) * gen_f + sigma * rt[...].astype(F32)).astype(BF).astype(F32)
    all_rows = pl.ds(0, HALF)
    xgf_2 = xgf.at[1]

    def inputs_here():
        wait_recv(gen.at[other, :], grecv.at[4])
        remote(gen, gout, tsend.at[3], trecv.at[3], flip, when=off_diag)
        remote(xgf_2, xgf_2, gsend.at[5], grecv.at[5], near, when=is_2)

    gain_row = jnp.where(is_late, gain[2:3, :], gain[1:2, :])
    out = forward(
        1, HALF, x_t, gain_row, xgf.at[half], all_rows, hf.at[half], all_rows,
        (sb2, rb2, po2, zs2, zr2, acc2, ta2, tb2, tc2, td2),
        inputs_here,
    )
    fk[...] = (x_t + out).astype(BF)
    remote(fk, fother, gsend.at[6], grecv.at[6], dev(gg=g_pair), when=is_late)

    scale = 1.0 / math.sqrt(TOKENS)
    dy = dyb.at[half]

    @pl.when(is_late)
    def _():
        dy[t] = ((fk[...].astype(F32) - gen_f) * scale).astype(BF)
        dmine[...] = jnp.zeros_like(dmine)

    @pl.when(is_early)
    def _():
        real = fk[...].astype(F32)
        distance = jnp.sum(jnp.sum(jnp.abs(gen_f - real), axis=1, keepdims=True), axis=0, keepdims=True)
        dmine[0] = jnp.broadcast_to(distance, (8, LANES))
        cp = pltpu.make_async_remote_copy(
            src_ref=dmine.at[0], dst_ref=dmine.at[1], send_sem=gsend.at[7], recv_sem=grecv.at[7],
            device_id=near, device_id_type=MESH,
        )
        cp.start()
        wait_recv(fother, grecv.at[6])
        dy[t] = ((fother[...].astype(F32) - real) * scale).astype(BF)
        cp.wait()

    dy_block = lambda b: dy.at[b]
    gather_tp(2, dy_block)
    scalar_start(2, dmine[0, 0:1, :] + dmine[1, 0:1, :])

    da = dab.at[half]
    back = dnw.at[late]
    slope = gd.at[late]

    def product(rows, c):
        return lax.dot_general(
            rows, back[c * HC : (c + 1) * HC, :], (((1,), (1,)), ((), ())), preferred_element_type=F32
        )

    def da_piece(buf, yy, c):
        return buf.at[pl.ds(2 * yy, 2), :, pl.ds(c * HC, HC)]

    def image_scale(b):
        norm = sc_all[2, b, 0:1, 0:1] * (1.0 / (IMG_TOK * D_ALL)) + 1e-5
        return jnp.where(is_late, 1.0, 1.0 / norm)

    wait_recv(gd.at[0, :, pl.ds(QUARTER, QUARTER), :], grecv.at[1], is_early)
    not_2 = g != 2
    da_2 = dab.at[1]

    def pass_on(c):
        behind, ahead = lax.rem(y + (1 if c % 2 else 3), 4), lax.rem(y + (3 if c % 2 else 1), 4)
        passed = da_piece(da, behind, c)
        if c < CHUNKS - 1:
            wait_recv(passed, h_r.at[2, c, behind], not_2)
            remote(passed, passed, hy_s.at[2, c, 0], h_r.at[2, c, behind], row_peer(ahead), when=not_2)
        last = c == CHUNKS - 1
        for j in (1, 3, 2) if last else (2,):
            pair_2 = lax.rem(y + j, 4)
            crossing = da_piece(da_2, pair_2, c)
            wait_recv(crossing, h_r.at[2, c, pair_2], is_2)
            remote(crossing, crossing, xs_s.at[c, j], xs_r.at[c, pair_2], near, when=is_2)
        wait_recv(da_piece(da_2, y, c), xs_r.at[c, y], is_3)
        if not last:
            for j in (1, 3):
                remote(
                    da_piece(da_2, y, c), da_piece(da_2, y, c), xs_s.at[c, 3 + j], xs_r.at[c, y],
                    row_peer(lax.rem(y + j, 4)), when=is_3,
                )

    def when_sent(c, j):
        if j == 2:
            return None if c == CHUNKS - 1 else is_2
        return None if c == CHUNKS - 1 else not_2

    row_state = {}

    def finish(c, dh):
        if c == 0:
            scales = [jnp.broadcast_to(image_scale(2 * y + k), (HALF, 1)) for k in range(2)]
            row_state["scale"] = jnp.concatenate(scales, axis=0)
        cols = slice(c * HC, (c + 1) * HC)
        slopes = slope[:, :, cols].reshape(2 * HALF, HC).astype(F32)
        da[pl.ds(2 * y, 2), :, cols] = (dh * row_state["scale"] * slopes).astype(BF).reshape(2, HALF, HC)
        own_piece = da_piece(da, y, c)
        remote(own_piece, own_piece, xs_s.at[c, 0], xs_r.at[c, y], near, when=is_2)
        for j in (2, 1, 3):
            remote(
                own_piece, own_piece, hy_s.at[2, c, j], h_r.at[2, c, y], row_peer(lax.rem(y + j, 4)),
                when=when_sent(c, j),
            )

    dyb_2 = dyb.at[1]
    n_half, n_all = BLOCKS * HALF, 2 * BLOCKS * HALF

    def turned():
        @pl.when(is_early)
        def _():
            wait_recv(xgs_other, grecv.at[2])
            for k in range(BLOCKS // 2):
                two = xgs[2 * k : 2 * k + 2].reshape(2 * HALF, FEAT)
                ut[:, k * LANES : (k + 1) * LANES] = two.T

        @pl.when(is_3)
        def _():
            wait_recv(xgf_2, grecv.at[5])
            for k in range(BLOCKS):
                two = xgf[k // 4, 2 * (k % 4) : 2 * (k % 4) + 2].reshape(2 * HALF, FEAT)
                ut[:, k * LANES : (k + 1) * LANES] = two.T

    tn = (((0,), (0,)), ((), ()))
    step = 256

    def down_tiles(first, last):
        for i in range(first, last):
            cols = slice(i * step, (i + 1) * step)

            @pl.when(is_early)
            def _():
                dng_out[cols, :] = lax.dot_general(
                    hs[:, :, cols].reshape(n_half, step), dys[...].reshape(n_half, FEAT), tn,
                    preferred_element_type=F32,
                ).astype(BF)

            @pl.when(is_3)
            def _():
                dng_out[cols, :] = lax.dot_general(
                    hf[:, :, :, cols].reshape(n_all, step), dyb[...].reshape(n_all, FEAT), tn,
                    preferred_element_type=F32,
                ).astype(BF)

    def after(c):
        pass_on(c)
        if c == 0:

            @pl.when(is_early)
            def _():
                wait_recv(hs_other, grecv.at[3])
                for b in range(BLOCKS):
                    dys[b] = (dy[b].astype(F32) * image_scale(b)).astype(BF)

            @pl.when(is_3)
            def _():
                for k in range(CHUNKS):
                    for yy in range(4):
                        wait_recv(hf.at[1, 2 * yy : 2 * yy + 2, :, pl.ds(k * HC, HC)], hx_r.at[k, yy])
                wait_recv(dyb_2, grecv.at[8])

        if c < 3:
            down_tiles(2 * c, 2 * c + 2)

    xgs_other, hs_other = xgs.at[:, pl.ds(QUARTER, QUARTER), :], hs.at[:, pl.ds(QUARTER, QUARTER), :]
    reduce_rep(
        2, HALF, lambda yy: dy[pl.ds(2 * yy, 2)].reshape(2 * HALF, FEAT), dy_block, product,
        (sb3, rb3, po3, zs3, zr3), finish,
        lambda: remote(dyb_2, dyb_2, gsend.at[8], grecv.at[8], near, when=is_2), turned, after,
    )

    outs = [pltpu.make_async_copy(gout, gen_hbm, osem.at[0]), pltpu.make_async_copy(dng_out, dng_hbm, osem.at[1])]
    wait_recv(gout, trecv.at[3], off_diag)

    @pl.when(jnp.logical_not(off_diag))
    def _():
        gout[...] = gen[...]

    @pl.when(is_2)
    def _():
        upg_out[...] = jnp.zeros_like(upg_out)
        dng_out[...] = jnp.zeros_like(dng_out)

    outs[0].start()
    outs[1].start()
    for c in range(CHUNKS):
        cols = slice(c * HC, (c + 1) * HC)
        for j in (1, 3, 2):
            yy = lax.rem(y + j, 4)
            if c == CHUNKS - 1 or j != (1 if c % 2 else 3):
                wait_recv(da_piece(da, yy, c), h_r.at[2, c, yy], not_2)
            wait_recv(da_piece(da_2, yy, c), xs_r.at[c, yy], is_3)

        @pl.when(is_early)
        def _():
            upg_out[:, cols] = jnp.dot(
                ut[:, :n_half], da[:, :, cols].reshape(n_half, HC), preferred_element_type=F32
            ).astype(BF)

        @pl.when(is_3)
        def _():
            upg_out[:, cols] = jnp.dot(
                ut[...], dab[:, :, :, cols].reshape(n_all, HC), preferred_element_type=F32
            ).astype(BF)

        outs.append(pltpu.make_async_copy(upg_out.at[:, cols], upg_hbm.at[:, cols], osem.at[2 + c]))
        outs[-1].start()

    for cp, when in sends:
        if when is None:
            cp.wait_send()
        else:
            pl.when(when)(cp.wait_send)
    for cp in outs:
        cp.wait()


def widen(gen, up, down, gen_out, up_out, down_out):
    gen_out[...] = gen[...]
    up_out[0] = up[...].astype(F32)
    down_out[0] = down[...].astype(F32)


def rep_buffers(n):
    return [
        pltpu.VMEM((4, 2 * n, HID), BF),
        pltpu.VMEM((4, 2 * n, HID), BF),
        pltpu.VMEM((2 * n, HID), F32),
        pltpu.VMEM((2 * n, HID), BF),
        pltpu.VMEM((2 * n, HID), BF),
    ]


def tp_buffers(n):
    return [
        pltpu.VMEM((BLOCKS, n, FEAT), F32),
        pltpu.VMEM((4, n, FEAT), BF),
        pltpu.VMEM((4, n, FEAT), BF),
        pltpu.VMEM((3, n, FEAT), BF),
        pltpu.VMEM((3, n, FEAT), BF),
    ]


def body(noise_in, noise_renoise, text_cond, t_index, gains, up_weights, down_weights):
    vmem = pl.BlockSpec(memory_space=pltpu.VMEM)
    smem = pl.BlockSpec(memory_space=pltpu.SMEM)
    hbm = pl.BlockSpec(memory_space=pl.ANY)
    dma = pltpu.SemaphoreType.DMA
    generated, up_grad, down_grad = pl.pallas_call(
        kernel,
        name="step",
        out_shape=(
            jax.ShapeDtypeStruct((IMG_TOK, FEAT), BF),
            jax.ShapeDtypeStruct((FEAT, HID), BF),
            jax.ShapeDtypeStruct((HID, FEAT), BF),
        ),
        in_specs=[hbm, hbm, vmem, smem, hbm, hbm, hbm],
        out_specs=(hbm, hbm, hbm),
        scratch_shapes=[
            pltpu.VMEM((QUARTER, FEAT), BF),
            pltpu.VMEM((HALF, FEAT), BF),
            pltpu.VMEM((3, FEAT), F32),
            pltpu.VMEM((FEAT, HID), BF),
            pltpu.VMEM((HID, FEAT), BF),
            dma((3,)),
            dma((2 + CHUNKS,)),
            pltpu.VMEM((16, FEAT), BF),
            pltpu.VMEM((QUARTER, FEAT), BF),
            pltpu.VMEM((16, FEAT), BF),
            pltpu.VMEM((HALF, FEAT), BF),
            pltpu.VMEM((IMG_TOK, FEAT), BF),
            pltpu.VMEM((IMG_TOK, FEAT), BF),
            pltpu.VMEM((HALF, FEAT), BF),
            pltpu.VMEM((HALF, FEAT), BF),
            pltpu.VMEM((2, 8, LANES), F32),
            pltpu.VMEM((2, FEAT, HID), BF),
            pltpu.VMEM((2, HID, FEAT), BF),
            pltpu.VMEM((BLOCKS, HALF, FEAT), BF),
            pltpu.VMEM((BLOCKS, HALF, HID), BF),
            pltpu.VMEM((2, BLOCKS, HALF, FEAT), BF),
            pltpu.VMEM((2, BLOCKS, HALF, HID), BF),
            pltpu.VMEM((2, BLOCKS, HALF, FEAT), BF),
            pltpu.VMEM((2, BLOCKS, HALF, HID), BF),
            pltpu.VMEM((2, 2, HALF, HID), BF),
            pltpu.VMEM((BLOCKS, HALF, FEAT), BF),
            pltpu.VMEM((FEAT, 2 * BLOCKS * HALF), BF),
            pltpu.VMEM((3, 8, LANES), F32),
            pltpu.VMEM((3, 4, 8, LANES), F32),
            pltpu.VMEM((3, 8, LANES), F32),
            pltpu.VMEM((3, 8, LANES), F32),
            pltpu.VMEM((3, BLOCKS, 8, LANES), F32),
            *rep_buffers(QUARTER),
            *tp_buffers(QUARTER),
            *rep_buffers(HALF),
            *tp_buffers(HALF),
            *rep_buffers(HALF),
            dma((4,)),
            dma((4,)),
            dma((4,)),
            dma((10,)),
            dma((10,)),
            dma((3, 7)),
            dma((3, 8)),
            dma((3, CHUNKS, 4)),
            dma((3, CHUNKS, 4)),
            dma((3, CHUNKS)),
            dma((3, CHUNKS)),
            dma((3, CHUNKS, 4)),
            dma((3, CHUNKS, 4)),
            dma((2, 7)),
            dma((2, 7)),
            dma((CHUNKS, 7)),
            dma((CHUNKS, 4)),
            dma((CHUNKS, 4)),
            dma((CHUNKS, 4)),
            dma((3, 4)),
            dma((3, 4)),
            dma((3,)),
            dma((3,)),
            dma((3, 7)),
            dma((3, 8)),
        ],
        compiler_params=pltpu.CompilerParams(
            collective_id=0, has_side_effects=True, vmem_limit_bytes=60 * 2**20
        ),
    )(noise_in, noise_renoise, text_cond, t_index, gains, up_weights, down_weights)
    parts = 4
    rows = [
        pl.BlockSpec((IMG_TOK // parts, FEAT), lambda i: (i, 0)),
        pl.BlockSpec((FEAT // parts, HID), lambda i: (i, 0)),
        pl.BlockSpec((HID // parts, FEAT), lambda i: (i, 0)),
    ]
    wide = [
        rows[0],
        pl.BlockSpec((1, FEAT // parts, HID), lambda i: (0, i, 0)),
        pl.BlockSpec((1, HID // parts, FEAT), lambda i: (0, i, 0)),
    ]
    return pl.pallas_call(
        widen,
        name="widen",
        grid=(parts,),
        out_shape=(
            jax.ShapeDtypeStruct((IMG_TOK, FEAT), BF),
            jax.ShapeDtypeStruct((1, FEAT, HID), F32),
            jax.ShapeDtypeStruct((1, HID, FEAT), F32),
        ),
        in_specs=rows,
        out_specs=wide,
    )(generated, up_grad, down_grad)


def solution(mesh):
    in_specs = (
        P("rep", "tp"),
        P("rep", "tp"),
        P("rep", None),
        P("rep"),
        P(),
        P(None, "rep", "tp"),
        P(None, "tp", "rep"),
    )
    out_specs = (P("rep", "tp"), P("grp", "rep", "tp"), P("grp", "tp", "rep"))
    return jax.shard_map(body, mesh=mesh, in_specs=in_specs, out_specs=out_specs, check_vma=False)
```

```python
import functools
import math

import jax
import jax.numpy as jnp
from jax import lax
from jax.experimental import pallas as pl
from jax.experimental.pallas import tpu as pltpu
from jax.sharding import PartitionSpec as P

MESH = pl.DeviceIdType.MESH
BF = jnp.bfloat16
F32 = jnp.float32
FEAT = 384
HID = 1536
LANES = 128
CHUNKS = 4
HC = HID // CHUNKS
BLOCKS = 8
HALF = 64
QUARTER = 32
IMG_TOK = 128
D_ALL = 3072
TOKENS = 1024
GELU_C = math.sqrt(2.0 / math.pi)


def diagonal(n):
    return lax.broadcasted_iota(jnp.int32, (n, LANES), 0) == lax.broadcasted_iota(jnp.int32, (n, LANES), 1)


def to_lanes(column):
    return jnp.sum(jnp.where(diagonal(column.shape[0]), column, 0.0), axis=0, keepdims=True)


def to_column(lanes, n):
    return jnp.sum(jnp.where(diagonal(n), lanes, 0.0), axis=1, keepdims=True)


def gelu_both(a):
    a2 = a * a
    th = jnp.tanh(GELU_C * a * (1.0 + 0.044715 * a2))
    half = 0.5 * (1.0 + th)
    grad = half + 0.5 * a * (1.0 - th * th) * (GELU_C * (1.0 + 3.0 * 0.044715 * a2))
    return a * half, grad


def kernel(
    noise_hbm, renoise_hbm, cond_in, t_in, gains_hbm, up_hbm, down_hbm,
    gen_hbm, upg_hbm, dng_hbm,
    noise, renoise, gain, upg_out, dng_out, isem, osem,
    msgc, xt, ct, rt, gen, gout, fk, fother, dmine,
    upw, dnw, xgs, hs, xgf, hf, dyb, dab, gd, dys, ut,
    sc_own, sc_row, sc_zs, sc_zr, sc_all,
    sb1, rb1, po1, zs1, zr1, acc1, ta1, tb1, tc1, td1,
    sb2, rb2, po2, zs2, zr2, acc2, ta2, tb2, tc2, td2,
    sb3, rb3, po3, zs3, zr3,
    wsem, tsend, trecv, gsend, grecv,
    ag_s, ag_r, ry_s, ry_r, rz_s, rz_r, hy_s, h_r, tp_s, tp_r, xs_s, xs_r, hx_s, hx_r,
    sy_s, sy_r, sz_s, sz_r, st_s, st_r,
):
    g, r, t = lax.axis_index("grp"), lax.axis_index("rep"), lax.axis_index("tp")
    y, zh = lax.div(r, 2), lax.rem(r, 2)
    zl, core = lax.div(t, 2), lax.rem(t, 2)
    is_late, is_early = g >= 2, g < 2
    is_2, is_3 = g == 2, g == 3
    late = is_late.astype(jnp.int32)
    quart = late
    low = lax.rem(g, 2)
    half = low + late - 2 * low * late
    g_pair = 3 - g
    g_near = g + 1 - 2 * low
    qrow = pl.multiple_of(quart * QUARTER, QUARTER)
    sends = []

    def dev(gg=None, rr=None, tt=None):
        return (g if gg is None else gg, r if rr is None else rr, t if tt is None else tt)

    def remote(src, dst, ssem, rsem, to, when=None):
        cp = pltpu.make_async_remote_copy(
            src_ref=src, dst_ref=dst, send_sem=ssem, recv_sem=rsem, device_id=to, device_id_type=MESH
        )
        if when is None:
            cp.start()
        else:
            pl.when(when)(cp.start)
        sends.append((cp, when))
        return cp

    near = dev(gg=g_near)

    def wait_recv(dst, rsem, when=None):
        cp = pltpu.make_async_remote_copy(
            src_ref=dst, dst_ref=dst, send_sem=rsem, recv_sem=rsem, device_id=dev(), device_id_type=MESH
        )
        if when is None:
            cp.wait_recv()
        else:
            pl.when(when)(cp.wait_recv)

    own = pl.ds(pl.multiple_of(half * HALF + quart * QUARTER, QUARTER), QUARTER)
    pair = pl.ds(pl.multiple_of(half * HALF + (1 - quart) * QUARTER, QUARTER), QUARTER)
    mine = pl.ds(pl.multiple_of(half * HALF, HALF), HALF)
    other = pl.ds(pl.multiple_of((1 - half) * HALF, HALF), HALF)
    inputs = [
        pltpu.make_async_copy(noise_hbm.at[own, :], noise, isem.at[0]),
        pltpu.make_async_copy(renoise_hbm.at[mine, :], renoise, isem.at[1]),
        pltpu.make_async_copy(gains_hbm.at[:, pl.ds(pl.multiple_of(r * FEAT, LANES), FEAT)], gain, isem.at[2]),
    ]

    model = 1 + late
    loads = [
        pltpu.make_async_copy(up_hbm.at[0], upw.at[0], wsem.at[0]),
        pltpu.make_async_copy(down_hbm.at[0], dnw.at[0], wsem.at[1]),
        pltpu.make_async_copy(up_hbm.at[model], upw.at[1], wsem.at[2]),
        pltpu.make_async_copy(down_hbm.at[model], dnw.at[1], wsem.at[3]),
    ]
    barrier = pltpu.get_barrier_semaphore()
    sibling = dev(tt=2 * zl + 1 - core)
    flip = dev(rr=t, tt=r)
    off_diag = r != t
    row_peer = lambda yy: dev(rr=2 * yy + zh)
    z_peer = dev(rr=2 * y + 1 - zh)
    peers = [sibling, z_peer, dev(gg=g_pair), dev(gg=g_near)]
    peers += [dev(tt=2 * lax.rem(zl + d, 4) + core) for d in range(1, 4)]
    peers += [row_peer(lax.rem(y + j, 4)) for j in range(1, 4)]
    for peer in peers:
        pl.semaphore_signal(barrier, inc=1, device_id=peer, device_id_type=MESH)

    for cp in inputs + loads:
        cp.start()

    cond_row = cond_in[0:1, pl.ds(pl.multiple_of(t * FEAT, LANES), FEAT)].astype(F32)
    t_all = jnp.full((16, FEAT), t_in[0], jnp.int32)
    row = lax.broadcasted_iota(jnp.int32, (16, FEAT), 0)
    lane = lax.broadcasted_iota(jnp.int32, (16, FEAT), 1)
    t_part = jnp.where(lane < LANES, t_all >> 8, t_all & 255).astype(F32)
    msgc[...] = jnp.where(row < 8, jnp.broadcast_to(cond_row, (16, FEAT)), t_part).astype(BF)

    @pl.when(off_diag)
    def _():
        pl.semaphore_signal(barrier, inc=1, device_id=flip, device_id_type=MESH)
        pl.semaphore_wait(barrier, len(peers) + 1)

    @pl.when(jnp.logical_not(off_diag))
    def _():
        pl.semaphore_wait(barrier, len(peers))

    for cp in inputs:
        cp.wait()
    remote(noise, xt, tsend.at[0], trecv.at[0], flip, when=off_diag)
    remote(msgc, ct, tsend.at[1], trecv.at[1], flip, when=off_diag)
    remote(renoise, rt, tsend.at[2], trecv.at[2], flip, when=off_diag)

    @pl.when(jnp.logical_not(off_diag))
    def _():
        xt[...] = noise[...]
        ct[...] = msgc[...]
        rt[...] = renoise[...]

    wait_recv(xt, trecv.at[0], off_diag)
    wait_recv(ct, trecv.at[1], off_diag)
    cond1 = 1.0 + ct[0:1, :].astype(F32)

    def gather_tp(phase, block_of):
        remote(block_of(t), block_of(t), ag_s.at[phase, 0], ag_r.at[phase, t], sibling)
        for d in (2, 1, 3):
            to = dev(tt=2 * lax.rem(zl + d, 4) + core)
            remote(block_of(t), block_of(t), ag_s.at[phase, d], ag_r.at[phase, t], to)

    def wait_link(phase, block_of, d):
        b = 2 * lax.rem(zl + d, 4) + core
        wait_recv(block_of(b), ag_r.at[phase, b])
        remote(block_of(b), block_of(b), ag_s.at[phase, 3 + d], ag_r.at[phase, b], sibling)

    def wait_chip(phase, block_of, d):
        for nearest in {1: (1, 3), 3: (2,)}.get(d, ()):
            wait_link(phase, block_of, nearest)
        b = 2 * lax.rem(zl + d, 4) + 1 - core
        wait_recv(block_of(b), ag_r.at[phase, b])

    def scalar_start(phase, lanes):
        sc_own[phase] = jnp.broadcast_to(lanes, (8, LANES))
        for j in (2, 1, 3):
            remote(
                sc_own.at[phase], sc_row.at[phase, y], sy_s.at[phase, j], sy_r.at[phase, y],
                row_peer(lax.rem(y + j, 4)),
            )

    def scalar_to_z(phase):
        total = sc_own[phase]
        for j in (1, 3, 2):
            yy = lax.rem(y + j, 4)
            wait_recv(sc_row.at[phase, yy], sy_r.at[phase, yy])
            total += sc_row[phase, yy]
        sc_zs[phase] = total
        remote(sc_zs.at[phase], sc_zr.at[phase], sz_s.at[phase], sz_r.at[phase], z_peer)

    def scalar_to_tp(phase):
        wait_recv(sc_zr.at[phase], sz_r.at[phase])
        sc_all[phase, t] = sc_zs[phase] + sc_zr[phase]
        tile = sc_all.at[phase, t]
        remote(tile, tile, st_s.at[phase, 0], st_r.at[phase, t], sibling)
        for d in (2, 1, 3):
            remote(tile, tile, st_s.at[phase, d], st_r.at[phase, t], dev(tt=2 * lax.rem(zl + d, 4) + core))

    def scalar_end(phase):
        for d in (1, 3, 2):
            b = 2 * lax.rem(zl + d, 4) + core
            tile = sc_all.at[phase, b]
            wait_recv(tile, st_r.at[phase, b])
            remote(tile, tile, st_s.at[phase, 3 + d], st_r.at[phase, b], sibling)
        for d in range(4):
            b = 2 * lax.rem(zl + d, 4) + 1 - core
            wait_recv(sc_all.at[phase, b], st_r.at[phase, b])

    def reduce_rep(phase, n, rows_of, block_of, product, bufs, finish, gathered, sent, after):
        sb, rb, po, zs, zr = bufs
        span = lambda c: pl.ds(c * HC, HC)
        for c in range(CHUNKS):
            lo = c * HC
            for d in (0, 1, 3, 2):
                yy = lax.rem(zl + d, 4)
                if c == 0:
                    wait_chip(phase, block_of, d)
                part = product(rows_of(yy), c)

                @pl.when(yy == y)
                def _():
                    po[:, lo : lo + HC] = part

                @pl.when(yy != y)
                def _():
                    sb[yy, :, lo : lo + HC] = part.astype(BF)

                remote(
                    sb.at[yy, :, span(c)], rb.at[y, :, span(c)], ry_s.at[phase, c, d], ry_r.at[phase, c, y],
                    row_peer(yy), when=yy != y,
                )
                if c == 0 and d == 1:
                    scalar_to_z(phase)
            if c == 0:
                gathered()
        scalar_to_tp(phase)
        sent()

        def to_z(c):
            lo = c * HC
            total = po[:, lo : lo + HC]
            for j in (1, 3, 2):
                yy = lax.rem(y + j, 4)
                wait_recv(rb.at[yy, :, span(c)], ry_r.at[phase, c, yy])
                total += rb[yy, :, lo : lo + HC].astype(F32)
            po[:, lo : lo + HC] = total
            zs[:, lo : lo + HC] = total.astype(BF)
            remote(zs.at[:, span(c)], zr.at[:, span(c)], rz_s.at[phase, c], rz_r.at[phase, c], z_peer)

        def from_z(c):
            lo = c * HC
            if c == 0:
                scalar_end(phase)
            wait_recv(zr.at[:, span(c)], rz_r.at[phase, c])
            finish(c, po[:, lo : lo + HC] + zr[:, lo : lo + HC].astype(F32))

        early = n == HALF
        for c in range(CHUNKS):
            if early and c == CHUNKS - 1:
                from_z(0)
            to_z(c)
        for c in range(1 if early else 0, CHUNKS):
            from_z(c)
            if c >= 2:
                after(c - 2)
        for c in (CHUNKS - 2, CHUNKS - 1):
            after(c)

    def forward(phase, n, x_rows, gain_row, xg, xg_rows, h, h_rows, bufs, gathered):
        acc, ta, tb, tc, td = bufs[5:]
        up, down, grad = upw.at[phase], dnw.at[phase], gd.at[phase]
        xg[t, xg_rows, :] = (x_rows * (gain_row * cond1)).astype(BF)
        block_of = lambda b: xg.at[b, xg_rows, :]
        gather_tp(phase, block_of)
        scalar_start(phase, to_lanes(jnp.sum(x_rows * x_rows, axis=1, keepdims=True)))
        rows_of = lambda yy: xg[pl.ds(2 * yy, 2), xg_rows, :].reshape(2 * n, FEAT)
        loads[2 * phase].wait()

        def product(rows, c):
            return jnp.dot(rows, up[:, c * HC : (c + 1) * HC], preferred_element_type=F32)

        piece = lambda yy, c: h.at[pl.ds(2 * yy, 2), h_rows, pl.ds(c * HC, HC)]

        state = {}
        relayed = n == HALF
        passing = lambda c: relayed and c < CHUNKS - 2

        def pass_on(c):
            behind, ahead = lax.rem(y + (1 if c % 2 else 3), 4), lax.rem(y + (3 if c % 2 else 1), 4)
            passed = piece(behind, c)
            wait_recv(passed, h_r.at[phase, c, behind])
            remote(passed, passed, hy_s.at[phase, c, 2], h_r.at[phase, c, behind], row_peer(ahead))
            remote(passed, passed, hx_s.at[c, 1 if c % 2 else 3], hx_r.at[c, behind], near, when=is_2)

        def finish(c, a):
            if c == 0:
                squares = [to_column(sc_all[phase, 2 * y + k, 0:1, :], n) for k in range(2)]
                state["factor"] = lax.rsqrt(jnp.concatenate(squares, axis=0) * (1.0 / D_ALL) + 1e-6)
            factor = state["factor"]
            hidden, slope = gelu_both(a * factor)
            cols = slice(c * HC, (c + 1) * HC)
            h[pl.ds(2 * y, 2), h_rows, cols] = hidden.astype(BF).reshape(2, n, HC)
            for j in (1, 3) if passing(c) else (2, 1, 3):
                remote(
                    piece(y, c), piece(y, c), hy_s.at[phase, c, j], h_r.at[phase, c, y],
                    row_peer(lax.rem(y + j, 4)),
                )
            remote(piece(y, c), piece(y, c), hx_s.at[c, 0], hx_r.at[c, y], near, when=is_2) if relayed else None
            grad[:, h_rows, cols] = (slope * factor).astype(BF).reshape(2, n, HC)

        def project(c):
            if c == 0:
                loads[2 * phase + 1].wait()
            cols = slice(c * HC, (c + 1) * HC)
            for j in (0, 1, 3, 2):
                yy = lax.rem(y + j, 4)
                if j and not (passing(c) and j == (1 if c % 2 else 3)):
                    wait_recv(piece(yy, c), h_r.at[phase, c, yy])
                    if relayed:
                        remote(piece(yy, c), piece(yy, c), hx_s.at[c, j], hx_r.at[c, yy], near, when=is_2)
                both = h[pl.ds(2 * yy, 2), h_rows, cols].reshape(2 * n, HC)
                part = jnp.dot(both, down[cols, :], preferred_element_type=F32).reshape(2, n, FEAT)
                if c:
                    part += acc[pl.ds(2 * yy, 2)]
                acc[pl.ds(2 * yy, 2)] = part
                if c == CHUNKS - 1:
                    ta[yy] = acc[2 * yy + 1 - core].astype(BF)
                    remote(ta.at[yy], tb.at[yy], tp_s.at[phase, yy], tp_r.at[phase, yy], sibling)

        def after(c):
            if passing(c):
                pass_on(c)
            if relayed and c >= 3:
                project(c - 3)

        reduce_rep(phase, n, rows_of, block_of, product, bufs[:5], finish, gathered, lambda: None, after)
        for c in range(CHUNKS - 3 if relayed else 0, CHUNKS):
            project(c)
        total = None
        for d in (2, 1, 3, 0):
            yy = lax.rem(zl + d, 4)
            wait_recv(tb.at[yy], tp_r.at[phase, yy])
            both = acc[2 * yy + core] + tb[yy].astype(F32)
            if d:
                tc[d - 1] = both.astype(BF)
                remote(
                    tc.at[d - 1], td.at[d - 1], tp_s.at[phase, 3 + d], tp_r.at[phase, 3 + d],
                    dev(tt=2 * yy + core),
                )
            else:
                total = both
        for d in (1, 3, 2):
            wait_recv(td.at[d - 1], tp_r.at[phase, 3 + d])
            total += td[d - 1].astype(F32)
        return total

    x0 = xt[...].astype(F32)
    q_rows = pl.ds(qrow, QUARTER)
    out = forward(
        0, QUARTER, x0, gain[0:1, :], xgs, q_rows, hs, q_rows,
        (sb1, rb1, po1, zs1, zr1, acc1, ta1, tb1, tc1, td1), lambda: None,
    )
    gen[own, :] = (x0 + out).astype(BF)
    remote(gen.at[own, :], gen.at[own, :], gsend.at[0], grecv.at[0], dev(gg=g_pair))
    for i, ref in enumerate((gd.at[0, :, q_rows, :], xgs.at[:, q_rows, :], hs.at[:, q_rows, :])):
        remote(ref, ref, gsend.at[1 + i], grecv.at[1 + i], dev(gg=g_pair), when=is_late)
    wait_recv(rt, trecv.at[2], off_diag)
    t_row = ct[8:9, :].astype(F32)
    sigma = 0.1 + 0.8 * (t_row[:, 0:1] * 256.0 + t_row[:, LANES : LANES + 1]) / 999.0
    wait_recv(gen.at[pair, :], grecv.at[0])
    remote(gen.at[mine, :], gen.at[mine, :], gsend.at[4], grecv.at[4], dev(gg=g_near))

    gen_f = gen[mine, :].astype(F32)
    x_t = ((1.0 - sigma) * gen_f + sigma * rt[...].astype(F32)).astype(BF).astype(F32)
    all_rows = pl.ds(0, HALF)
    xgf_2 = xgf.at[1]

    def inputs_here():
        wait_recv(gen.at[other, :], grecv.at[4])
        remote(gen, gout, tsend.at[3], trecv.at[3], flip, when=off_diag)
        remote(xgf_2, xgf_2, gsend.at[5], grecv.at[5], near, when=is_2)

    gain_row = jnp.where(is_late, gain[2:3, :], gain[1:2, :])
    out = forward(
        1, HALF, x_t, gain_row, xgf.at[half], all_rows, hf.at[half], all_rows,
        (sb2, rb2, po2, zs2, zr2, acc2, ta2, tb2, tc2, td2),
        inputs_here,
    )
    fk[...] = (x_t + out).astype(BF)
    remote(fk, fother, gsend.at[6], grecv.at[6], dev(gg=g_pair), when=is_late)

    scale = 1.0 / math.sqrt(TOKENS)
    dy = dyb.at[half]

    @pl.when(is_late)
    def _():
        dy[t] = ((fk[...].astype(F32) - gen_f) * scale).astype(BF)
        dmine[...] = jnp.zeros_like(dmine)

    @pl.when(is_early)
    def _():
        real = fk[...].astype(F32)
        distance = jnp.sum(jnp.sum(jnp.abs(gen_f - real), axis=1, keepdims=True), axis=0, keepdims=True)
        dmine[0] = jnp.broadcast_to(distance, (8, LANES))
        cp = pltpu.make_async_remote_copy(
            src_ref=dmine.at[0], dst_ref=dmine.at[1], send_sem=gsend.at[7], recv_sem=grecv.at[7],
            device_id=near, device_id_type=MESH,
        )
        cp.start()
        wait_recv(fother, grecv.at[6])
        dy[t] = ((fother[...].astype(F32) - real) * scale).astype(BF)
        cp.wait()

    dy_block = lambda b: dy.at[b]
    gather_tp(2, dy_block)
    scalar_start(2, dmine[0, 0:1, :] + dmine[1, 0:1, :])

    da = dab.at[half]
    back = dnw.at[late]
    slope = gd.at[late]

    def product(rows, c):
        return lax.dot_general(
            rows, back[c * HC : (c + 1) * HC, :], (((1,), (1,)), ((), ())), preferred_element_type=F32
        )

    def da_piece(buf, yy, c):
        return buf.at[pl.ds(2 * yy, 2), :, pl.ds(c * HC, HC)]

    def image_scale(b):
        norm = sc_all[2, b, 0:1, 0:1] * (1.0 / (IMG_TOK * D_ALL)) + 1e-5
        return jnp.where(is_late, 1.0, 1.0 / norm)

    wait_recv(gd.at[0, :, pl.ds(QUARTER, QUARTER), :], grecv.at[1], is_early)
    not_2 = g != 2
    da_2 = dab.at[1]

    def pass_on(c):
        behind, ahead = lax.rem(y + (1 if c % 2 else 3), 4), lax.rem(y + (3 if c % 2 else 1), 4)
        passed = da_piece(da, behind, c)
        if c < CHUNKS - 1:
            wait_recv(passed, h_r.at[2, c, behind], not_2)
            remote(passed, passed, hy_s.at[2, c, 0], h_r.at[2, c, behind], row_peer(ahead), when=not_2)
        last = c == CHUNKS - 1
        for j in (1, 3, 2) if last else (2,):
            pair_2 = lax.rem(y + j, 4)
            crossing = da_piece(da_2, pair_2, c)
            wait_recv(crossing, h_r.at[2, c, pair_2], is_2)
            remote(crossing, crossing, xs_s.at[c, j], xs_r.at[c, pair_2], near, when=is_2)
        wait_recv(da_piece(da_2, y, c), xs_r.at[c, y], is_3)
        if not last:
            for j in (1, 3):
                remote(
                    da_piece(da_2, y, c), da_piece(da_2, y, c), xs_s.at[c, 3 + j], xs_r.at[c, y],
                    row_peer(lax.rem(y + j, 4)), when=is_3,
                )

    def when_sent(c, j):
        if j == 2:
            return None if c == CHUNKS - 1 else is_2
        return None if c == CHUNKS - 1 else not_2

    row_state = {}

    def finish(c, dh):
        if c == 0:
            scales = [jnp.broadcast_to(image_scale(2 * y + k), (HALF, 1)) for k in range(2)]
            row_state["scale"] = jnp.concatenate(scales, axis=0)
        cols = slice(c * HC, (c + 1) * HC)
        slopes = slope[:, :, cols].reshape(2 * HALF, HC).astype(F32)
        da[pl.ds(2 * y, 2), :, cols] = (dh * row_state["scale"] * slopes).astype(BF).reshape(2, HALF, HC)
        own_piece = da_piece(da, y, c)
        remote(own_piece, own_piece, xs_s.at[c, 0], xs_r.at[c, y], near, when=is_2)
        for j in (2, 1, 3):
            remote(
                own_piece, own_piece, hy_s.at[2, c, j], h_r.at[2, c, y], row_peer(lax.rem(y + j, 4)),
                when=when_sent(c, j),
            )

    dyb_2 = dyb.at[1]
    n_half, n_all = BLOCKS * HALF, 2 * BLOCKS * HALF

    def turned():
        @pl.when(is_early)
        def _():
            wait_recv(xgs_other, grecv.at[2])
            for k in range(BLOCKS // 2):
                two = xgs[2 * k : 2 * k + 2].reshape(2 * HALF, FEAT)
                ut[:, k * LANES : (k + 1) * LANES] = two.T

        @pl.when(is_3)
        def _():
            wait_recv(xgf_2, grecv.at[5])
            for k in range(BLOCKS):
                two = xgf[k // 4, 2 * (k % 4) : 2 * (k % 4) + 2].reshape(2 * HALF, FEAT)
                ut[:, k * LANES : (k + 1) * LANES] = two.T

    tn = (((0,), (0,)), ((), ()))
    step = 256

    def down_tiles(first, last):
        for i in range(first, last):
            cols = slice(i * step, (i + 1) * step)

            @pl.when(is_early)
            def _():
                dng_out[cols, :] = lax.dot_general(
                    hs[:, :, cols].reshape(n_half, step), dys[...].reshape(n_half, FEAT), tn,
                    preferred_element_type=F32,
                ).astype(BF)

            @pl.when(is_3)
            def _():
                dng_out[cols, :] = lax.dot_general(
                    hf[:, :, :, cols].reshape(n_all, step), dyb[...].reshape(n_all, FEAT), tn,
                    preferred_element_type=F32,
                ).astype(BF)

    def after(c):
        pass_on(c)
        if c == 0:

            @pl.when(is_early)
            def _():
                wait_recv(hs_other, grecv.at[3])
                for b in range(BLOCKS):
                    dys[b] = (dy[b].astype(F32) * image_scale(b)).astype(BF)

            @pl.when(is_3)
            def _():
                for k in range(CHUNKS):
                    for yy in range(4):
                        wait_recv(hf.at[1, 2 * yy : 2 * yy + 2, :, pl.ds(k * HC, HC)], hx_r.at[k, yy])
                wait_recv(dyb_2, grecv.at[8])

        if c < 3:
            down_tiles(2 * c, 2 * c + 2)

    xgs_other, hs_other = xgs.at[:, pl.ds(QUARTER, QUARTER), :], hs.at[:, pl.ds(QUARTER, QUARTER), :]
    reduce_rep(
        2, HALF, lambda yy: dy[pl.ds(2 * yy, 2)].reshape(2 * HALF, FEAT), dy_block, product,
        (sb3, rb3, po3, zs3, zr3), finish,
        lambda: remote(dyb_2, dyb_2, gsend.at[8], grecv.at[8], near, when=is_2), turned, after,
    )

    outs = [pltpu.make_async_copy(gout, gen_hbm, osem.at[0]), pltpu.make_async_copy(dng_out, dng_hbm, osem.at[1])]
    wait_recv(gout, trecv.at[3], off_diag)

    @pl.when(jnp.logical_not(off_diag))
    def _():
        gout[...] = gen[...]

    @pl.when(is_2)
    def _():
        upg_out[...] = jnp.zeros_like(upg_out)
        dng_out[...] = jnp.zeros_like(dng_out)

    outs[0].start()
    outs[1].start()
    for c in range(CHUNKS):
        cols = slice(c * HC, (c + 1) * HC)
        for j in (1, 3, 2):
            yy = lax.rem(y + j, 4)
            if c == CHUNKS - 1 or j != (1 if c % 2 else 3):
                wait_recv(da_piece(da, yy, c), h_r.at[2, c, yy], not_2)
            wait_recv(da_piece(da_2, yy, c), xs_r.at[c, yy], is_3)

        @pl.when(is_early)
        def _():
            upg_out[:, cols] = jnp.dot(
                ut[:, :n_half], da[:, :, cols].reshape(n_half, HC), preferred_element_type=F32
            ).astype(BF)

        @pl.when(is_3)
        def _():
            upg_out[:, cols] = jnp.dot(
                ut[...], dab[:, :, :, cols].reshape(n_all, HC), preferred_element_type=F32
            ).astype(BF)

        outs.append(pltpu.make_async_copy(upg_out.at[:, cols], upg_hbm.at[:, cols], osem.at[2 + c]))
        outs[-1].start()

    for cp, when in sends:
        if when is None:
            cp.wait_send()
        else:
            pl.when(when)(cp.wait_send)
    for cp in outs:
        cp.wait()


def widen(gen, up, down, gen_out, up_out, down_out):
    gen_out[...] = gen[...]
    up_out[0] = up[...].astype(F32)
    down_out[0] = down[...].astype(F32)


def rep_buffers(n):
    return [
        pltpu.VMEM((4, 2 * n, HID), BF),
        pltpu.VMEM((4, 2 * n, HID), BF),
        pltpu.VMEM((2 * n, HID), F32),
        pltpu.VMEM((2 * n, HID), BF),
        pltpu.VMEM((2 * n, HID), BF),
    ]


def tp_buffers(n):
    return [
        pltpu.VMEM((BLOCKS, n, FEAT), F32),
        pltpu.VMEM((4, n, FEAT), BF),
        pltpu.VMEM((4, n, FEAT), BF),
        pltpu.VMEM((3, n, FEAT), BF),
        pltpu.VMEM((3, n, FEAT), BF),
    ]


def body(noise_in, noise_renoise, text_cond, t_index, gains, up_weights, down_weights):
    vmem = pl.BlockSpec(memory_space=pltpu.VMEM)
    smem = pl.BlockSpec(memory_space=pltpu.SMEM)
    hbm = pl.BlockSpec(memory_space=pl.ANY)
    dma = pltpu.SemaphoreType.DMA
    generated, up_grad, down_grad = pl.pallas_call(
        kernel,
        name="step",
        out_shape=(
            jax.ShapeDtypeStruct((IMG_TOK, FEAT), BF),
            jax.ShapeDtypeStruct((FEAT, HID), BF),
            jax.ShapeDtypeStruct((HID, FEAT), BF),
        ),
        in_specs=[hbm, hbm, vmem, smem, hbm, hbm, hbm],
        out_specs=(hbm, hbm, hbm),
        scratch_shapes=[
            pltpu.VMEM((QUARTER, FEAT), BF),
            pltpu.VMEM((HALF, FEAT), BF),
            pltpu.VMEM((3, FEAT), F32),
            pltpu.VMEM((FEAT, HID), BF),
            pltpu.VMEM((HID, FEAT), BF),
            dma((3,)),
            dma((2 + CHUNKS,)),
            pltpu.VMEM((16, FEAT), BF),
            pltpu.VMEM((QUARTER, FEAT), BF),
            pltpu.VMEM((16, FEAT), BF),
            pltpu.VMEM((HALF, FEAT), BF),
            pltpu.VMEM((IMG_TOK, FEAT), BF),
            pltpu.VMEM((IMG_TOK, FEAT), BF),
            pltpu.VMEM((HALF, FEAT), BF),
            pltpu.VMEM((HALF, FEAT), BF),
            pltpu.VMEM((2, 8, LANES), F32),
            pltpu.VMEM((2, FEAT, HID), BF),
            pltpu.VMEM((2, HID, FEAT), BF),
            pltpu.VMEM((BLOCKS, HALF, FEAT), BF),
            pltpu.VMEM((BLOCKS, HALF, HID), BF),
            pltpu.VMEM((2, BLOCKS, HALF, FEAT), BF),
            pltpu.VMEM((2, BLOCKS, HALF, HID), BF),
            pltpu.VMEM((2, BLOCKS, HALF, FEAT), BF),
            pltpu.VMEM((2, BLOCKS, HALF, HID), BF),
            pltpu.VMEM((2, 2, HALF, HID), BF),
            pltpu.VMEM((BLOCKS, HALF, FEAT), BF),
            pltpu.VMEM((FEAT, 2 * BLOCKS * HALF), BF),
            pltpu.VMEM((3, 8, LANES), F32),
            pltpu.VMEM((3, 4, 8, LANES), F32),
            pltpu.VMEM((3, 8, LANES), F32),
            pltpu.VMEM((3, 8, LANES), F32),
            pltpu.VMEM((3, BLOCKS, 8, LANES), F32),
            *rep_buffers(QUARTER),
            *tp_buffers(QUARTER),
            *rep_buffers(HALF),
            *tp_buffers(HALF),
            *rep_buffers(HALF),
            dma((4,)),
            dma((4,)),
            dma((4,)),
            dma((10,)),
            dma((10,)),
            dma((3, 7)),
            dma((3, 8)),
            dma((3, CHUNKS, 4)),
            dma((3, CHUNKS, 4)),
            dma((3, CHUNKS)),
            dma((3, CHUNKS)),
            dma((3, CHUNKS, 4)),
            dma((3, CHUNKS, 4)),
            dma((2, 7)),
            dma((2, 7)),
            dma((CHUNKS, 7)),
            dma((CHUNKS, 4)),
            dma((CHUNKS, 4)),
            dma((CHUNKS, 4)),
            dma((3, 4)),
            dma((3, 4)),
            dma((3,)),
            dma((3,)),
            dma((3, 7)),
            dma((3, 8)),
        ],
        compiler_params=pltpu.CompilerParams(
            collective_id=0, has_side_effects=True, vmem_limit_bytes=60 * 2**20
        ),
    )(noise_in, noise_renoise, text_cond, t_index, gains, up_weights, down_weights)
    parts = 2
    rows = [
        pl.BlockSpec((IMG_TOK // parts, FEAT), lambda i: (i, 0)),
        pl.BlockSpec((FEAT // parts, HID), lambda i: (i, 0)),
        pl.BlockSpec((HID // parts, FEAT), lambda i: (i, 0)),
    ]
    wide = [
        rows[0],
        pl.BlockSpec((1, FEAT // parts, HID), lambda i: (0, i, 0)),
        pl.BlockSpec((1, HID // parts, FEAT), lambda i: (0, i, 0)),
    ]
    return pl.pallas_call(
        widen,
        name="widen",
        grid=(parts,),
        out_shape=(
            jax.ShapeDtypeStruct((IMG_TOK, FEAT), BF),
            jax.ShapeDtypeStruct((1, FEAT, HID), F32),
            jax.ShapeDtypeStruct((1, HID, FEAT), F32),
        ),
        in_specs=rows,
        out_specs=wide,
    )(generated, up_grad, down_grad)


def solution(mesh):
    in_specs = (
        P("rep", "tp"),
        P("rep", "tp"),
        P("rep", None),
        P("rep"),
        P(),
        P(None, "rep", "tp"),
        P(None, "tp", "rep"),
    )
    out_specs = (P("rep", "tp"), P("grp", "rep", "tp"), P("grp", "tp", "rep"))
    return jax.shard_map(body, mesh=mesh, in_specs=in_specs, out_specs=out_specs, check_vma=False)
```
